32 devices in a mesh: dp: 8 (over z, y), tensor: 4 (over x, core).
Axes of the slice: x: 2, y: 2, z: 4, core: 2. Of those that a mesh axis runs over, the one named last changes fastest.
Arguments:
- image_rows: bfloat16 [16, 197, 768], P('dp', None, 'tensor'), may hold values from -6 to 6
- text_rows: bfloat16 [8, 512, 768], P('dp', None, 'tensor'), may hold values from -6 to 6
- pair_rows: bfloat16 [8, 711, 768], P('dp', None, 'tensor'), may hold values from -6 to 6
- text_lengths: int32 [8], P('dp'), may hold values from 128 to 512, as said below
- pair_lengths: int32 [8], P('dp'), may hold values from 128 to 512, as said below
- qkv_weight: bfloat16 [3, 768, 3, 768], P(None, None, None, 'tensor'), may hold values from -0.21875 to 0.21875
- qv_bias: bfloat16 [3, 2, 768], P(None, None, 'tensor'), may hold values from -3 to 3
- out_weight: bfloat16 [3, 768, 768], P(None, 'tensor'), may hold values from -3.5 to 3.5
- out_bias: bfloat16 [3, 768], P(None, 'tensor'), may hold values from -3 to 3
- up_weight: bfloat16 [3, 768, 3072], P(None, None, 'tensor'), may hold values from -0.21875 to 0.21875
- up_bias: bfloat16 [3, 3072], P(None, 'tensor'), may hold values from -3 to 3
- down_weight: bfloat16 [3, 3072, 768], P(None, 'tensor'), may hold values from -0.109375 to 0.109375
- down_bias: bfloat16 [3, 768], P(None, 'tensor'), may hold values from -3 to 3
- norm_gain: bfloat16 [3, 2, 768], P(None, None, 'tensor'), may hold values from 0.099609375 to 1.8984375
- norm_bias: bfloat16 [3, 2, 768], P(None, None, 'tensor'), may hold values from -3 to 3
- image_upstream: bfloat16 [16, 197, 768], P('dp', None, 'tensor'), may hold values from -6 to 6
- text_upstream: bfloat16 [8, 512, 768], P('dp', None, 'tensor'), may hold values from -6 to 6
- pair_upstream: bfloat16 [8, 711, 768], P('dp', None, 'tensor'), may hold values from -6 to 6
Outputs:
- image_out: bfloat16 [16, 197, 768], P('dp', None, 'tensor')
- text_out: bfloat16 [8, 512, 768], P('dp', None, 'tensor')
- pair_out: bfloat16 [8, 711, 768], P('dp', None, 'tensor')
- image_input_grad: bfloat16 [16, 197, 768], P('dp', None, 'tensor')
- text_input_grad: bfloat16 [8, 512, 768], P('dp', None, 'tensor')
- pair_input_grad: bfloat16 [8, 711, 768], P('dp', None, 'tensor')
- qkv_grad: float32 [3, 768, 3, 768], P(None, 'dp', None, 'tensor')
- qv_bias_grad: float32 [3, 2, 768], P(None, None, 'tensor')
- out_weight_grad: float32 [3, 768, 768], P(None, 'tensor', 'dp')
- out_bias_grad: float32 [3, 768], P(None, 'tensor')
- up_weight_grad: float32 [3, 768, 3072], P(None, 'dp', 'tensor')
- up_bias_grad: float32 [3, 3072], P(None, 'tensor')
- down_weight_grad: float32 [3, 3072, 768], P(None, 'tensor', 'dp')
- down_bias_grad: float32 [3, 768], P(None, 'tensor')
- norm_gain_grad: float32 [3, 2, 768], P(None, None, 'tensor')
- norm_bias_grad: float32 [3, 2, 768], P(None, None, 'tensor')
The draws below stay inside these ranges and needn't reach their ends.
Inputs may be any that keep to these rules, and one draw needn't show every extreme that they name: Each text example's first text_lengths rows of 512 are valid; some example of every draw has all 512. Each pair's text rows after its 197 image rows: the first pair_lengths are valid, the rest and the two pad rows are not; some pair of every draw has all 512.
All inputs are finite; a program needn't handle non-finite values.
Results may differ from the reference program's by a relative error of at most 0.017.
Values may be sent and summed in bfloat16 or wider, within the bound.
A program may use at most 192 MiB of HBM per device.

```python
import math
import jax
import jax.numpy as jnp
from jax import lax

D = 768
HEADS = 12
HEAD_DIM = 64
FF = 3072
TOWERS = 3
PATCHES = 196
TXT_LEN = 512
IMG_LEN = 197
MM_LEN = 711
IMG_EX = 16
TXT_EX = 8
MM_EX = 8
N_TENSOR = 4


def length_draw(key, example_count):
    key_one, key_two = jax.random.split(key)
    drawn_len = jax.random.randint(key_one, (example_count,), TXT_LEN // 4, TXT_LEN + 1)
    position_at = jax.random.randint(key_two, (), 0, example_count)
    return jnp.where(jnp.arange(example_count) == position_at, TXT_LEN, drawn_len).astype(jnp.int32)


def draw_text_lengths(key, part):
    return length_draw(jax.random.fold_in(key, 17), TXT_EX)


def draw_pair_lengths(key, part):
    return length_draw(jax.random.fold_in(key, 29), MM_EX)


def block_levels(rng, extent, cuts, smallest, high):
    factor_of, own = 1.0, jax.random.fold_in(rng, 6)
    for dim, shards_of in cuts:
        draws = jnp.exp(jax.random.uniform(jax.random.fold_in(own, dim), (shards_of,), jnp.float32, smallest / len(cuts), high / len(cuts)))
        factor_of = factor_of * jnp.repeat(draws, extent[dim] // shards_of).reshape([-1 if axis == dim else 1 for axis in range(len(extent))])
    return factor_of


def gaussian(own_key, dims, deviation, reach, shards=(), kind=jnp.bfloat16):
    result = deviation * jax.random.normal(own_key, dims, jnp.float32)
    if shards:
        result = result * block_levels(own_key, dims, shards, -0.22, 0.18)
    return jnp.clip(result, -reach, reach).astype(kind)


def setup_inputs(seed: int = 0) -> dict:
    keys = jax.random.split(jax.random.key(seed), 19)
    image_rows = gaussian(keys[0], (IMG_EX, IMG_LEN, D), 1.0, 6.0, ((0, 8), (2, 4)))
    text_rows = gaussian(keys[1], (TXT_EX, TXT_LEN, D), 1.0, 6.0, ((0, 8), (2, 4)))
    pair_rows = gaussian(keys[2], (MM_EX, MM_LEN, D), 1.0, 6.0, ((0, 8), (2, 4)))
    text_lengths = draw_text_lengths(jax.random.fold_in(keys[18], 71), 0)
    pair_lengths = draw_pair_lengths(jax.random.fold_in(keys[18], 71), 0)
    qkv_weight = gaussian(keys[5], (TOWERS, D, 3, D), D ** -0.5, 0.21875, ((3, 4),))
    qv_bias = gaussian(keys[6], (TOWERS, 2, D), 0.5, 3.0, ((2, 4),))
    out_weight = gaussian(keys[7], (TOWERS, D, D), (max(1, D // 256)) ** -0.5, 3.5, ((1, 4),))
    out_bias = gaussian(keys[8], (TOWERS, D), 0.5, 3.0, ((1, 4),))
    up_weight = gaussian(keys[9], (TOWERS, D, FF), D ** -0.5, 0.21875, ((2, 4),))
    up_bias = gaussian(keys[10], (TOWERS, FF), 0.5, 3.0, ((1, 4),))
    down_weight = gaussian(keys[11], (TOWERS, FF, D), FF ** -0.5, 0.109375, ((1, 4),))
    down_bias = gaussian(keys[12], (TOWERS, D), 0.5, 3.0, ((1, 4),))
    norm_gain = jnp.clip(1.0 + 0.18 * jax.random.normal(keys[13], (TOWERS, 2, D), jnp.float32), 0.099609375, 1.8984375).astype(jnp.bfloat16)
    norm_bias = gaussian(keys[14], (TOWERS, 2, D), 0.5, 3.0, ((2, 4),))
    image_upstream = gaussian(keys[15], (IMG_EX, IMG_LEN, D), 1.0, 6.0, ((0, 8), (2, 4)))
    text_upstream = gaussian(keys[16], (TXT_EX, TXT_LEN, D), 1.0, 6.0, ((0, 8), (2, 4)))
    pair_upstream = gaussian(keys[17], (MM_EX, MM_LEN, D), 1.0, 6.0, ((0, 8), (2, 4)))
    return dict(image_rows=image_rows, text_rows=text_rows, pair_rows=pair_rows, text_lengths=text_lengths, pair_lengths=pair_lengths, qkv_weight=qkv_weight, qv_bias=qv_bias, out_weight=out_weight, out_bias=out_bias, up_weight=up_weight, up_bias=up_bias, down_weight=down_weight, down_bias=down_bias, norm_gain=norm_gain, norm_bias=norm_bias, image_upstream=image_upstream, text_upstream=text_upstream, pair_upstream=pair_upstream)


@jax.custom_vjp
def low(v):
    return lax.optimization_barrier(v.astype(jnp.bfloat16)).astype(jnp.float32)

@jax.custom_vjp
def low_back(v):
    return v

def low_keep(v):
    return (low(v), None)

def low_pass(kept, grad):
    return (grad,)

def back_keep(v):
    return (v, None)

def back_low(kept, grad):
    return (low(grad),)
low.defvjp(low_keep, low_pass)
low_back.defvjp(back_keep, back_low)
NORM_EPS = 1e-06
PRECISE = lax.Precision.HIGHEST

def rounded_both(value):
    return low_back(low(value))

def layer_norm(value, gain, shift):
    center = value - lax.optimization_barrier(jnp.mean(value, axis=-1, keepdims=True))
    spread = lax.optimization_barrier(jnp.mean(center * center, axis=-1, keepdims=True))
    return center * lax.rsqrt(spread + NORM_EPS) * gain + shift

def layer_block(row_block, key_mask, weights):
    qkv_w, qv_b, out_w, out_b, up_w, up_b, down_w, down_b, gain, shift = weights
    length = row_block.shape[0]
    groups = N_TENSOR
    share = D // groups
    hidden_share = FF // groups
    head_count = HEADS // groups
    scale = 1.0 / math.sqrt(HEAD_DIM)
    normed = low(layer_norm(row_block, gain[0], shift[0]))
    copies = low_back(jnp.broadcast_to(normed, (groups, length, D)))
    qkv_groups = qkv_w.reshape(D, 3, groups, share).transpose(2, 0, 1, 3)
    zero_bias = jnp.zeros_like(qv_b[0])
    bias_all = jnp.stack([qv_b[0], zero_bias, qv_b[1]], 0).reshape(3, groups, share).transpose(1, 0, 2)
    projected = rounded_both(jnp.einsum('gld,gdcf->glcf', copies, qkv_groups, precision=PRECISE) + bias_all[:, None])
    queries = projected[:, :, 0].reshape(groups, length, head_count, HEAD_DIM)
    key_heads = projected[:, :, 1].reshape(groups, length, head_count, HEAD_DIM)
    value_heads = projected[:, :, 2].reshape(groups, length, head_count, HEAD_DIM)
    scores = jnp.einsum('glhd,gmhd->ghlm', queries, key_heads, precision=PRECISE) * scale
    scores = low_back(jnp.where(key_mask[None, None, None, :], scores, -1000000000.0))
    probs_low = low(jax.nn.softmax(scores, axis=-1))
    mixed = rounded_both(jnp.einsum('ghlm,gmhd->glhd', probs_low, value_heads, precision=PRECISE).reshape(groups, length, share))
    partials = low(jnp.einsum('glf,gfe->gle', mixed, out_w.reshape(groups, share, D), precision=PRECISE))
    attention = low_back(lax.optimization_barrier(jnp.sum(partials, axis=0)) + out_b)
    residual_stream = row_block + attention
    normed_two = low(layer_norm(residual_stream, gain[1], shift[1]))
    copies_two = low_back(jnp.broadcast_to(normed_two, (groups, length, D)))
    up_groups = up_w.reshape(D, groups, hidden_share).transpose(1, 0, 2)
    hidden = low_back(jnp.einsum('gld,gdf->glf', copies_two, up_groups, precision=PRECISE) + up_b.reshape(groups, 1, hidden_share))
    activated = low(jax.nn.gelu(hidden, approximate=False))
    partials_two = low(jnp.einsum('glf,gfe->gle', activated, down_w.reshape(groups, hidden_share, D), precision=PRECISE))
    feedforward = low_back(lax.optimization_barrier(jnp.sum(partials_two, axis=0)) + down_b)
    return residual_stream + feedforward

def tower_pass(row_blocks, masks, weights):

    def one_example(example_in):
        return layer_block(example_in[0], example_in[1], weights)
    return lax.map(jax.checkpoint(one_example), (row_blocks, masks))

def reference(image_rows, text_rows, pair_rows, text_lengths, pair_lengths, qkv_weight, qv_bias, out_weight, out_bias, up_weight, up_bias, down_weight, down_bias, norm_gain, norm_bias, image_upstream, text_upstream, pair_upstream):
    image_mask = jnp.ones((image_rows.shape[0], IMG_LEN), dtype=bool)
    text_mask = jnp.arange(TXT_LEN, dtype=jnp.int32)[None, :] < text_lengths[:, None]
    pair_mask = jnp.arange(MM_LEN, dtype=jnp.int32)[None, :] < pair_lengths[:, None] + (PATCHES + 1)
    masks = (image_mask, text_mask, pair_mask)
    inputs = tuple((array_in.astype(jnp.float32) for array_in in (image_rows, text_rows, pair_rows)))
    params = tuple((array_in.astype(jnp.float32) for array_in in (qkv_weight, qv_bias, out_weight, out_bias, up_weight, up_bias, down_weight, down_bias, norm_gain, norm_bias)))

    def forward(tower_inputs, tower_params):
        results = []
        for tower_id in range(3):
            weights = tuple((entry[tower_id] for entry in tower_params))
            results.append(tower_pass(tower_inputs[tower_id], masks[tower_id], weights))
        return tuple(results)
    primal, pullback = jax.vjp(forward, inputs, params)
    upstreams = (image_upstream, text_upstream, pair_upstream)
    cotangent = tuple((upstreams[tower_id].astype(jnp.float32) for tower_id in range(3)))
    input_grads, param_grads = pullback(cotangent)
    return (primal[0].astype(jnp.bfloat16), primal[1].astype(jnp.bfloat16), primal[2].astype(jnp.bfloat16), input_grads[0].astype(jnp.bfloat16), input_grads[1].astype(jnp.bfloat16), input_grads[2].astype(jnp.bfloat16), param_grads[0], param_grads[1], param_grads[2], param_grads[3], param_grads[4], param_grads[5], param_grads[6], param_grads[7], param_grads[8], param_grads[9])
```

```python
from types import SimpleNamespace

import jax
import jax.numpy as jnp
from jax import lax
from jax.experimental import pallas as pl
from jax.experimental.pallas import tpu as pltpu
from jax.sharding import PartitionSpec as P

HEAD_DIM = 64
PATCHES = 196
EPSILON = 1e-06
TOWERS = 3
FIRST, SECOND = 0, 1
FFN, ATTN = 0, 1
TILE = 256
COLS = 12
N_REMOTE = 160
BF16 = jnp.bfloat16
F32 = jnp.float32
MESH = pl.DeviceIdType.MESH
INV_SQRT2 = 0.7071067811865476
INV_SQRT_2PI = 0.3989422804014327


def nn(a, b):
    return lax.dot_general(a, b, (((1,), (0,)), ((), ())), preferred_element_type=F32)


def nt(a, b):
    return lax.dot_general(a, b, (((1,), (1,)), ((), ())), preferred_element_type=F32)


def up(value, multiple):
    return -(-value // multiple) * multiple


class Plan:
    def __init__(self, rows, weights, dp, tensor):
        qkv, out, upw = weights
        self.dp = dp
        self.examples = [r.shape[0] for r in rows]
        self.length = [r.shape[1] for r in rows]
        self.padded = [up(n, TILE) for n in self.length]
        self.lanes = [e * n for e, n in zip(self.examples, self.padded)]
        self.width = qkv.shape[1]
        self.share = out.shape[1]
        self.hidden = upw.shape[2]
        self.heads = self.share // HEAD_DIM
        self.grad_lanes = (2 * self.hidden, 4 * self.share)
        self.pad = (3 * self.share) % TILE
        assert tensor == 4 and self.width == 4 * self.share
        assert self.pad + self.share == TILE and self.hidden % TILE == 0
        self.fused = dp % 2 == 0 and dp > 1 and self.width % (16 * dp) == 0
        self.nz = dp // 2 if self.fused else 1
        self.slab = self.width // dp if self.fused else self.width
        self.halves = 2 if self.fused else 1


class Out:
    def __init__(self, spec, shape, dtype=F32):
        self.spec, self.shape, self.dtype = spec, shape, dtype


def flatten(tree):
    return jax.tree.flatten(tree, is_leaf=lambda v: not isinstance(v, (dict, list)))


def scratch(plan):
    width, share, hidden, nz = plan.width, plan.share, plan.hidden, plan.nz
    half, most = width // 2, max(plan.lanes)
    dma = pltpu.SemaphoreType.DMA

    def vm(*shape, dtype=BF16):
        return pltpu.VMEM(shape, dtype)

    def each(*lead, dtype=BF16):
        return [pltpu.VMEM((*lead, lanes), dtype) for lanes in plan.lanes]

    k = SimpleNamespace()
    k.x, k.dy, k.n = each(width), each(width), each(width)
    k.sums = [each(width), each(width)]
    k.part, k.rpart = each(width), each(width)
    k.qkv, k.m = each(3 * share), each(TILE)
    k.p = [vm(e * plan.heads, n, n) for e, n in zip(plan.examples, plan.padded)]
    k.near, k.far = each(half), [each(half), each(half)]
    k.rnear, k.rfar = each(2, share), [each(share), each(share)]
    k.own, k.row = each(share, dtype=F32), each(8, dtype=F32)
    k.stat_own, k.stat_near = each(8, dtype=F32), each(8, dtype=F32)
    k.stat_chip, k.stat_far = each(8, dtype=F32), each(8, dtype=F32)
    land = plan.slab if plan.fused else 16
    k.g_all = [vm(plan.halves, nz, plan.slab, n) for n in plan.grad_lanes]
    k.g_y = [vm(nz, land, n) for n in plan.grad_lanes]
    k.g_z = [vm(nz, land, n) for n in plan.grad_lanes]
    k.credit = [pltpu.SemaphoreType.REGULAR for _ in plan.grad_lanes]
    k.out_sem = [dma((2,)) for _ in plan.grad_lanes]
    if plan.fused:
        k.g_far = [
            [vm(max(nz - 1, 1), plan.slab, n) for _ in range(TOWERS)] for n in plan.grad_lanes
        ]
        k.s_ffn = vm(2, plan.slab, hidden, dtype=F32)
        k.s_qkv = vm(3, plan.slab, share, dtype=F32)
        k.s_out = vm(share, plan.slab, dtype=F32)
    k.wqkv_v, k.wout_v = vm(2, 3 * share, width), vm(2, share, width)
    k.wup_v, k.wdown_v = vm(width, hidden), vm(hidden, width)
    k.up_t, k.down_t = vm(hidden, width), vm(width, hidden)
    k.work_n, k.work_a = vm(width, most), vm(hidden, most)
    k.work_h, k.work_m = vm(width, most), vm(share, most)
    k.pown, k.pfull = vm(share, 128, dtype=F32), vm(width, 128)
    k.small, k.small_y = vm(share, 128, dtype=F32), vm(share, 128, dtype=F32)
    k.small_z = vm(nz, share, 128, dtype=F32)
    k.in_sem, k.w_sem, k.part_sem = dma((2 * TOWERS,)), dma((18,)), dma((TOWERS,))
    k.send_sem, k.recv_sem = dma((N_REMOTE,)), dma((N_REMOTE,))
    return k


def kernel(plan, r):
    width, share, hidden, heads = plan.width, plan.share, plan.hidden, plan.heads
    half = width // 2
    nz = plan.nz

    dp_at = lax.axis_index("dp")
    me = lax.axis_index("tensor")
    core = lax.rem(me, 2)
    chip = lax.div(me, 2)
    y_at = lax.rem(dp_at, 2)
    z_at = lax.div(dp_at, 2)
    sibling = (dp_at, me + 1 - 2 * core)
    across = (dp_at, lax.rem(me + 2, 4))
    y_peer = (dp_at + 1 - 2 * y_at, me)

    def z_index(k):
        return lax.rem(z_at + k, nz)

    def z_peer(k):
        return (z_index(k) * 2 + y_at, me)

    counter = [0]
    pending = []

    def remote(src, dst, device):
        at = counter[0]
        counter[0] += 1
        assert at < N_REMOTE
        return pltpu.make_async_remote_copy(
            src_ref=src,
            dst_ref=dst,
            send_sem=r.send_sem.at[at],
            recv_sem=r.recv_sem.at[at],
            device_id=device,
            device_id_type=MESH,
        )

    def launch(copy):
        copy.start()
        pending.append(copy)
        return copy

    def sent(copy):
        copy.wait_send()
        pending[:] = [other for other in pending if other is not copy]

    def block(at, size):
        return pl.ds(pl.multiple_of(at * size, size), size)

    own = block(me, share)
    my_half, other_half = block(core, half), block(1 - core, half)

    def lanes_loop(lanes, tile, body):
        def step(at, carry):
            body(block(at, tile))
            return carry

        lax.fori_loop(0, lanes // tile, step, 0)

    lane_of_small = lax.broadcasted_iota(jnp.int32, (share, 128), 1)

    def keep_sum(t, j, value):
        column = jnp.sum(value.astype(F32), axis=1, keepdims=True)
        small = r.small
        small[...] = jnp.where(lane_of_small == t * COLS + j, column, small[...])

    def own_col(t, j):
        return r.pown[:, t * COLS + j : t * COLS + j + 1]

    def full_col(t, j):
        return r.pfull[...].astype(F32)[:, t * COLS + j : t * COLS + j + 1]

    class Gather:
        def __init__(self, buf):
            self.to_sibling = remote(buf.at[own], buf.at[own], sibling)
            self.to_across = remote(buf.at[own], buf.at[own], across)
            blk = block(lax.rem(me + 2, 4), share)
            self.forwarded = remote(buf.at[blk], buf.at[blk], sibling)

        def start(self):
            launch(self.to_across)
            launch(self.to_sibling)

        def forward(self):
            self.to_across.wait_recv()
            launch(self.forwarded)

        def finish(self):
            self.to_sibling.wait_recv()
            self.forwarded.wait_recv()

    class AllReduce:
        def __init__(self, t, which):
            self.part, self.near = r.part[t], r.near[t]
            self.far, self.out = r.far[which][t], r.sums[which][t]
            self.c1 = remote(self.part.at[other_half], self.near, sibling)
            self.c2 = remote(self.part.at[my_half], self.far, across)
            self.c3 = remote(self.out.at[my_half], self.out.at[my_half], sibling)

        def begin(self):
            launch(self.c1)

        def cross(self):
            self.c1.wait_recv()
            total = self.part[my_half].astype(F32) + self.near[...].astype(F32)
            self.part[my_half] = total.astype(BF16)
            launch(self.c2)

        def back(self):
            self.c2.wait_recv()
            total = self.part[my_half].astype(F32) + self.far[...].astype(F32)
            self.out[my_half] = total.astype(BF16)
            launch(self.c3)

        def finish(self):
            self.c3.wait_recv()

        def free(self):
            sent(self.c1)
            sent(self.c2)
            sent(self.c3)

    class Scatter:
        def __init__(self, t, which):
            self.part, self.near, self.far = r.rpart[t], r.rnear[t], r.rfar[which][t]
            self.far_blk = block(2 * (1 - chip) + core, share)
            theirs = (2 * (1 - chip) + 1 - core, 2 * chip + 1 - core)
            self.c1 = [
                remote(self.part.at[block(theirs[j], share)], self.near.at[j], sibling)
                for j in range(2)
            ]
            self.c2 = remote(self.part.at[self.far_blk], self.far, across)

        def begin(self):
            for copy in self.c1:
                launch(copy)

        def cross(self):
            self.c1[0].wait_recv()
            blk = self.far_blk
            self.part[blk] = (self.part[blk].astype(F32) + self.near[0].astype(F32)).astype(BF16)
            launch(self.c2)
            self.c1[1].wait_recv()
            self.part[own] = (self.part[own].astype(F32) + self.near[1].astype(F32)).astype(BF16)

        def finish(self):
            self.c2.wait_recv()

        def free(self):
            for copy in self.c1:
                sent(copy)
            sent(self.c2)

    class Stats:
        def __init__(self, t):
            self.c1 = remote(r.stat_own[t], r.stat_near[t], sibling)
            self.c2 = remote(r.stat_chip[t], r.stat_far[t], across)
            self.t = t

        def begin(self):
            launch(self.c1)

        def cross(self):
            t = self.t
            self.c1.wait_recv()
            r.stat_chip[t][...] = r.stat_own[t][...] + r.stat_near[t][...]
            launch(self.c2)

        def finish(self):
            self.c2.wait_recv()

    class GradSum:
        def __init__(self, which):
            self.all, self.land, self.sums = r.g_all[which], r.g_y[which], r.g_z[which]
            self.credit = r.credit[which]
            self.which = which
            self.y_copies, self.z_copies, self.hbm = {}, {}, {}

        def send(self, t):
            if not plan.fused:
                copy = pltpu.make_async_copy(
                    self.all.at[0, 0], r.o_g[self.which].at[t], r.part_sem.at[t]
                )
                copy.start()
                copy.wait()
                return
            if t:
                pl.semaphore_wait(self.credit, 1)
            self.y_copies[t] = []
            for j in range(nz):
                at = z_index(1 + j)
                copy = remote(self.all.at[1 - y_at, at], self.land.at[at], y_peer)
                self.y_copies[t].append(launch(copy))

        def relay(self, t):
            if not plan.fused:
                return
            if t:
                for copy in self.z_copies[t - 1]:
                    sent(copy)
            self.z_copies[t] = []
            for j in range(nz):
                at = z_index(1 + j)
                copy = self.y_copies[t][j]
                copy.wait_recv()
                total = self.all[y_at, at].astype(F32) + self.land[at].astype(F32)
                self.sums[at] = total.astype(BF16)
                if j < nz - 1:
                    dst = r.g_far[self.which][t].at[j]
                    self.z_copies[t].append(launch(remote(self.sums.at[at], dst, z_peer(1 + j))))
            for copy in self.y_copies[t]:
                sent(copy)
            if t < TOWERS - 1:
                pl.semaphore_signal(self.credit, inc=1, device_id=y_peer, device_id_type=MESH)

        def finish(self, t):
            if not plan.fused:
                return
            total = self.sums[z_at].astype(F32)
            for j in range(nz - 1):
                self.z_copies[t][j].wait_recv()
                total = total + r.g_far[self.which][t][j].astype(F32)
            if t:
                for copy in self.hbm[t - 1]:
                    copy.wait()
            sem = r.out_sem[self.which]
            if self.which == FFN:
                r.s_ffn[0] = total[:, :hidden]
                r.s_ffn[1] = total[:, hidden:]
                self.hbm[t] = [
                    pltpu.make_async_copy(r.s_ffn.at[0], r.o_up.at[t], sem.at[0]),
                    pltpu.make_async_copy(r.s_ffn.at[1], r.o_down.at[t], sem.at[1]),
                ]
            else:
                for c in range(3):
                    r.s_qkv[c] = total[:, c * share : (c + 1) * share]
                r.s_out[...] = total[:, 3 * share :].T
                self.hbm[t] = [
                    pltpu.make_async_copy(r.s_qkv, r.o_qkv.at[t], sem.at[0]),
                    pltpu.make_async_copy(r.s_out, r.o_out.at[t], sem.at[1]),
                ]
            for copy in self.hbm[t]:
                copy.start()

    gx = [Gather(r.x[t]) for t in range(TOWERS)]
    gdy = [Gather(r.dy[t]) for t in range(TOWERS)]
    gp = Gather(r.pfull)
    ar1 = [AllReduce(t, FIRST) for t in range(TOWERS)]
    ar2 = [AllReduce(t, SECOND) for t in range(TOWERS)]
    rs1 = [Scatter(t, FIRST) for t in range(TOWERS)]
    rs2 = [Scatter(t, SECOND) for t in range(TOWERS)]
    stats = [Stats(t) for t in range(TOWERS)]
    grad_b, grad_c = GradSum(FFN), GradSum(ATTN)

    def attn_load(use):
        t, slot = use % TOWERS, use % 2
        pairs = ((r.wqkv, r.wqkv_v), (r.wout, r.wout_v))
        return [
            pltpu.make_async_copy(src.at[t], dst.at[slot], r.w_sem.at[6 + 2 * use + i])
            for i, (src, dst) in enumerate(pairs)
        ]

    attn_w = [attn_load(use) for use in range(2 * TOWERS)]
    ffn_w = [
        [
            pltpu.make_async_copy(r.wup.at[t], r.wup_v, r.w_sem.at[2 * t]),
            pltpu.make_async_copy(r.wdown.at[t], r.wdown_v, r.w_sem.at[2 * t + 1]),
        ]
        for t in range(TOWERS)
    ]

    def transpose_into(dst, src, rows, cols):
        for at in range(0, rows, TILE):
            size = min(TILE, rows - at)
            dst[:cols, at : at + size] = src[at : at + size, :].T

    def stage_in(ref, t, source):
        length, padded = plan.length[t], plan.padded[t]
        for e in range(plan.examples[t]):
            base = e * padded
            if length < padded:
                first = length // 128 * 128
                ref[own, base + first : base + padded] = jnp.zeros((share, padded - first), BF16)
            ref[own, base : base + length] = source[e]

    def a_norm(t):
        gain, shift = full_col(t, 0), full_col(t, 2)

        def body(ls):
            x = r.x[t][:, ls].astype(F32)
            mean = jnp.sum(x, axis=0, keepdims=True) / width
            center = x - mean
            inv = lax.rsqrt(jnp.sum(center * center, axis=0, keepdims=True) / width + EPSILON)
            r.n[t][:, ls] = (center * inv * gain + shift).astype(BF16)
            r.row[t][0:1, ls] = mean
            r.row[t][1:2, ls] = inv

        lanes_loop(plan.lanes[t], 128, body)

    def a_qkv(t):
        for copy in attn_w[t]:
            copy.wait()
        bias = jnp.concatenate(
            [own_col(t, 5), jnp.zeros((share, 1), F32), own_col(t, 6)], axis=0
        )

        def body(ls):
            value = nn(r.wqkv_v[t % 2], r.n[t][:, ls]) + bias
            r.qkv[t][:, ls] = value.astype(BF16)

        lanes_loop(plan.lanes[t], TILE, body)

    def valid_keys(t, e):
        if t == 0:
            return plan.length[0]
        if t == 1:
            return r.lengths[e]
        return r.lengths[plan.examples[1] + e] + (PATCHES + 1)

    def a_heads(t):
        padded = plan.padded[t]
        key_at = lax.broadcasted_iota(jnp.int32, (padded, 1), 0)
        qkv = r.qkv[t]
        for e in range(plan.examples[t]):
            base = e * padded
            valid = key_at < valid_keys(t, e)

            def head(h, carry):
                rows_q = block(h, HEAD_DIM)
                rows_k = block(h + heads, HEAD_DIM)
                rows_v = block(h + 2 * heads, HEAD_DIM)
                rows_m = block(h + plan.pad // HEAD_DIM, HEAD_DIM)
                keys = qkv[rows_k, base : base + padded].T
                values = qkv[rows_v, base : base + padded]
                for q in range(padded // TILE):
                    at = base + q * TILE
                    s = nn(keys, qkv[rows_q, at : at + TILE]) * (HEAD_DIM**-0.5)
                    s = jnp.where(valid, s, -1000000000.0)
                    p = jnp.exp(s - jnp.max(s, axis=0, keepdims=True))
                    p = (p * (1.0 / jnp.sum(p, axis=0, keepdims=True))).astype(BF16)
                    r.p[t][e * heads + h, :, q * TILE : (q + 1) * TILE] = p
                    r.m[t][rows_m, at : at + TILE] = nn(values, p).astype(BF16)
                return carry

            lax.fori_loop(0, heads, head, 0)

    def a_out(t):
        transpose_into(r.up_t, r.wout_v.at[t % 2], share, width)

        def body(ls):
            mixed = r.m[t][plan.pad :, ls]
            r.part[t][:, ls] = nn(r.up_t[:, :share], mixed).astype(BF16)

        lanes_loop(plan.lanes[t], TILE, body)
        ar1[t].begin()
        for copy in attn_w[t + 2]:
            copy.start()

    def b_main(t):
        for copy in ffn_w[t]:
            copy.wait()
        transpose_into(r.up_t, r.wup_v, width, hidden)
        transpose_into(r.down_t, r.wdown_v, hidden, width)
        out_bias, gain, shift = full_col(t, 4), full_col(t, 1), full_col(t, 3)
        up_bias = jnp.concatenate([own_col(t, 8 + j) for j in range(hidden // share)], axis=0)
        ar1[t].free()

        def body(ls):
            x, s = r.x[t], r.sums[FIRST][t]
            resid = x[:, ls].astype(F32) + (s[:, ls].astype(F32) + out_bias)
            r.own[t][:, ls] = x[own, ls].astype(F32) + (s[own, ls].astype(F32) + own_col(t, 4))
            mean = jnp.sum(resid, axis=0, keepdims=True) / width
            center = resid - mean
            inv = lax.rsqrt(jnp.sum(center * center, axis=0, keepdims=True) / width + EPSILON)
            xhat = center * inv
            r.row[t][2:3, ls] = inv
            normed = (xhat * gain + shift).astype(BF16)
            s[:, ls] = xhat.astype(BF16)
            r.work_n[:, ls] = normed
            h = nn(r.up_t[...], normed) + up_bias
            cdf = 0.5 * (1.0 + lax.erf(h * INV_SQRT2))
            r.work_a[:, ls] = (h * cdf).astype(BF16)
            slope = cdf + h * (jnp.exp(-0.5 * (h * h)) * INV_SQRT_2PI)
            dact = nn(r.wdown_v[...], r.dy[t][:, ls])
            dhid = (dact * slope).astype(BF16)
            r.work_h[:hidden, ls] = dhid
            r.part[t][:, ls] = nn(r.wup_v[...], dhid).astype(BF16)

        lanes_loop(plan.lanes[t], TILE, body)
        ar2[t].begin()

    def b_ffn(t):
        def body(ls):
            r.rpart[t][:, ls] = nn(r.down_t[...], r.work_a[:, ls]).astype(BF16)

        lanes_loop(plan.lanes[t], TILE, body)
        rs1[t].begin()

    def spread(dst, value, ls):
        for b in range(plan.halves * nz):
            part = value[b * plan.slab : (b + 1) * plan.slab].astype(BF16)
            dst[b % plan.halves, b // plan.halves, :, ls] = part

    def b_grad(t):
        lanes = plan.lanes[t]

        def step(at, carry):
            rows = block(at, TILE)
            value = nt(r.work_n[:, :lanes], r.work_h[rows, :lanes])
            spread(r.g_all[FFN], value, rows)
            value = nt(r.dy[t][...], r.work_a[rows, :lanes])
            spread(r.g_all[FFN], value, block(at + hidden // TILE, TILE))
            return carry

        lax.fori_loop(0, hidden // TILE, step, 0)
        grad_b.send(t)
        for j in range(hidden // share):
            keep_sum(t, 3 + j, r.work_h[j * share : (j + 1) * share, :lanes])
        keep_sum(t, 7, r.dy[t][own])

    def y_out(t):
        rs1[t].finish()
        value = r.own[t][...] + (
            r.rpart[t][own].astype(F32) + r.rfar[FIRST][t][...].astype(F32) + own_col(t, 7)
        )
        padded = plan.padded[t]
        for e in range(plan.examples[t]):
            out = value[:, e * padded : e * padded + plan.length[t]]
            r.o_y[t][e] = out.astype(BF16)

    def c_norm(t):
        ar2[t].finish()
        for copy in attn_w[TOWERS + t]:
            copy.wait()
        slot = (TOWERS + t) % 2
        gain, gain_own = full_col(t, 1), own_col(t, 1)

        def body(ls):
            dn, xhat = r.sums[SECOND][t], r.sums[FIRST][t]
            xh = xhat[:, ls].astype(F32)
            e = dn[:, ls].astype(F32) * gain
            m1 = jnp.sum(e, axis=0, keepdims=True) / width
            m2 = jnp.sum(e * xh, axis=0, keepdims=True) / width
            inv = r.row[t][2:3, ls]
            dres = r.dy[t][:, ls].astype(F32) + inv * (e - m1 - xh * m2)
            r.work_n[:, ls] = dres.astype(BF16)
            e_own = dn[own, ls].astype(F32) * gain_own
            r.own[t][:, ls] = r.dy[t][own, ls].astype(F32) + inv * (
                e_own - m1 - xhat[own, ls].astype(F32) * m2
            )

        lanes_loop(plan.lanes[t], 128, body)

        def mix(ls):
            r.work_m[:, ls] = nn(r.wout_v[slot], r.work_n[:, ls]).astype(BF16)

        lanes_loop(plan.lanes[t], TILE, mix)

    def c_heads(t):
        padded = plan.padded[t]
        qkv = r.qkv[t]
        scale = HEAD_DIM**-0.5
        for e in range(plan.examples[t]):
            base = e * padded

            def head(h, carry):
                rows_q = block(h, HEAD_DIM)
                rows_k = block(h + heads, HEAD_DIM)
                rows_v = block(h + 2 * heads, HEAD_DIM)
                keys = qkv[rows_k, base : base + padded]
                values = qkv[rows_v, base : base + padded].T
                dk = dv = None
                for q in range(padded // TILE):
                    at = base + q * TILE
                    dm = r.work_m[rows_q, at : at + TILE]
                    p = r.p[t][e * heads + h, :, q * TILE : (q + 1) * TILE]
                    dp = nn(values, dm)
                    pf = p.astype(F32)
                    delta = jnp.sum(pf * dp, axis=0, keepdims=True)
                    ds = (pf * (dp - delta)).astype(BF16)
                    dq = nn(keys, ds) * scale
                    r.work_h[rows_q, at : at + TILE] = dq.astype(BF16)
                    dk_q = nt(qkv[rows_q, at : at + TILE], ds)
                    dv_q = nt(dm, p)
                    dk = dk_q if dk is None else dk + dk_q
                    dv = dv_q if dv is None else dv + dv_q
                r.work_h[rows_k, base : base + padded] = (dk * scale).astype(BF16)
                r.work_h[rows_v, base : base + padded] = dv.astype(BF16)
                return carry

            lax.fori_loop(0, heads, head, 0)

    def c_norm_in(t):
        transpose_into(r.up_t, r.wqkv_v.at[(TOWERS + t) % 2], 3 * share, width)
        gain = full_col(t, 0)
        rs1[t].free()

        def body(ls):
            dn = nn(r.up_t[:, : 3 * share], r.work_h[: 3 * share, ls])
            e = dn * gain
            xhat = (r.x[t][:, ls].astype(F32) - r.row[t][0:1, ls]) * r.row[t][1:2, ls]
            r.stat_own[t][0:1, ls] = jnp.sum(e, axis=0, keepdims=True)
            r.stat_own[t][1:2, ls] = jnp.sum(e * xhat, axis=0, keepdims=True)
            r.rpart[t][:, ls] = dn.astype(BF16)

        lanes_loop(plan.lanes[t], TILE, body)
        rs2[t].begin()
        stats[t].begin()
        if t == 0:
            for copy in attn_w[5]:
                copy.start()

    def c_grad(t):
        lanes = plan.lanes[t]
        r.work_h[3 * share :, :lanes] = jnp.zeros((width - 3 * share, lanes), BF16)
        whole = 3 * share // TILE

        def step(at, carry):
            rows = block(at, TILE)
            spread(r.g_all[ATTN], nt(r.n[t][...], r.work_h[rows, :lanes]), rows)
            return carry

        lax.fori_loop(0, whole, step, 0)
        last = slice(whole * TILE, (whole + 1) * TILE)
        value = nt(r.n[t][...], r.work_h[last, :lanes])
        value = value + nt(r.work_n[:, :lanes], r.m[t][...])
        spread(r.g_all[ATTN], value, last)
        grad_c.send(t)
        keep_sum(t, 0, r.work_h[:share, :lanes])
        keep_sum(t, 1, r.work_h[2 * share : 3 * share, :lanes])
        keep_sum(t, 2, r.work_n[own, :lanes])
        dn, xhat = r.sums[SECOND][t], r.sums[FIRST][t]
        keep_sum(t, 9, dn[own].astype(F32) * xhat[own].astype(F32))
        keep_sum(t, 11, dn[own])

    def last_norm(t):
        rs2[t].finish()
        stats[t].finish()
        gain = own_col(t, 0)
        dn = r.rpart[t][own].astype(F32) + r.rfar[SECOND][t][...].astype(F32)
        total = r.stat_chip[t][...] + r.stat_far[t][...]
        inv = r.row[t][1:2, :]
        xhat = (r.x[t][own].astype(F32) - r.row[t][0:1, :]) * inv
        value = r.own[t][...] + inv * (
            dn * gain - total[0:1] / width - xhat * (total[1:2] / width)
        )
        padded = plan.padded[t]
        for e in range(plan.examples[t]):
            out = value[:, e * padded : e * padded + plan.length[t]]
            r.o_dx[t][e] = out.astype(BF16)
        keep_sum(t, 8, dn * xhat)
        keep_sum(t, 10, dn)

    def small_out():
        small = r.small
        if not plan.fused:
            r.o_small[...] = small[...]
            return
        copy = launch(remote(small, r.small_y, y_peer))
        copy.wait_recv()
        r.small_z[z_at] = small[...] + r.small_y[...]
        copies = []
        for k in range(1, nz):
            slot = r.small_z.at[z_at]
            copies.append(launch(remote(slot, slot, z_peer(k))))
        for copy in copies:
            copy.wait_recv()
        total = r.small_z[0]
        for k in range(1, nz):
            total = total + r.small_z[k]
        rows = total.T
        for t in range(TOWERS):
            base = t * COLS
            for j in range(2):
                r.o_qvb[t, j, :] = rows[base + j, :]
                r.o_gain[t, j, :] = rows[base + 8 + j, :]
                r.o_bias[t, j, :] = rows[base + 10 + j, :]
            r.o_outb[t, :] = rows[base + 2, :]
            r.o_downb[t, :] = rows[base + 7, :]
            for j in range(hidden // share):
                r.o_upb[t * (hidden // share) + j, :] = rows[base + 3 + j, :]

    loads = [
        pltpu.make_async_copy(src[t], dst[t], r.in_sem.at[i * TOWERS + t])
        for i, (src, dst) in enumerate(((r.in_x, r.o_y), (r.in_dy, r.o_dx)))
        for t in range(TOWERS)
    ]
    for copy in loads + attn_w[0] + attn_w[1] + ffn_w[0]:
        copy.start()
    for t in range(TOWERS):
        loads[t].wait()
        stage_in(r.x[t], t, r.o_y[t])
    r.pown[...] = r.prm[...].T
    r.pfull[own] = r.pown[...].astype(BF16)
    barrier = pltpu.get_barrier_semaphore()
    partners = [sibling, across]
    if plan.fused:
        partners += [y_peer] + [z_peer(k) for k in range(1, nz)]
    for device in partners:
        pl.semaphore_signal(barrier, inc=1, device_id=device, device_id_type=MESH)
    pl.semaphore_wait(barrier, len(partners))
    gp.start()
    gx[0].start()
    gx[1].start()
    gx[2].start()
    for t in range(TOWERS):
        loads[TOWERS + t].wait()
        stage_in(r.dy[t], t, r.o_dx[t])
        r.m[t][: plan.pad] = jnp.zeros((plan.pad, plan.lanes[t]), BF16)
        r.stat_own[t][...] = jnp.zeros_like(r.stat_own[t])
    r.small[...] = jnp.zeros_like(r.small)
    gp.forward()
    gx[0].forward()
    gp.finish()
    gx[0].finish()

    a_norm(0)
    a_qkv(0)
    gx[1].forward()
    a_heads(0)
    a_out(0)
    gx[1].finish()
    a_norm(1)
    ar1[0].cross()
    gdy[0].start()
    gx[2].forward()
    a_qkv(1)
    a_heads(1)
    a_out(1)
    gx[2].finish()
    ar1[0].back()
    a_norm(2)
    gdy[0].forward()
    ar1[1].cross()
    gdy[1].start()
    a_qkv(2)
    ar1[0].finish()
    gdy[0].finish()
    b_main(0)
    b_ffn(0)
    ar1[1].back()
    ar2[0].cross()
    rs1[0].cross()
    b_grad(0)
    for copy in ffn_w[1]:
        copy.start()
    gdy[1].forward()
    a_heads(2)
    a_out(2)
    ar2[0].back()
    grad_b.relay(0)
    ar1[1].finish()
    gdy[1].finish()
    ar1[2].cross()
    gdy[2].start()
    b_main(1)
    ar1[2].back()
    b_ffn(1)
    ar2[1].cross()
    rs1[1].cross()
    y_out(0)
    b_grad(1)
    for copy in ffn_w[2]:
        copy.start()
    gdy[2].forward()
    c_norm(0)
    c_heads(0)
    ar2[1].back()
    c_norm_in(0)
    rs2[0].cross()
    stats[0].cross()
    c_grad(0)
    grad_b.finish(0)
    grad_b.relay(1)
    ar1[2].finish()
    gdy[2].finish()
    b_main(2)
    b_ffn(2)
    ar2[2].cross()
    rs1[2].cross()
    grad_c.relay(0)
    y_out(1)
    b_grad(2)
    last_norm(0)
    c_norm(1)
    c_heads(1)
    ar2[2].back()
    c_norm_in(1)
    rs2[1].cross()
    stats[1].cross()
    c_grad(1)
    grad_b.finish(1)
    grad_b.relay(2)
    grad_c.finish(0)
    y_out(2)
    c_norm(2)
    grad_c.relay(1)
    c_heads(2)
    c_norm_in(2)
    rs2[2].cross()
    stats[2].cross()
    c_grad(2)
    last_norm(1)
    grad_b.finish(2)
    grad_c.finish(1)
    grad_c.relay(2)
    last_norm(2)
    small_out()
    grad_c.finish(2)
    for copy in list(pending):
        sent(copy)
    for grad in (grad_b, grad_c):
        for copy in grad.hbm.get(TOWERS - 1, []):
            copy.wait()


def per_device(dp, tensor, *args):
    rows, ups = args[0:3], args[15:18]
    text_lengths, pair_lengths = args[3:5]
    qkv_w, qv_b, out_w, out_b, up_w, up_b, down_w, down_b, gain, shift = args[5:15]
    plan = Plan(rows, (qkv_w, out_w, up_w), dp, tensor)
    width, share, hidden = plan.width, plan.share, plan.hidden
    ratio = hidden // share
    nz = plan.nz

    turned = [jnp.transpose(x, (0, 2, 1)) for x in rows]
    turned_up = [jnp.transpose(x, (0, 2, 1)) for x in ups]
    wqkv = jnp.transpose(qkv_w, (0, 2, 3, 1)).reshape(TOWERS, 3 * share, width)
    columns = jnp.concatenate(
        [gain, shift, out_b[:, None], qv_b, down_b[:, None], up_b.reshape(TOWERS, ratio, share)],
        axis=1,
    ).reshape(TOWERS * COLS, share)
    columns = jnp.pad(columns, ((0, 128 - TOWERS * COLS), (0, 0))).astype(F32)
    lengths = jnp.concatenate([text_lengths, pair_lengths])

    vmem = pl.BlockSpec(memory_space=pltpu.VMEM)
    hbm = pl.BlockSpec(memory_space=pl.ANY)
    smem = pl.BlockSpec(memory_space=pltpu.SMEM)

    ins, specs = SimpleNamespace(), SimpleNamespace()
    ins.in_x, specs.in_x = turned, [hbm] * TOWERS
    ins.in_dy, specs.in_dy = turned_up, [hbm] * TOWERS
    ins.prm, specs.prm = columns, vmem
    ins.lengths, specs.lengths = lengths, smem
    ins.wqkv, specs.wqkv = wqkv, hbm
    ins.wout, specs.wout = out_w, hbm
    ins.wup, specs.wup = up_w, hbm
    ins.wdown, specs.wdown = down_w, hbm

    outs = SimpleNamespace()
    outs.o_y = [Out(vmem, x.shape, BF16) for x in turned]
    outs.o_dx = [Out(vmem, x.shape, BF16) for x in turned]
    if plan.fused:
        outs.o_qkv = Out(hbm, (TOWERS, 3, plan.slab, share))
        outs.o_out = Out(hbm, (TOWERS, share, plan.slab))
        outs.o_up = Out(hbm, (TOWERS, plan.slab, hidden))
        outs.o_down = Out(hbm, (TOWERS, plan.slab, hidden))
        outs.o_qvb = Out(vmem, (TOWERS, 2, share))
        outs.o_outb = Out(vmem, (TOWERS, share))
        outs.o_upb = Out(vmem, (TOWERS * ratio, share))
        outs.o_downb = Out(vmem, (TOWERS, share))
        outs.o_gain = Out(vmem, (TOWERS, 2, share))
        outs.o_bias = Out(vmem, (TOWERS, 2, share))
    else:
        outs.o_g = [Out(hbm, (TOWERS, width, n), BF16) for n in plan.grad_lanes]
        outs.o_small = Out(vmem, (share, 128))

    room = scratch(plan)
    in_refs, in_tree = flatten(vars(ins))
    out_refs, out_tree = flatten(vars(outs))
    room_refs, room_tree = flatten(vars(room))

    def body(*refs):
        first, second = len(in_refs), len(in_refs) + len(out_refs)
        r = SimpleNamespace()
        vars(r).update(jax.tree.unflatten(in_tree, refs[:first]))
        vars(r).update(jax.tree.unflatten(out_tree, refs[first:second]))
        vars(r).update(jax.tree.unflatten(room_tree, refs[second:]))
        kernel(plan, r)

    results = pl.pallas_call(
        body,
        out_shape=[jax.ShapeDtypeStruct(out.shape, out.dtype) for out in out_refs],
        in_specs=flatten(vars(specs))[0],
        out_specs=[out.spec for out in out_refs],
        scratch_shapes=room_refs,
        compiler_params=pltpu.CompilerParams(
            collective_id=1, has_side_effects=True, vmem_limit_bytes=67043328
        ),
        name="layer",
    )(*in_refs)
    got = SimpleNamespace(**jax.tree.unflatten(out_tree, results))

    if not plan.fused:
        sums_b, sums_c = [
            lax.psum_scatter(g.astype(F32), "dp", scatter_dimension=1, tiled=True)
            for g in got.o_g
        ]
        small = lax.psum(got.o_small, "dp").T[: TOWERS * COLS].reshape(TOWERS, COLS, share)
        got.o_up, got.o_down = sums_b[:, :, :hidden], sums_b[:, :, hidden:]
        slab = sums_c.shape[1]
        qkv = sums_c[:, :, : 3 * share].reshape(TOWERS, slab, 3, share)
        got.o_qkv = jnp.transpose(qkv, (0, 2, 1, 3))
        got.o_out = jnp.transpose(sums_c[:, :, 3 * share :], (0, 2, 1))
        got.o_qvb, got.o_outb = small[:, 0:2], small[:, 2]
        got.o_upb, got.o_downb = small[:, 3 : 3 + ratio], small[:, 7]
        got.o_gain, got.o_bias = small[:, 8:10], small[:, 10:12]

    return (
        *[jnp.transpose(y, (0, 2, 1)) for y in got.o_y],
        *[jnp.transpose(dx, (0, 2, 1)) for dx in got.o_dx],
        jnp.transpose(got.o_qkv, (0, 2, 1, 3)),
        got.o_qvb,
        got.o_out,
        got.o_outb,
        got.o_up,
        got.o_upb.reshape(TOWERS, hidden),
        jnp.transpose(got.o_down, (0, 2, 1)),
        got.o_downb,
        got.o_gain,
        got.o_bias,
    )


def solution(mesh):
    dp, tensor = mesh.shape["dp"], mesh.shape["tensor"]

    def step(*args):
        return per_device(dp, tensor, *args)

    rows = P("dp", None, "tensor")
    return jax.shard_map(
        step,
        mesh=mesh,
        in_specs=(
            rows,
            rows,
            rows,
            P("dp"),
            P("dp"),
            P(None, None, None, "tensor"),
            P(None, None, "tensor"),
            P(None, "tensor", None),
            P(None, "tensor"),
            P(None, None, "tensor"),
            P(None, "tensor"),
            P(None, "tensor", None),
            P(None, "tensor"),
            P(None, None, "tensor"),
            P(None, None, "tensor"),
            rows,
            rows,
            rows,
        ),
        out_specs=(
            rows,
            rows,
            rows,
            rows,
            rows,
            rows,
            P(None, "dp", None, "tensor"),
            P(None, None, "tensor"),
            P(None, "tensor", "dp"),
            P(None, "tensor"),
            P(None, "dp", "tensor"),
            P(None, "tensor"),
            P(None, "tensor", "dp"),
            P(None, "tensor"),
            P(None, None, "tensor"),
            P(None, None, "tensor"),
        ),
        check_vma=False,
    )
```

```python
from types import SimpleNamespace

import jax
import jax.numpy as jnp
from jax import lax
from jax.experimental import pallas as pl
from jax.experimental.pallas import tpu as pltpu
from jax.sharding import PartitionSpec as P

HEAD_DIM = 64
PATCHES = 196
EPSILON = 1e-06
TOWERS = 3
FIRST, SECOND = 0, 1
UP, DOWN, ATTN = 0, 1, 2
RING = 3
UNITS = (
    (0, DOWN),
    (0, UP),
    (1, DOWN),
    (1, UP),
    (0, ATTN),
    (2, DOWN),
    (2, UP),
    (1, ATTN),
    (2, ATTN),
)
TILE = 256
COLS = 12
N_REMOTE = 160
EARLY, LATE = 32, 8
SMALL = EARLY + LATE
LATE_COLS = (0, 1, 2, 8, 9, 10, 11)
BF16 = jnp.bfloat16
F32 = jnp.float32
MESH = pl.DeviceIdType.MESH
INV_SQRT2 = 0.7071067811865476
INV_SQRT_2PI = 0.3989422804014327


def nn(a, b):
    return lax.dot_general(a, b, (((1,), (0,)), ((), ())), preferred_element_type=F32)


def nt(a, b):
    return lax.dot_general(a, b, (((1,), (1,)), ((), ())), preferred_element_type=F32)


def up(value, multiple):
    return -(-value // multiple) * multiple


class Plan:
    def __init__(self, rows, weights, dp, tensor):
        qkv, out, upw = weights
        self.dp = dp
        self.examples = [r.shape[0] for r in rows]
        self.length = [r.shape[1] for r in rows]
        self.padded = [up(n, TILE) for n in self.length]
        self.lanes = [e * n for e, n in zip(self.examples, self.padded)]
        self.width = qkv.shape[1]
        self.share = out.shape[1]
        self.hidden = upw.shape[2]
        self.heads = self.share // HEAD_DIM
        self.pad = (3 * self.share) % TILE
        assert tensor == 4 and self.width == 4 * self.share
        assert self.pad + self.share == TILE and self.hidden == self.width
        self.fused = dp % 2 == 0 and dp > 1 and self.width % (16 * dp) == 0
        self.nz = dp // 2 if self.fused else 1
        self.slab = self.width // dp if self.fused else self.width
        self.halves = 2 if self.fused else 1


def small_row(t, j):
    if t < TOWERS - 1:
        return t * COLS + j
    if j in LATE_COLS:
        return EARLY + LATE_COLS.index(j)
    return t * COLS + [c for c in range(COLS) if c not in LATE_COLS].index(j)


class Out:
    def __init__(self, spec, shape, dtype=F32):
        self.spec, self.shape, self.dtype = spec, shape, dtype


def flatten(tree):
    return jax.tree.flatten(tree, is_leaf=lambda v: not isinstance(v, (dict, list)))


def scratch(plan):
    width, share, hidden, nz = plan.width, plan.share, plan.hidden, plan.nz
    half, most = width // 2, max(plan.lanes)
    dma = pltpu.SemaphoreType.DMA

    def vm(*shape, dtype=BF16):
        return pltpu.VMEM(shape, dtype)

    def each(*lead, dtype=BF16):
        return [pltpu.VMEM((*lead, lanes), dtype) for lanes in plan.lanes]

    k = SimpleNamespace()
    k.x, k.dy, k.n = each(width), each(width), each(width)
    k.sums = [each(width), each(width)]
    k.part, k.rpart = each(width), each(width)
    k.qkv, k.m = each(3 * share), each(TILE)
    k.p = [vm(e * plan.heads, n, n) for e, n in zip(plan.examples, plan.padded)]
    k.near, k.far = each(half), [each(half), each(half)]
    k.rnear, k.rfar = each(2, share), [each(share), each(share)]
    k.own, k.row = each(share, dtype=F32), each(8, dtype=F32)
    k.stat_own, k.stat_near = each(8, dtype=F32), each(8, dtype=F32)
    k.stat_chip, k.stat_far = each(8, dtype=F32), each(8, dtype=F32)
    k.g_all = vm(RING, plan.halves, nz, plan.slab, width)
    k.credit = pltpu.SemaphoreType.REGULAR((RING,))
    k.out_sem = dma((4,))
    if plan.fused:
        k.g_y = vm(RING, nz, plan.slab, width)
        k.g_z = vm(RING, nz, plan.slab, width)
        k.g_far = vm(len(UNITS), max(nz - 1, 1), plan.slab, width)
        k.s_ffn = vm(2, plan.slab, hidden, dtype=F32)
        k.s_qkv = vm(3, plan.slab, share, dtype=F32)
        k.s_out = vm(share, plan.slab, dtype=F32)
        k.rows = [vm(n, share, dtype=F32) for n in (EARLY, LATE)]
        k.rows_y = [vm(n, share, dtype=F32) for n in (EARLY, LATE)]
        k.rows_z = [vm(nz, n, share, dtype=F32) for n in (EARLY, LATE)]
    k.wqkv_v, k.wout_v = vm(2, 3 * share, width), vm(2, share, width)
    k.wup_v, k.wdown_v = vm(width, hidden), vm(hidden, width)
    k.up_t, k.down_t = vm(hidden, width), vm(width, hidden)
    k.work_n, k.work_a = vm(width, most), vm(hidden, most)
    k.work_h, k.work_m = vm(width, most), vm(share, most)
    k.pown, k.pfull = vm(share, 128, dtype=F32), vm(width, 128)
    k.prm, k.small = vm(128, share, dtype=F32), vm(share, 128, dtype=F32)
    k.in_sem, k.w_sem, k.part_sem = dma((2 * TOWERS,)), dma((18,)), dma(())
    k.send_sem, k.recv_sem = dma((N_REMOTE,)), dma((N_REMOTE,))
    return k


def kernel(plan, r):
    width, share, hidden, heads = plan.width, plan.share, plan.hidden, plan.heads
    half = width // 2
    nz = plan.nz

    dp_at = lax.axis_index("dp")
    me = lax.axis_index("tensor")
    core = lax.rem(me, 2)
    chip = lax.div(me, 2)
    y_at = lax.rem(dp_at, 2)
    z_at = lax.div(dp_at, 2)
    sibling = (dp_at, me + 1 - 2 * core)
    across = (dp_at, lax.rem(me + 2, 4))
    y_peer = (dp_at + 1 - 2 * y_at, me)

    def z_index(k):
        return lax.rem(z_at + k, nz)

    def z_peer(k):
        return (z_index(k) * 2 + y_at, me)

    counter = [0]
    pending = []

    def remote(src, dst, device):
        at = counter[0]
        counter[0] += 1
        assert at < N_REMOTE
        return pltpu.make_async_remote_copy(
            src_ref=src,
            dst_ref=dst,
            send_sem=r.send_sem.at[at],
            recv_sem=r.recv_sem.at[at],
            device_id=device,
            device_id_type=MESH,
        )

    def launch(copy):
        copy.start()
        pending.append(copy)
        return copy

    def sent(copy):
        copy.wait_send()
        pending[:] = [other for other in pending if other is not copy]

    def block(at, size):
        return pl.ds(pl.multiple_of(at * size, size), size)

    own = block(me, share)
    my_half, other_half = block(core, half), block(1 - core, half)

    def lanes_loop(lanes, tile, body):
        def step(at, carry):
            body(block(at, tile))
            return carry

        lax.fori_loop(0, lanes // tile, step, 0)

    lane_of_small = lax.broadcasted_iota(jnp.int32, (share, 128), 1)

    def keep_sum(t, j, value):
        column = jnp.sum(value.astype(F32), axis=1, keepdims=True)
        small = r.small
        small[...] = jnp.where(lane_of_small == small_row(t, j), column, small[...])

    def own_col(t, j):
        return r.pown[:, t * COLS + j : t * COLS + j + 1]

    def full_col(t, j):
        return r.pfull[...].astype(F32)[:, t * COLS + j : t * COLS + j + 1]

    class Gather:
        def __init__(self, buf):
            self.to_sibling = remote(buf.at[own], buf.at[own], sibling)
            self.to_across = remote(buf.at[own], buf.at[own], across)
            blk = block(lax.rem(me + 2, 4), share)
            self.forwarded = remote(buf.at[blk], buf.at[blk], sibling)

        def start(self):
            launch(self.to_across)
            launch(self.to_sibling)

        def forward(self):
            self.to_across.wait_recv()
            launch(self.forwarded)

        def finish(self):
            self.to_sibling.wait_recv()
            self.forwarded.wait_recv()

    class AllReduce:
        def __init__(self, t, which):
            self.part, self.near = r.part[t], r.near[t]
            self.far, self.out = r.far[which][t], r.sums[which][t]
            self.c1 = remote(self.part.at[other_half], self.near, sibling)
            self.c2 = remote(self.part.at[my_half], self.far, across)
            self.c3 = remote(self.out.at[my_half], self.out.at[my_half], sibling)

        def begin(self):
            launch(self.c1)

        def cross(self):
            self.c1.wait_recv()
            total = self.part[my_half].astype(F32) + self.near[...].astype(F32)
            self.part[my_half] = total.astype(BF16)
            launch(self.c2)

        def back(self):
            self.c2.wait_recv()
            total = self.part[my_half].astype(F32) + self.far[...].astype(F32)
            self.out[my_half] = total.astype(BF16)
            launch(self.c3)

        def finish(self):
            self.c3.wait_recv()

        def free(self):
            sent(self.c1)
            sent(self.c2)
            sent(self.c3)

    class Scatter:
        def __init__(self, t, which):
            self.part, self.near, self.far = r.rpart[t], r.rnear[t], r.rfar[which][t]
            self.far_blk = block(2 * (1 - chip) + core, share)
            theirs = (2 * (1 - chip) + 1 - core, 2 * chip + 1 - core)
            self.c1 = [
                remote(self.part.at[block(theirs[j], share)], self.near.at[j], sibling)
                for j in range(2)
            ]
            self.c2 = remote(self.part.at[self.far_blk], self.far, across)

        def begin(self):
            for copy in self.c1:
                launch(copy)

        def cross(self):
            self.c1[0].wait_recv()
            blk = self.far_blk
            self.part[blk] = (self.part[blk].astype(F32) + self.near[0].astype(F32)).astype(BF16)
            launch(self.c2)
            self.c1[1].wait_recv()
            self.part[own] = (self.part[own].astype(F32) + self.near[1].astype(F32)).astype(BF16)

        def finish(self):
            self.c2.wait_recv()

        def free(self):
            for copy in self.c1:
                sent(copy)
            sent(self.c2)

    class Stats:
        def __init__(self, t):
            self.c1 = remote(r.stat_own[t], r.stat_near[t], sibling)
            self.c2 = remote(r.stat_chip[t], r.stat_far[t], across)
            self.t = t

        def begin(self):
            launch(self.c1)

        def cross(self):
            t = self.t
            self.c1.wait_recv()
            r.stat_chip[t][...] = r.stat_own[t][...] + r.stat_near[t][...]
            launch(self.c2)

        def finish(self):
            self.c2.wait_recv()

    class Unit:
        def __init__(self, at, t, kind):
            self.at, self.t, self.kind = at, t, kind
            self.slot = at % RING
            self.all = r.g_all.at[self.slot]
            self.y_copies, self.z_copies, self.hbm = [], [], []

        def send(self):
            if not plan.fused:
                dst = r.o_g.at[self.kind, self.t]
                copy = pltpu.make_async_copy(self.all.at[0, 0], dst, r.part_sem)
                copy.start()
                copy.wait()
                return
            if self.at >= RING:
                pl.semaphore_wait(r.credit.at[self.slot], 1)
            for j in range(nz):
                at = z_index(1 + j)
                src, dst = self.all.at[1 - y_at, at], r.g_y.at[self.slot, at]
                self.y_copies.append(launch(remote(src, dst, y_peer)))

        def relay(self, quarter):
            if plan.fused:
                for j in range(nz * quarter // 4, nz * (quarter + 1) // 4):
                    self.relay_piece(j)

        def relay_piece(self, j):
            if j == 0 and self.at >= RING:
                for copy in units[self.at - RING].z_copies:
                    sent(copy)
            at = z_index(1 + j)
            sums = r.g_z.at[self.slot, at]
            self.y_copies[j].wait_recv()
            total = self.all[y_at, at].astype(F32) + r.g_y[self.slot, at].astype(F32)
            sums[...] = total.astype(BF16)
            if j < nz - 1:
                dst = r.g_far.at[self.at, j]
                self.z_copies.append(launch(remote(sums, dst, z_peer(1 + j))))
                return
            for copy in self.y_copies:
                sent(copy)
            if self.at + RING < len(units):
                credit = r.credit.at[self.slot]
                pl.semaphore_signal(credit, inc=1, device_id=y_peer, device_id_type=MESH)

        def finish(self):
            if not plan.fused:
                return
            total = r.g_z[self.slot, z_at].astype(F32)
            for j in range(nz - 1):
                self.z_copies[j].wait_recv()
                total = total + r.g_far[self.at, j].astype(F32)
            t, sem = self.t, r.out_sem
            for before in units[: self.at]:
                if before.kind == self.kind:
                    for copy in before.hbm:
                        copy.wait()
                    before.hbm = []
            if self.kind == UP or self.kind == DOWN:
                out = r.o_up if self.kind == UP else r.o_down
                r.s_ffn[self.kind] = total
                self.hbm = [pltpu.make_async_copy(r.s_ffn.at[self.kind], out.at[t], sem.at[self.kind])]
            else:
                for c in range(3):
                    r.s_qkv[c] = total[:, c * share : (c + 1) * share]
                r.s_out[...] = total[:, 3 * share :].T
                self.hbm = [
                    pltpu.make_async_copy(r.s_qkv, r.o_qkv.at[t], sem.at[2]),
                    pltpu.make_async_copy(r.s_out, r.o_out.at[t], sem.at[3]),
                ]
            for copy in self.hbm:
                copy.start()

    gx = [Gather(r.x[t]) for t in range(TOWERS)]
    gdy = [Gather(r.dy[t]) for t in range(TOWERS)]
    gp = Gather(r.pfull)
    ar1 = [AllReduce(t, FIRST) for t in range(TOWERS)]
    ar2 = [AllReduce(t, SECOND) for t in range(TOWERS)]
    rs1 = [Scatter(t, FIRST) for t in range(TOWERS)]
    rs2 = [Scatter(t, SECOND) for t in range(TOWERS)]
    stats = [Stats(t) for t in range(TOWERS)]
    units = []
    for at, (t, kind) in enumerate(UNITS):
        units.append(Unit(at, t, kind))
    unit_of = {(unit.t, unit.kind): unit for unit in units}

    def attn_load(use):
        t, slot = use % TOWERS, use % 2
        pairs = ((r.wqkv, r.wqkv_v), (r.wout, r.wout_v))
        return [
            pltpu.make_async_copy(src.at[t], dst.at[slot], r.w_sem.at[6 + 2 * use + i])
            for i, (src, dst) in enumerate(pairs)
        ]

    attn_w = [attn_load(use) for use in range(2 * TOWERS)]
    ffn_w = [
        [
            pltpu.make_async_copy(r.wup.at[t], r.wup_v, r.w_sem.at[2 * t]),
            pltpu.make_async_copy(r.wdown.at[t], r.wdown_v, r.w_sem.at[2 * t + 1]),
        ]
        for t in range(TOWERS)
    ]

    def transpose_into(dst, src, rows, cols):
        for at in range(0, rows, TILE):
            size = min(TILE, rows - at)
            dst[:cols, at : at + size] = src[at : at + size, :].T

    def stage_in(ref, t, source):
        length, padded = plan.length[t], plan.padded[t]
        for e in range(plan.examples[t]):
            base = e * padded
            if length < padded:
                first = length // 128 * 128
                ref[own, base + first : base + padded] = jnp.zeros((share, padded - first), BF16)
            ref[own, base : base + length] = source[e]

    def param_rows():
        prm = r.prm
        prm[...] = jnp.zeros_like(prm)
        up_bias = r.in_up_b[...].astype(F32)
        for t in range(TOWERS):
            base = t * COLS
            for j in range(2):
                prm[base + j, :] = r.in_gain[t, j, :].astype(F32)
                prm[base + 2 + j, :] = r.in_shift[t, j, :].astype(F32)
                prm[base + 5 + j, :] = r.in_qv_b[t, j, :].astype(F32)
            prm[base + 4, :] = r.in_out_b[t, :].astype(F32)
            prm[base + 7, :] = r.in_down_b[t, :].astype(F32)
            for j in range(hidden // share):
                prm[base + 8 + j, :] = up_bias[t, j * share : (j + 1) * share]
        r.pown[...] = prm[...].T
        r.pfull[own] = r.pown[...].astype(BF16)

    def a_norm(t):
        gain, shift = full_col(t, 0), full_col(t, 2)

        def body(ls):
            x = r.x[t][:, ls].astype(F32)
            mean = jnp.sum(x, axis=0, keepdims=True) / width
            center = x - mean
            inv = lax.rsqrt(jnp.sum(center * center, axis=0, keepdims=True) / width + EPSILON)
            r.n[t][:, ls] = (center * inv * gain + shift).astype(BF16)
            r.row[t][0:1, ls] = mean
            r.row[t][1:2, ls] = inv

        lanes_loop(plan.lanes[t], 128, body)

    def a_qkv(t):
        for copy in attn_w[t]:
            copy.wait()
        bias = jnp.concatenate(
            [own_col(t, 5), jnp.zeros((share, 1), F32), own_col(t, 6)], axis=0
        )

        def body(ls):
            value = nn(r.wqkv_v[t % 2], r.n[t][:, ls]) + bias
            r.qkv[t][:, ls] = value.astype(BF16)

        lanes_loop(plan.lanes[t], TILE, body)

    def valid_keys(t, e):
        if t == 0:
            return plan.length[0]
        if t == 1:
            return r.in_text[e]
        return r.in_pair[e] + (PATCHES + 1)

    def a_heads(t):
        padded = plan.padded[t]
        key_at = lax.broadcasted_iota(jnp.int32, (padded, 1), 0)
        qkv = r.qkv[t]
        r.m[t][: plan.pad] = jnp.zeros((plan.pad, plan.lanes[t]), BF16)
        for e in range(plan.examples[t]):
            base = e * padded
            valid = key_at < valid_keys(t, e)

            def head(h, carry):
                rows_q = block(h, HEAD_DIM)
                rows_k = block(h + heads, HEAD_DIM)
                rows_v = block(h + 2 * heads, HEAD_DIM)
                rows_m = block(h + plan.pad // HEAD_DIM, HEAD_DIM)
                keys = qkv[rows_k, base : base + padded].T
                values = qkv[rows_v, base : base + padded]
                for q in range(padded // TILE):
                    at = base + q * TILE
                    s = nn(keys, qkv[rows_q, at : at + TILE]) * (HEAD_DIM**-0.5)
                    s = jnp.where(valid, s, -1000000000.0)
                    p = jnp.exp(s - jnp.max(s, axis=0, keepdims=True))
                    p = (p * (1.0 / jnp.sum(p, axis=0, keepdims=True))).astype(BF16)
                    r.p[t][e * heads + h, :, q * TILE : (q + 1) * TILE] = p
                    r.m[t][rows_m, at : at + TILE] = nn(values, p).astype(BF16)
                return carry

            lax.fori_loop(0, heads, head, 0)

    def a_out(t):
        transpose_into(r.work_a, r.wout_v.at[t % 2], share, width)

        def body(ls):
            mixed = r.m[t][plan.pad :, ls]
            r.part[t][:, ls] = nn(r.work_a[:, :share], mixed).astype(BF16)

        lanes_loop(plan.lanes[t], TILE, body)
        ar1[t].begin()
        for copy in attn_w[t + 2]:
            copy.start()

    def b_prep(t):
        for copy in ffn_w[t]:
            copy.wait()
        transpose_into(r.up_t, r.wup_v, width, hidden)
        transpose_into(r.down_t, r.wdown_v, hidden, width)

    def b_main(t):
        out_bias, gain, shift = full_col(t, 4), full_col(t, 1), full_col(t, 3)
        up_bias = jnp.concatenate([own_col(t, 8 + j) for j in range(hidden // share)], axis=0)
        ar1[t].free()

        def body(ls):
            x, s = r.x[t], r.sums[FIRST][t]
            resid = x[:, ls].astype(F32) + (s[:, ls].astype(F32) + out_bias)
            r.own[t][:, ls] = x[own, ls].astype(F32) + (s[own, ls].astype(F32) + own_col(t, 4))
            mean = jnp.sum(resid, axis=0, keepdims=True) / width
            center = resid - mean
            inv = lax.rsqrt(jnp.sum(center * center, axis=0, keepdims=True) / width + EPSILON)
            xhat = center * inv
            r.row[t][2:3, ls] = inv
            normed = (xhat * gain + shift).astype(BF16)
            s[:, ls] = xhat.astype(BF16)
            r.work_n[:, ls] = normed
            h = nn(r.up_t[...], normed) + up_bias
            cdf = 0.5 * (1.0 + lax.erf(h * INV_SQRT2))
            r.work_a[:, ls] = (h * cdf).astype(BF16)
            slope = cdf + h * (jnp.exp(-0.5 * (h * h)) * INV_SQRT_2PI)
            dact = nn(r.wdown_v[...], r.dy[t][:, ls])
            dhid = (dact * slope).astype(BF16)
            r.work_h[:hidden, ls] = dhid
            r.part[t][:, ls] = nn(r.wup_v[...], dhid).astype(BF16)

        lanes_loop(plan.lanes[t], TILE, body)
        ar2[t].begin()
        if t + 1 < TOWERS:
            for copy in ffn_w[t + 1]:
                copy.start()

    def b_ffn(t):
        def body(ls):
            r.rpart[t][:, ls] = nn(r.down_t[...], r.work_a[:, ls]).astype(BF16)

        lanes_loop(plan.lanes[t], TILE, body)
        rs1[t].begin()

    def spread(dst, value, ls):
        for b in range(plan.halves * nz):
            part = value[b * plan.slab : (b + 1) * plan.slab].astype(BF16)
            dst[b % plan.halves, b // plan.halves, :, ls] = part

    def grad_loop(unit, lhs, rhs):
        dst = unit.all

        def step(at, carry):
            rows = block(at, TILE)
            spread(dst, nt(lhs(), rhs(rows)), rows)
            return carry

        lax.fori_loop(0, hidden // TILE, step, 0)
        unit.send()

    def b_up(t):
        lanes = plan.lanes[t]
        grad_loop(
            unit_of[t, UP], lambda: r.work_n[:, :lanes], lambda rows: r.work_h[rows, :lanes]
        )

    def b_down(t):
        lanes = plan.lanes[t]
        grad_loop(unit_of[t, DOWN], lambda: r.dy[t][...], lambda rows: r.work_a[rows, :lanes])

    def b_sum(t):
        lanes = plan.lanes[t]
        for j in range(hidden // share):
            keep_sum(t, 3 + j, r.work_h[j * share : (j + 1) * share, :lanes])
        keep_sum(t, 7, r.dy[t][own])

    def y_out(t):
        rs1[t].finish()
        value = r.own[t][...] + (
            r.rpart[t][own].astype(F32) + r.rfar[FIRST][t][...].astype(F32) + own_col(t, 7)
        )
        padded = plan.padded[t]
        for e in range(plan.examples[t]):
            out = value[:, e * padded : e * padded + plan.length[t]]
            r.o_y[t][e] = out.astype(BF16)

    def c_norm(t):
        for copy in attn_w[TOWERS + t]:
            copy.wait()
        slot = (TOWERS + t) % 2
        gain, gain_own = full_col(t, 1), own_col(t, 1)

        def body(ls):
            dn, xhat = r.sums[SECOND][t], r.sums[FIRST][t]
            xh = xhat[:, ls].astype(F32)
            e = dn[:, ls].astype(F32) * gain
            m1 = jnp.sum(e, axis=0, keepdims=True) / width
            m2 = jnp.sum(e * xh, axis=0, keepdims=True) / width
            inv = r.row[t][2:3, ls]
            dres = r.dy[t][:, ls].astype(F32) + inv * (e - m1 - xh * m2)
            r.work_n[:, ls] = dres.astype(BF16)
            e_own = dn[own, ls].astype(F32) * gain_own
            r.own[t][:, ls] = r.dy[t][own, ls].astype(F32) + inv * (
                e_own - m1 - xhat[own, ls].astype(F32) * m2
            )

        lanes_loop(plan.lanes[t], 128, body)

        def mix(ls):
            r.work_m[:, ls] = nn(r.wout_v[slot], r.work_n[:, ls]).astype(BF16)

        lanes_loop(plan.lanes[t], TILE, mix)

    def c_heads(t):
        padded = plan.padded[t]
        qkv = r.qkv[t]
        scale = HEAD_DIM**-0.5
        for e in range(plan.examples[t]):
            base = e * padded

            def head(h, carry):
                rows_q = block(h, HEAD_DIM)
                rows_k = block(h + heads, HEAD_DIM)
                rows_v = block(h + 2 * heads, HEAD_DIM)
                keys = qkv[rows_k, base : base + padded]
                values = qkv[rows_v, base : base + padded].T
                dk = dv = None
                for q in range(padded // TILE):
                    at = base + q * TILE
                    dm = r.work_m[rows_q, at : at + TILE]
                    p = r.p[t][e * heads + h, :, q * TILE : (q + 1) * TILE]
                    dp = nn(values, dm)
                    pf = p.astype(F32)
                    delta = jnp.sum(pf * dp, axis=0, keepdims=True)
                    ds = (pf * (dp - delta)).astype(BF16)
                    dq = nn(keys, ds) * scale
                    r.work_h[rows_q, at : at + TILE] = dq.astype(BF16)
                    dk_q = nt(qkv[rows_q, at : at + TILE], ds)
                    dv_q = nt(dm, p)
                    dk = dk_q if dk is None else dk + dk_q
                    dv = dv_q if dv is None else dv + dv_q
                r.work_h[rows_k, base : base + padded] = (dk * scale).astype(BF16)
                r.work_h[rows_v, base : base + padded] = dv.astype(BF16)
                return carry

            lax.fori_loop(0, heads, head, 0)

    def c_prep(t):
        transpose_into(r.up_t, r.wqkv_v.at[(TOWERS + t) % 2], 3 * share, width)

    def c_dn(t):
        gain = full_col(t, 0)
        rs1[t].free()
        r.stat_own[t][...] = jnp.zeros_like(r.stat_own[t])

        def body(ls):
            dn = nn(r.up_t[:, : 3 * share], r.work_h[: 3 * share, ls])
            e = dn * gain
            xhat = (r.x[t][:, ls].astype(F32) - r.row[t][0:1, ls]) * r.row[t][1:2, ls]
            r.stat_own[t][0:1, ls] = jnp.sum(e, axis=0, keepdims=True)
            r.stat_own[t][1:2, ls] = jnp.sum(e * xhat, axis=0, keepdims=True)
            r.rpart[t][:, ls] = dn.astype(BF16)

        lanes_loop(plan.lanes[t], TILE, body)
        rs2[t].begin()
        stats[t].begin()
        if t == 0:
            for copy in attn_w[5]:
                copy.start()

    def c_grad(t):
        lanes = plan.lanes[t]
        unit = unit_of[t, ATTN]
        r.work_h[3 * share :, :lanes] = jnp.zeros((width - 3 * share, lanes), BF16)
        whole = 3 * share // TILE

        def step(at, carry):
            rows = block(at, TILE)
            spread(unit.all, nt(r.n[t][...], r.work_h[rows, :lanes]), rows)
            return carry

        lax.fori_loop(0, whole, step, 0)
        last = slice(whole * TILE, (whole + 1) * TILE)
        value = nt(r.n[t][...], r.work_h[last, :lanes])
        value = value + nt(r.work_n[:, :lanes], r.m[t][...])
        spread(unit.all, value, last)
        unit.send()

    def c_sum(t):
        lanes = plan.lanes[t]
        keep_sum(t, 0, r.work_h[:share, :lanes])
        keep_sum(t, 1, r.work_h[2 * share : 3 * share, :lanes])
        keep_sum(t, 2, r.work_n[own, :lanes])
        dn, xhat = r.sums[SECOND][t], r.sums[FIRST][t]
        keep_sum(t, 9, dn[own].astype(F32) * xhat[own].astype(F32))
        keep_sum(t, 11, dn[own])

    def last_norm(t):
        rs2[t].finish()
        stats[t].finish()
        gain = own_col(t, 0)
        dn = r.rpart[t][own].astype(F32) + r.rfar[SECOND][t][...].astype(F32)
        total = r.stat_chip[t][...] + r.stat_far[t][...]
        inv = r.row[t][1:2, :]
        xhat = (r.x[t][own].astype(F32) - r.row[t][0:1, :]) * inv
        value = r.own[t][...] + inv * (
            dn * gain - total[0:1] / width - xhat * (total[1:2] / width)
        )
        padded = plan.padded[t]
        for e in range(plan.examples[t]):
            out = value[:, e * padded : e * padded + plan.length[t]]
            r.o_dx[t][e] = out.astype(BF16)
        keep_sum(t, 8, dn * xhat)
        keep_sum(t, 10, dn)

    def small_send(late):
        rows = r.small[...].T
        first, last = (EARLY, EARLY + LATE) if late else (0, EARLY)
        part = rows[first:last]
        if not plan.fused:
            r.o_rows[first:last] = part
            return
        r.rows[late][...] = part
        small_y[late] = launch(remote(r.rows[late], r.rows_y[late], y_peer))

    def small_relay(late):
        if not plan.fused:
            return
        small_y[late].wait_recv()
        r.rows_z[late][z_at] = r.rows[late][...] + r.rows_y[late][...]
        for k in range(1, nz):
            slot = r.rows_z[late].at[z_at]
            small_z[late].append(launch(remote(slot, slot, z_peer(k))))

    def small_finish(late):
        if not plan.fused:
            return
        for copy in small_z[late]:
            copy.wait_recv()
        total = r.rows_z[late][0]
        for k in range(1, nz):
            total = total + r.rows_z[late][k]
        if late:
            r.o_rows[EARLY : EARLY + LATE] = total
        else:
            r.o_rows[:EARLY] = total

    small_y, small_z = [None, None], [[], []]

    barrier = pltpu.get_barrier_semaphore()
    partners = [sibling, across]
    if plan.fused:
        partners += [y_peer] + [z_peer(k) for k in range(1, nz)]
    for device in partners:
        pl.semaphore_signal(barrier, inc=1, device_id=device, device_id_type=MESH)
    loads = [
        pltpu.make_async_copy(src[t], dst[t], r.in_sem.at[i * TOWERS + t])
        for i, (src, dst) in enumerate(((r.in_x, r.o_y), (r.in_dy, r.o_dx)))
        for t in range(TOWERS)
    ]
    for copy in loads + attn_w[0] + ffn_w[0] + attn_w[1]:
        copy.start()
    param_rows()
    loads[0].wait()
    stage_in(r.x[0], 0, r.o_y[0])
    pl.semaphore_wait(barrier, len(partners))
    gp.start()
    gx[0].start()
    for t in range(1, TOWERS):
        loads[t].wait()
        stage_in(r.x[t], t, r.o_y[t])
    for t in range(TOWERS):
        loads[TOWERS + t].wait()
        stage_in(r.dy[t], t, r.o_dx[t])
    r.small[...] = jnp.zeros_like(r.small)
    gp.forward()
    gx[1].start()
    gp.finish()
    gdy[0].start()
    b_prep(0)
    gx[0].forward()
    gx[0].finish()
    a_norm(0)
    a_qkv(0)
    a_heads(0)
    a_out(0)
    ar1[0].cross()
    gdy[0].forward()
    gx[1].forward()
    gx[1].finish()
    a_norm(1)
    a_qkv(1)
    a_heads(1)
    a_out(1)
    gdy[0].finish()
    gx[2].start()
    gdy[1].start()
    gdy[2].start()
    ar1[1].cross()
    ar1[0].back()
    ar1[0].finish()
    b_main(0)
    gx[2].forward()
    b_down(0)
    b_up(0)
    b_ffn(0)
    b_prep(1)
    units[0].relay(0)
    gdy[1].forward()
    gdy[1].finish()
    b_sum(0)
    rs1[0].cross()
    gx[2].finish()
    a_norm(2)
    a_qkv(2)
    gdy[2].forward()
    gdy[2].finish()
    ar2[0].cross()
    units[0].relay(1)
    units[0].relay(2)
    a_heads(2)
    units[0].relay(3)
    units[1].relay(0)
    ar1[1].back()
    ar1[1].finish()
    units[1].relay(1)
    b_main(1)
    b_down(1)
    units[1].relay(2)
    b_up(1)
    b_ffn(1)
    y_out(0)
    b_sum(1)
    units[0].finish()
    a_out(2)
    units[1].relay(3)
    units[2].relay(0)
    rs1[1].cross()
    ar1[2].cross()
    ar2[0].back()
    ar2[0].finish()
    units[2].relay(1)
    c_norm(0)
    c_heads(0)
    c_sum(0)
    units[2].relay(2)
    units[2].relay(3)
    c_prep(0)
    c_grad(0)
    units[3].relay(0)
    units[1].finish()
    ar2[1].cross()
    y_out(1)
    c_dn(0)
    units[3].relay(1)
    units[2].finish()
    b_prep(2)
    rs2[0].cross()
    units[3].relay(2)
    stats[0].cross()
    ar1[2].back()
    ar1[2].finish()
    b_main(2)
    units[3].relay(3)
    units[4].relay(0)
    units[4].relay(1)
    b_down(2)
    units[3].finish()
    units[4].relay(2)
    b_sum(2)
    b_ffn(2)
    units[4].relay(3)
    last_norm(0)
    ar2[1].back()
    ar2[1].finish()
    units[5].relay(0)
    ar2[2].cross()
    b_up(2)
    units[4].finish()
    units[5].relay(1)
    rs1[2].cross()
    c_norm(1)
    units[5].relay(2)
    c_prep(1)
    c_heads(1)
    c_grad(1)
    units[5].relay(3)
    units[6].relay(0)
    ar2[2].back()
    ar2[2].finish()
    c_sum(1)
    c_dn(1)
    rs2[1].cross()
    stats[1].cross()
    units[6].relay(1)
    units[6].relay(2)
    units[5].finish()
    y_out(2)
    units[6].relay(3)
    c_norm(2)
    units[7].relay(0)
    last_norm(1)
    small_send(0)
    c_heads(2)
    small_relay(0)
    units[7].relay(1)
    c_grad(2)
    c_prep(2)
    units[6].finish()
    units[7].relay(2)
    units[7].relay(3)
    c_sum(2)
    c_dn(2)
    rs2[2].cross()
    stats[2].cross()
    units[8].relay(0)
    units[8].relay(1)
    units[7].finish()
    units[8].relay(2)
    last_norm(2)
    small_send(1)
    units[8].relay(3)
    small_relay(1)
    small_finish(0)
    units[8].finish()
    small_finish(1)
    for copy in list(pending):
        sent(copy)
    for unit in units:
        for copy in unit.hbm:
            copy.wait()


def deliver(*refs):
    count = 2 * TOWERS + 4
    src, rows = refs[:count], refs[count]
    dst = refs[count + 1 : 2 * count + 1]
    qvb, outb, upb, downb, gains, shifts = refs[2 * count + 1 : 2 * count + 7]
    room = refs[2 * count + 7 : 3 * count + 7]
    in_sem, out_sem = refs[3 * count + 7 :]
    reads = [pltpu.make_async_copy(src[i], room[i], in_sem.at[i]) for i in range(count)]
    writes = [pltpu.make_async_copy(room[i], dst[i], out_sem.at[i]) for i in range(count)]
    for copy in reads:
        copy.start()
    share = rows.shape[1]
    for t in range(TOWERS):
        for j in range(2):
            qvb[t, j, :] = rows[small_row(t, j), :]
            gains[t, j, :] = rows[small_row(t, 8 + j), :]
            shifts[t, j, :] = rows[small_row(t, 10 + j), :]
        outb[t, :] = rows[small_row(t, 2), :]
        downb[t, :] = rows[small_row(t, 7), :]
        for j in range(upb.shape[1] // share):
            upb[t, j * share : (j + 1) * share] = rows[small_row(t, 3 + j), :]
    for read, write in zip(reads, writes):
        read.wait()
        write.start()
    for copy in writes:
        copy.wait()


def per_device(dp, tensor, *args):
    rows, ups = args[0:3], args[15:18]
    text_lengths, pair_lengths = args[3:5]
    qkv_w, qv_b, out_w, out_b, up_w, up_b, down_w, down_b, gain, shift = args[5:15]
    plan = Plan(rows, (qkv_w, out_w, up_w), dp, tensor)
    width, share, hidden = plan.width, plan.share, plan.hidden
    nz = plan.nz

    turned = [jnp.transpose(x, (0, 2, 1)) for x in rows]
    turned_up = [jnp.transpose(x, (0, 2, 1)) for x in ups]
    wqkv = jnp.transpose(qkv_w, (0, 2, 3, 1)).reshape(TOWERS, 3 * share, width)
    vmem = pl.BlockSpec(memory_space=pltpu.VMEM)
    hbm = pl.BlockSpec(memory_space=pl.ANY)
    smem = pl.BlockSpec(memory_space=pltpu.SMEM)

    ins, specs = SimpleNamespace(), SimpleNamespace()
    ins.in_x, specs.in_x = turned, [hbm] * TOWERS
    ins.in_dy, specs.in_dy = turned_up, [hbm] * TOWERS
    ins.in_text, specs.in_text = text_lengths, smem
    ins.in_pair, specs.in_pair = pair_lengths, smem
    ins.in_gain, specs.in_gain = gain, vmem
    ins.in_shift, specs.in_shift = shift, vmem
    ins.in_out_b, specs.in_out_b = out_b, vmem
    ins.in_qv_b, specs.in_qv_b = qv_b, vmem
    ins.in_down_b, specs.in_down_b = down_b, vmem
    ins.in_up_b, specs.in_up_b = up_b, vmem
    ins.wqkv, specs.wqkv = wqkv, hbm
    ins.wout, specs.wout = out_w, hbm
    ins.wup, specs.wup = up_w, hbm
    ins.wdown, specs.wdown = down_w, hbm

    outs = SimpleNamespace()
    outs.o_y = [Out(vmem, x.shape, BF16) for x in turned]
    outs.o_dx = [Out(vmem, x.shape, BF16) for x in turned]
    if plan.fused:
        outs.o_qkv = Out(hbm, (TOWERS, 3, plan.slab, share))
        outs.o_out = Out(hbm, (TOWERS, share, plan.slab))
        outs.o_up = Out(hbm, (TOWERS, plan.slab, hidden))
        outs.o_down = Out(hbm, (TOWERS, plan.slab, hidden))
    else:
        outs.o_g = Out(hbm, (3, TOWERS, width, width), BF16)
    outs.o_rows = Out(vmem, (SMALL, share))

    room = scratch(plan)
    in_refs, in_tree = flatten(vars(ins))
    out_refs, out_tree = flatten(vars(outs))
    room_refs, room_tree = flatten(vars(room))

    def body(*refs):
        first, second = len(in_refs), len(in_refs) + len(out_refs)
        r = SimpleNamespace()
        vars(r).update(jax.tree.unflatten(in_tree, refs[:first]))
        vars(r).update(jax.tree.unflatten(out_tree, refs[first:second]))
        vars(r).update(jax.tree.unflatten(room_tree, refs[second:]))
        kernel(plan, r)

    results = pl.pallas_call(
        body,
        out_shape=[jax.ShapeDtypeStruct(out.shape, out.dtype) for out in out_refs],
        in_specs=flatten(vars(specs))[0],
        out_specs=[out.spec for out in out_refs],
        scratch_shapes=room_refs,
        compiler_params=pltpu.CompilerParams(
            collective_id=1, has_side_effects=True, vmem_limit_bytes=67043328
        ),
        name="layer",
    )(*in_refs)
    got = SimpleNamespace(**jax.tree.unflatten(out_tree, results))

    if not plan.fused:
        sums = lax.psum_scatter(got.o_g.astype(F32), "dp", scatter_dimension=2, tiled=True)
        got.o_up, got.o_down = sums[UP], sums[DOWN]
        qkv = sums[ATTN, :, :, : 3 * share].reshape(TOWERS, sums.shape[2], 3, share)
        got.o_qkv = jnp.transpose(qkv, (0, 2, 1, 3))
        got.o_out = jnp.transpose(sums[ATTN, :, :, 3 * share :], (0, 2, 1))
        got.o_rows = lax.psum(got.o_rows, "dp")

    big = [*got.o_y, *got.o_dx, got.o_qkv, got.o_out, got.o_up, got.o_down]
    pairs = jax.ShapeDtypeStruct((TOWERS, 2, share), F32)
    single = jax.ShapeDtypeStruct((TOWERS, share), F32)
    small = [pairs, single, jax.ShapeDtypeStruct((TOWERS, hidden), F32), single, pairs, pairs]
    count = len(big)
    results = pl.pallas_call(
        deliver,
        out_shape=[jax.ShapeDtypeStruct(x.shape, x.dtype) for x in big] + small,
        in_specs=[hbm] * count + [vmem],
        out_specs=[hbm] * count + [vmem] * len(small),
        scratch_shapes=[pltpu.VMEM(x.shape, x.dtype) for x in big]
        + [pltpu.SemaphoreType.DMA((count,)), pltpu.SemaphoreType.DMA((count,))],
        compiler_params=pltpu.CompilerParams(vmem_limit_bytes=67043328),
    )(*big, got.o_rows)
    rows, sums = results[: 2 * TOWERS], results[2 * TOWERS : count]
    qvb, outb, upb, downb, gains, shifts = results[count:]
    return (
        *[jnp.transpose(x, (0, 2, 1)) for x in rows],
        jnp.transpose(sums[0], (0, 2, 1, 3)),
        qvb,
        sums[1],
        outb,
        sums[2],
        upb,
        jnp.transpose(sums[3], (0, 2, 1)),
        downb,
        gains,
        shifts,
    )


def solution(mesh):
    dp, tensor = mesh.shape["dp"], mesh.shape["tensor"]

    def step(*args):
        return per_device(dp, tensor, *args)

    rows = P("dp", None, "tensor")
    return jax.shard_map(
        step,
        mesh=mesh,
        in_specs=(
            rows,
            rows,
            rows,
            P("dp"),
            P("dp"),
            P(None, None, None, "tensor"),
            P(None, None, "tensor"),
            P(None, "tensor", None),
            P(None, "tensor"),
            P(None, None, "tensor"),
            P(None, "tensor"),
            P(None, "tensor", None),
            P(None, "tensor"),
            P(None, None, "tensor"),
            P(None, None, "tensor"),
            rows,
            rows,
            rows,
        ),
        out_specs=(
            rows,
            rows,
            rows,
            rows,
            rows,
            rows,
            P(None, "dp", None, "tensor"),
            P(None, None, "tensor"),
            P(None, "tensor", "dp"),
            P(None, "tensor"),
            P(None, "dp", "tensor"),
            P(None, "tensor"),
            P(None, "tensor", "dp"),
            P(None, "tensor"),
            P(None, None, "tensor"),
            P(None, None, "tensor"),
        ),
        check_vma=False,
    )
```

```python
from types import SimpleNamespace

import jax
import jax.numpy as jnp
from jax import lax
from jax.experimental import pallas as pl
from jax.experimental.pallas import tpu as pltpu
from jax.sharding import PartitionSpec as P

HEAD_DIM = 64
PATCHES = 196
EPSILON = 1e-06
TOWERS = 3
FIRST, SECOND = 0, 1
UP, DOWN, ATTN = 0, 1, 2
RING = 3
UNITS = (
    (0, DOWN),
    (0, UP),
    (1, DOWN),
    (1, UP),
    (2, DOWN),
    (2, UP),
    (0, ATTN),
    (1, ATTN),
    (2, ATTN),
)
Z_FIRST = (1,)
TILE = 256
COLS = 12
N_REMOTE = 160
EARLY, LATE = 32, 8
SMALL = EARLY + LATE
LATE_COLS = (0, 1, 2, 8, 9, 10, 11)
BF16 = jnp.bfloat16
F32 = jnp.float32
MESH = pl.DeviceIdType.MESH
INV_SQRT2 = 0.7071067811865476
INV_SQRT_2PI = 0.3989422804014327


def nn(a, b):
    return lax.dot_general(a, b, (((1,), (0,)), ((), ())), preferred_element_type=F32)


def nt(a, b):
    return lax.dot_general(a, b, (((1,), (1,)), ((), ())), preferred_element_type=F32)


def up(value, multiple):
    return -(-value // multiple) * multiple


class Plan:
    def __init__(self, rows, weights, dp, tensor):
        qkv, out, upw = weights
        self.dp = dp
        self.examples = [r.shape[0] for r in rows]
        self.length = [r.shape[1] for r in rows]
        self.padded = [up(n, TILE) for n in self.length]
        self.lanes = [e * n for e, n in zip(self.examples, self.padded)]
        self.width = qkv.shape[1]
        self.share = out.shape[1]
        self.hidden = upw.shape[2]
        self.heads = self.share // HEAD_DIM
        self.pad = (3 * self.share) % TILE
        assert tensor == 4 and self.width == 4 * self.share
        assert self.pad + self.share == TILE and self.hidden == self.width
        self.fused = dp == 8 and self.width % (16 * dp) == 0
        self.nz = dp // 2 if self.fused else 1
        self.slab = self.width // dp if self.fused else self.width
        self.halves = 2 if self.fused else 1


def small_row(t, j):
    if t < TOWERS - 1:
        return t * COLS + j
    if j in LATE_COLS:
        return EARLY + LATE_COLS.index(j)
    return t * COLS + [c for c in range(COLS) if c not in LATE_COLS].index(j)


class Out:
    def __init__(self, spec, shape, dtype=F32):
        self.spec, self.shape, self.dtype = spec, shape, dtype


def flatten(tree):
    return jax.tree.flatten(tree, is_leaf=lambda v: not isinstance(v, (dict, list)))


def scratch(plan):
    width, share, hidden, nz = plan.width, plan.share, plan.hidden, plan.nz
    half, most = width // 2, max(plan.lanes)
    dma = pltpu.SemaphoreType.DMA

    def vm(*shape, dtype=BF16):
        return pltpu.VMEM(shape, dtype)

    def each(*lead, dtype=BF16):
        return [pltpu.VMEM((*lead, lanes), dtype) for lanes in plan.lanes]

    k = SimpleNamespace()
    k.x, k.dy, k.n = each(width), each(width), each(width)
    k.sums = [each(width), each(width)]
    k.part, k.rpart = each(width), each(width)
    k.qkv, k.m = each(3 * share), each(TILE)
    k.p = [vm(e * plan.heads, n, n) for e, n in zip(plan.examples, plan.padded)]
    k.near, k.far = each(half), [each(half), each(half)]
    k.rnear, k.rfar = each(2, share), [each(share), each(share)]
    k.own, k.row = each(share, dtype=F32), each(8, dtype=F32)
    k.stat_own, k.stat_near = each(8, dtype=F32), each(8, dtype=F32)
    k.stat_chip, k.stat_far = each(8, dtype=F32), each(8, dtype=F32)
    k.g_all = vm(RING, plan.halves, nz, plan.slab, width)
    k.credit = pltpu.SemaphoreType.REGULAR((RING,))
    k.out_sem = dma((4,))
    if plan.fused:
        k.g_y = vm(RING, nz, plan.slab, width)
        k.g_z = vm(RING, nz, plan.slab, width)
        k.g_far = vm(len(UNITS), 3, plan.slab, width)
        k.zf_near = vm(2, 2, plan.slab, width)
        k.zf_far, k.zf_y = vm(2, plan.slab, width), vm(plan.slab, width)
        k.s_ffn = vm(2, plan.slab, hidden, dtype=F32)
        k.s_qkv = vm(3, plan.slab, share, dtype=F32)
        k.s_out = vm(share, plan.slab, dtype=F32)
        k.rows = [vm(3, n, share, dtype=F32) for n in (EARLY, LATE)]
        k.rows_in = [vm(3, n, share, dtype=F32) for n in (EARLY, LATE)]
    k.wqkv_v, k.wout_v = vm(2, 3 * share, width), vm(2, share, width)
    k.wup_v, k.wdown_v = vm(width, hidden), vm(hidden, width)
    k.up_t, k.down_t = vm(hidden, width), vm(width, hidden)
    k.work_n, k.work_a = vm(width, most), vm(hidden, most)
    k.work_h, k.work_m = vm(width, most), vm(share, most)
    k.pown, k.pfull = vm(share, 128, dtype=F32), vm(width, 128)
    k.prm, k.small = vm(128, share, dtype=F32), vm(share, 128, dtype=F32)
    k.v_y = [vm(e, share, n) for e, n in zip(plan.examples, plan.length)]
    k.v_dx = [vm(e, share, n) for e, n in zip(plan.examples, plan.length)]
    k.row_sem = dma((2 * TOWERS,))
    k.in_sem, k.w_sem, k.part_sem = dma((2 * TOWERS,)), dma((18,)), dma(())
    k.send_sem, k.recv_sem = dma((N_REMOTE,)), dma((N_REMOTE,))
    return k


def kernel(plan, r):
    width, share, hidden, heads = plan.width, plan.share, plan.hidden, plan.heads
    half = width // 2
    nz = plan.nz

    dp_at = lax.axis_index("dp")
    me = lax.axis_index("tensor")
    core = lax.rem(me, 2)
    chip = lax.div(me, 2)
    y_at = lax.rem(dp_at, 2)
    z_at = lax.div(dp_at, 2)
    sibling = (dp_at, me + 1 - 2 * core)
    across = (dp_at, lax.rem(me + 2, 4))
    y_peer = (dp_at + 1 - 2 * y_at, me)

    z_near = z_at + 1 - 2 * lax.rem(z_at, 2)
    z_far, z_near_far = lax.rem(z_at + 2, 4), lax.rem(z_near + 2, 4)
    near_dev, far_dev = (z_near * 2 + y_at, me), (z_far * 2 + y_at, me)

    row_copies = []
    counter = [0]
    pending = []

    def remote(src, dst, device):
        at = counter[0]
        counter[0] += 1
        assert at < N_REMOTE
        return pltpu.make_async_remote_copy(
            src_ref=src,
            dst_ref=dst,
            send_sem=r.send_sem.at[at],
            recv_sem=r.recv_sem.at[at],
            device_id=device,
            device_id_type=MESH,
        )

    def launch(copy):
        copy.start()
        pending.append(copy)
        return copy

    def sent(copy):
        copy.wait_send()
        pending[:] = [other for other in pending if other is not copy]

    def block(at, size):
        return pl.ds(pl.multiple_of(at * size, size), size)

    own = block(me, share)
    my_half, other_half = block(core, half), block(1 - core, half)

    def lanes_loop(lanes, tile, body):
        def step(at, carry):
            body(block(at, tile))
            return carry

        lax.fori_loop(0, lanes // tile, step, 0)

    lane_of_small = lax.broadcasted_iota(jnp.int32, (share, 128), 1)

    def keep_sum(t, j, value):
        column = jnp.sum(value.astype(F32), axis=1, keepdims=True)
        small = r.small
        small[...] = jnp.where(lane_of_small == small_row(t, j), column, small[...])

    def own_col(t, j):
        return r.pown[:, t * COLS + j : t * COLS + j + 1]

    def full_col(t, j):
        return r.pfull[...].astype(F32)[:, t * COLS + j : t * COLS + j + 1]

    class Gather:
        def __init__(self, buf):
            self.to_sibling = remote(buf.at[own], buf.at[own], sibling)
            self.to_across = remote(buf.at[own], buf.at[own], across)
            blk = block(lax.rem(me + 2, 4), share)
            self.forwarded = remote(buf.at[blk], buf.at[blk], sibling)

        def start(self):
            launch(self.to_across)
            launch(self.to_sibling)

        def forward(self):
            self.to_across.wait_recv()
            launch(self.forwarded)

        def finish(self):
            self.to_sibling.wait_recv()
            self.forwarded.wait_recv()

    class AllReduce:
        def __init__(self, t, which):
            self.part, self.near = r.part[t], r.near[t]
            self.far, self.out = r.far[which][t], r.sums[which][t]
            self.c1 = remote(self.part.at[other_half], self.near, sibling)
            self.c2 = remote(self.part.at[my_half], self.far, across)
            self.c3 = remote(self.out.at[my_half], self.out.at[my_half], sibling)

        def begin(self):
            launch(self.c1)

        def cross(self):
            self.c1.wait_recv()
            total = self.part[my_half].astype(F32) + self.near[...].astype(F32)
            self.part[my_half] = total.astype(BF16)
            launch(self.c2)

        def back(self):
            self.c2.wait_recv()
            total = self.part[my_half].astype(F32) + self.far[...].astype(F32)
            self.out[my_half] = total.astype(BF16)
            launch(self.c3)

        def finish(self):
            self.c3.wait_recv()

        def free(self):
            sent(self.c1)
            sent(self.c2)
            sent(self.c3)

    class Scatter:
        def __init__(self, t, which):
            self.part, self.near, self.far = r.rpart[t], r.rnear[t], r.rfar[which][t]
            self.far_blk = block(2 * (1 - chip) + core, share)
            theirs = (2 * (1 - chip) + 1 - core, 2 * chip + 1 - core)
            self.c1 = [
                remote(self.part.at[block(theirs[j], share)], self.near.at[j], sibling)
                for j in range(2)
            ]
            self.c2 = remote(self.part.at[self.far_blk], self.far, across)

        def begin(self):
            for copy in self.c1:
                launch(copy)

        def cross(self):
            self.c1[0].wait_recv()
            blk = self.far_blk
            self.part[blk] = (self.part[blk].astype(F32) + self.near[0].astype(F32)).astype(BF16)
            launch(self.c2)
            self.c1[1].wait_recv()
            self.part[own] = (self.part[own].astype(F32) + self.near[1].astype(F32)).astype(BF16)

        def finish(self):
            self.c2.wait_recv()

        def free(self):
            for copy in self.c1:
                sent(copy)
            sent(self.c2)

    class Stats:
        def __init__(self, t):
            self.c1 = remote(r.stat_own[t], r.stat_near[t], sibling)
            self.c2 = remote(r.stat_chip[t], r.stat_far[t], across)
            self.t = t

        def begin(self):
            launch(self.c1)

        def cross(self):
            t = self.t
            self.c1.wait_recv()
            r.stat_chip[t][...] = r.stat_own[t][...] + r.stat_near[t][...]
            launch(self.c2)

        def finish(self):
            self.c2.wait_recv()

    class Unit:
        def __init__(self, at, t, kind):
            self.at, self.t, self.kind = at, t, kind
            self.slot = at % RING
            self.all = r.g_all.at[self.slot]
            self.sums = r.g_z.at[self.slot] if plan.fused else None
            self.first, self.z_copies, self.hbm = [], [], []
            self.z_first = at in Z_FIRST

        def across_z(self, src, dst, device):
            self.z_copies.append(launch(remote(src, dst, device)))

        def send(self):
            if not plan.fused:
                dst = r.o_g.at[self.kind, self.t]
                copy = pltpu.make_async_copy(self.all.at[0, 0], dst, r.part_sem)
                copy.start()
                copy.wait()
                return
            if self.at >= RING:
                pl.semaphore_wait(r.credit.at[self.slot], 1)
            if self.z_first:
                for i, blk in enumerate((z_near_far, z_near)):
                    for yy in range(2):
                        dst = r.zf_near.at[i, yy]
                        self.first.append(launch(remote(self.all.at[yy, blk], dst, near_dev)))
                return
            for blk in (z_near_far, z_near, z_far, z_at):
                src, dst = self.all.at[1 - y_at, blk], r.g_y.at[self.slot, blk]
                self.first.append(launch(remote(src, dst, y_peer)))

        def relay(self, step):
            if not plan.fused:
                return
            if step == 0 and self.at >= RING:
                for copy in units[self.at - RING].z_copies:
                    sent(copy)
            if self.z_first:
                self.relay_z(step)
            else:
                self.relay_y(step)
            if step == 3:
                for copy in self.first:
                    sent(copy)
                if self.at + RING < len(units):
                    credit = r.credit.at[self.slot]
                    pl.semaphore_signal(credit, inc=1, device_id=y_peer, device_id_type=MESH)

        def relay_y(self, step):
            blk = (z_near_far, z_near, z_far, z_at)[step]
            self.first[step].wait_recv()
            total = self.all[y_at, blk].astype(F32) + r.g_y[self.slot, blk].astype(F32)
            land = r.g_far.at[self.at]
            if step == 2:
                self.z_copies[0].wait_recv()
                total = total + r.g_far[self.at, 1].astype(F32)
            self.sums[blk] = total.astype(BF16)
            if step == 0:
                self.across_z(self.sums.at[blk], land.at[1], near_dev)
            if step == 1:
                self.across_z(self.sums.at[blk], land.at[0], near_dev)
            if step == 2:
                self.across_z(self.sums.at[blk], land.at[2], far_dev)

        def relay_z(self, step):
            def known(i, yy, blk):
                return self.all[yy, blk].astype(F32) + r.zf_near[i, yy].astype(F32)

            if step == 0:
                for yy in range(2):
                    self.first[yy].wait_recv()
                    self.sums[yy] = known(0, yy, z_far).astype(BF16)
                    self.across_z(self.sums.at[yy], r.zf_far.at[yy], far_dev)
            if step == 1:
                for yy in range(2):
                    self.first[2 + yy].wait_recv()
                    self.z_copies[yy].wait_recv()
                for at, yy in ((2, 1 - y_at), (3, y_at)):
                    total = known(1, yy, z_at) + r.zf_far[yy].astype(F32)
                    self.sums[at] = total.astype(BF16)
                self.across_z(self.sums.at[2], r.zf_y, y_peer)

        def finish(self):
            if not plan.fused:
                return
            if self.z_first:
                self.z_copies[2].wait_recv()
                total = self.sums[3].astype(F32) + r.zf_y[...].astype(F32)
            else:
                self.z_copies[1].wait_recv()
                self.z_copies[2].wait_recv()
                total = self.sums[z_at].astype(F32)
                for i in (0, 2):
                    total = total + r.g_far[self.at, i].astype(F32)
            t, sem = self.t, r.out_sem
            for before in units[: self.at]:
                if before.kind == self.kind:
                    for copy in before.hbm:
                        copy.wait()
                    before.hbm = []
            if self.kind == UP or self.kind == DOWN:
                out = r.o_up if self.kind == UP else r.o_down
                r.s_ffn[self.kind] = total
                self.hbm = [pltpu.make_async_copy(r.s_ffn.at[self.kind], out.at[t], sem.at[self.kind])]
            else:
                for c in range(3):
                    r.s_qkv[c] = total[:, c * share : (c + 1) * share]
                r.s_out[...] = total[:, 3 * share :].T
                self.hbm = [
                    pltpu.make_async_copy(r.s_qkv, r.o_qkv.at[t], sem.at[2]),
                    pltpu.make_async_copy(r.s_out, r.o_out.at[t], sem.at[3]),
                ]
            for copy in self.hbm:
                copy.start()

    gx = [Gather(r.x[t]) for t in range(TOWERS)]
    gdy = [Gather(r.dy[t]) for t in range(TOWERS)]
    gp = Gather(r.pfull)
    ar1 = [AllReduce(t, FIRST) for t in range(TOWERS)]
    ar2 = [AllReduce(t, SECOND) for t in range(TOWERS)]
    rs1 = [Scatter(t, FIRST) for t in range(TOWERS)]
    rs2 = [Scatter(t, SECOND) for t in range(TOWERS)]
    stats = [Stats(t) for t in range(TOWERS)]
    units = []
    for at, (t, kind) in enumerate(UNITS):
        units.append(Unit(at, t, kind))
    unit_of = {(unit.t, unit.kind): unit for unit in units}

    def attn_load(use):
        t, slot = use % TOWERS, use % 2
        pairs = ((r.wqkv, r.wqkv_v), (r.wout, r.wout_v))
        return [
            pltpu.make_async_copy(src.at[t], dst.at[slot], r.w_sem.at[6 + 2 * use + i])
            for i, (src, dst) in enumerate(pairs)
        ]

    attn_w = [attn_load(use) for use in range(2 * TOWERS)]
    ffn_w = [
        [
            pltpu.make_async_copy(r.wup.at[t], r.wup_v, r.w_sem.at[2 * t]),
            pltpu.make_async_copy(r.wdown.at[t], r.wdown_v, r.w_sem.at[2 * t + 1]),
        ]
        for t in range(TOWERS)
    ]

    def transpose_into(dst, src, rows, cols):
        for at in range(0, rows, TILE):
            size = min(TILE, rows - at)
            dst[:cols, at : at + size] = src[at : at + size, :].T

    def stage_in(ref, t, source):
        length, padded = plan.length[t], plan.padded[t]
        for e in range(plan.examples[t]):
            base = e * padded
            if length < padded:
                first = length // 128 * 128
                ref[own, base + first : base + padded] = jnp.zeros((share, padded - first), BF16)
            ref[own, base : base + length] = source[e]

    def param_rows():
        prm = r.prm
        prm[...] = jnp.zeros_like(prm)
        up_bias = r.in_up_b[...].astype(F32)
        for t in range(TOWERS):
            base = t * COLS
            for j in range(2):
                prm[base + j, :] = r.in_gain[t, j, :].astype(F32)
                prm[base + 2 + j, :] = r.in_shift[t, j, :].astype(F32)
                prm[base + 5 + j, :] = r.in_qv_b[t, j, :].astype(F32)
            prm[base + 4, :] = r.in_out_b[t, :].astype(F32)
            prm[base + 7, :] = r.in_down_b[t, :].astype(F32)
            for j in range(hidden // share):
                prm[base + 8 + j, :] = up_bias[t, j * share : (j + 1) * share]
        r.pown[...] = prm[...].T
        r.pfull[own] = r.pown[...].astype(BF16)

    def a_norm(t):
        gain, shift = full_col(t, 0), full_col(t, 2)

        def body(ls):
            x = r.x[t][:, ls].astype(F32)
            mean = jnp.sum(x, axis=0, keepdims=True) / width
            center = x - mean
            inv = lax.rsqrt(jnp.sum(center * center, axis=0, keepdims=True) / width + EPSILON)
            r.n[t][:, ls] = (center * inv * gain + shift).astype(BF16)
            r.row[t][0:1, ls] = mean
            r.row[t][1:2, ls] = inv

        lanes_loop(plan.lanes[t], 128, body)

    def a_qkv(t):
        for copy in attn_w[t]:
            copy.wait()
        bias = jnp.concatenate(
            [own_col(t, 5), jnp.zeros((share, 1), F32), own_col(t, 6)], axis=0
        )

        def body(ls):
            value = nn(r.wqkv_v[t % 2], r.n[t][:, ls]) + bias
            r.qkv[t][:, ls] = value.astype(BF16)

        lanes_loop(plan.lanes[t], TILE, body)

    def valid_keys(t, e):
        if t == 0:
            return plan.length[0]
        if t == 1:
            return r.in_text[e]
        return r.in_pair[e] + (PATCHES + 1)

    def a_heads(t):
        padded = plan.padded[t]
        key_at = lax.broadcasted_iota(jnp.int32, (padded, 1), 0)
        qkv = r.qkv[t]
        r.m[t][: plan.pad] = jnp.zeros((plan.pad, plan.lanes[t]), BF16)
        for e in range(plan.examples[t]):
            base = e * padded
            valid = key_at < valid_keys(t, e)

            def head(h, carry):
                rows_q = block(h, HEAD_DIM)
                rows_k = block(h + heads, HEAD_DIM)
                rows_v = block(h + 2 * heads, HEAD_DIM)
                rows_m = block(h + plan.pad // HEAD_DIM, HEAD_DIM)
                keys = qkv[rows_k, base : base + padded].T
                values = qkv[rows_v, base : base + padded]
                for q in range(padded // TILE):
                    at = base + q * TILE
                    s = nn(keys, qkv[rows_q, at : at + TILE]) * (HEAD_DIM**-0.5)
                    s = jnp.where(valid, s, -1000000000.0)
                    p = jnp.exp(s - jnp.max(s, axis=0, keepdims=True))
                    p = (p * (1.0 / jnp.sum(p, axis=0, keepdims=True))).astype(BF16)
                    r.p[t][e * heads + h, :, q * TILE : (q + 1) * TILE] = p
                    r.m[t][rows_m, at : at + TILE] = nn(values, p).astype(BF16)
                return carry

            lax.fori_loop(0, heads, head, 0)

    def a_out(t):
        transpose_into(r.work_a, r.wout_v.at[t % 2], share, width)

        def body(ls):
            mixed = r.m[t][plan.pad :, ls]
            r.part[t][:, ls] = nn(r.work_a[:, :share], mixed).astype(BF16)

        lanes_loop(plan.lanes[t], TILE, body)
        ar1[t].begin()
        for copy in attn_w[t + 2]:
            copy.start()

    def b_prep(t):
        for copy in ffn_w[t]:
            copy.wait()
        transpose_into(r.up_t, r.wup_v, width, hidden)
        transpose_into(r.down_t, r.wdown_v, hidden, width)

    def b_main(t):
        out_bias, gain, shift = full_col(t, 4), full_col(t, 1), full_col(t, 3)
        up_bias = jnp.concatenate([own_col(t, 8 + j) for j in range(hidden // share)], axis=0)
        ar1[t].free()

        def body(ls):
            x, s = r.x[t], r.sums[FIRST][t]
            resid = x[:, ls].astype(F32) + (s[:, ls].astype(F32) + out_bias)
            r.own[t][:, ls] = x[own, ls].astype(F32) + (s[own, ls].astype(F32) + own_col(t, 4))
            mean = jnp.sum(resid, axis=0, keepdims=True) / width
            center = resid - mean
            inv = lax.rsqrt(jnp.sum(center * center, axis=0, keepdims=True) / width + EPSILON)
            xhat = center * inv
            r.row[t][2:3, ls] = inv
            normed = (xhat * gain + shift).astype(BF16)
            s[:, ls] = xhat.astype(BF16)
            r.work_n[:, ls] = normed
            h = nn(r.up_t[...], normed) + up_bias
            cdf = 0.5 * (1.0 + lax.erf(h * INV_SQRT2))
            r.work_a[:, ls] = (h * cdf).astype(BF16)
            slope = cdf + h * (jnp.exp(-0.5 * (h * h)) * INV_SQRT_2PI)
            dact = nn(r.wdown_v[...], r.dy[t][:, ls])
            dhid = (dact * slope).astype(BF16)
            r.work_h[:hidden, ls] = dhid
            r.part[t][:, ls] = nn(r.wup_v[...], dhid).astype(BF16)

        lanes_loop(plan.lanes[t], TILE, body)
        ar2[t].begin()
        if t + 1 < TOWERS:
            for copy in ffn_w[t + 1]:
                copy.start()

    def b_ffn(t):
        def body(ls):
            r.rpart[t][:, ls] = nn(r.down_t[...], r.work_a[:, ls]).astype(BF16)

        lanes_loop(plan.lanes[t], TILE, body)
        rs1[t].begin()

    def spread(dst, value, ls):
        for b in range(plan.halves * nz):
            part = value[b * plan.slab : (b + 1) * plan.slab].astype(BF16)
            dst[b % plan.halves, b // plan.halves, :, ls] = part

    def grad_loop(unit, lhs, rhs):
        dst = unit.all

        def step(at, carry):
            rows = block(at, TILE)
            spread(dst, nt(lhs(), rhs(rows)), rows)
            return carry

        lax.fori_loop(0, hidden // TILE, step, 0)
        unit.send()

    def b_up(t):
        lanes = plan.lanes[t]
        grad_loop(
            unit_of[t, UP], lambda: r.work_n[:, :lanes], lambda rows: r.work_h[rows, :lanes]
        )

    def b_down(t):
        lanes = plan.lanes[t]
        grad_loop(unit_of[t, DOWN], lambda: r.dy[t][...], lambda rows: r.work_a[rows, :lanes])

    def b_sum(t):
        lanes = plan.lanes[t]
        for j in range(hidden // share):
            keep_sum(t, 3 + j, r.work_h[j * share : (j + 1) * share, :lanes])
        keep_sum(t, 7, r.dy[t][own])

    def y_out(t):
        rs1[t].finish()
        value = r.own[t][...] + (
            r.rpart[t][own].astype(F32) + r.rfar[FIRST][t][...].astype(F32) + own_col(t, 7)
        )
        padded = plan.padded[t]
        for e in range(plan.examples[t]):
            out = value[:, e * padded : e * padded + plan.length[t]]
            r.v_y[t][e] = out.astype(BF16)
        row_copies.append(pltpu.make_async_copy(r.v_y[t], r.o_y[t], r.row_sem.at[t]))
        row_copies[-1].start()

    def c_norm(t):
        for copy in attn_w[TOWERS + t]:
            copy.wait()
        slot = (TOWERS + t) % 2
        gain, gain_own = full_col(t, 1), own_col(t, 1)

        def body(ls):
            dn, xhat = r.sums[SECOND][t], r.sums[FIRST][t]
            xh = xhat[:, ls].astype(F32)
            e = dn[:, ls].astype(F32) * gain
            m1 = jnp.sum(e, axis=0, keepdims=True) / width
            m2 = jnp.sum(e * xh, axis=0, keepdims=True) / width
            inv = r.row[t][2:3, ls]
            dres = r.dy[t][:, ls].astype(F32) + inv * (e - m1 - xh * m2)
            r.work_n[:, ls] = dres.astype(BF16)
            e_own = dn[own, ls].astype(F32) * gain_own
            r.own[t][:, ls] = r.dy[t][own, ls].astype(F32) + inv * (
                e_own - m1 - xhat[own, ls].astype(F32) * m2
            )

        lanes_loop(plan.lanes[t], 128, body)

        def mix(ls):
            r.work_m[:, ls] = nn(r.wout_v[slot], r.work_n[:, ls]).astype(BF16)

        lanes_loop(plan.lanes[t], TILE, mix)

    def c_heads(t):
        padded = plan.padded[t]
        qkv = r.qkv[t]
        scale = HEAD_DIM**-0.5
        for e in range(plan.examples[t]):
            base = e * padded

            def head(h, carry):
                rows_q = block(h, HEAD_DIM)
                rows_k = block(h + heads, HEAD_DIM)
                rows_v = block(h + 2 * heads, HEAD_DIM)
                keys = qkv[rows_k, base : base + padded]
                values = qkv[rows_v, base : base + padded].T
                dk = dv = None
                for q in range(padded // TILE):
                    at = base + q * TILE
                    dm = r.work_m[rows_q, at : at + TILE]
                    p = r.p[t][e * heads + h, :, q * TILE : (q + 1) * TILE]
                    dp = nn(values, dm)
                    pf = p.astype(F32)
                    delta = jnp.sum(pf * dp, axis=0, keepdims=True)
                    ds = (pf * (dp - delta)).astype(BF16)
                    dq = nn(keys, ds) * scale
                    r.work_h[rows_q, at : at + TILE] = dq.astype(BF16)
                    dk_q = nt(qkv[rows_q, at : at + TILE], ds)
                    dv_q = nt(dm, p)
                    dk = dk_q if dk is None else dk + dk_q
                    dv = dv_q if dv is None else dv + dv_q
                r.work_h[rows_k, base : base + padded] = (dk * scale).astype(BF16)
                r.work_h[rows_v, base : base + padded] = dv.astype(BF16)
                return carry

            lax.fori_loop(0, heads, head, 0)

    def c_prep(t):
        transpose_into(r.up_t, r.wqkv_v.at[(TOWERS + t) % 2], 3 * share, width)

    def c_dn(t):
        gain = full_col(t, 0)
        rs1[t].free()
        r.stat_own[t][...] = jnp.zeros_like(r.stat_own[t])

        def body(ls):
            dn = nn(r.up_t[:, : 3 * share], r.work_h[: 3 * share, ls])
            e = dn * gain
            xhat = (r.x[t][:, ls].astype(F32) - r.row[t][0:1, ls]) * r.row[t][1:2, ls]
            r.stat_own[t][0:1, ls] = jnp.sum(e, axis=0, keepdims=True)
            r.stat_own[t][1:2, ls] = jnp.sum(e * xhat, axis=0, keepdims=True)
            r.rpart[t][:, ls] = dn.astype(BF16)

        lanes_loop(plan.lanes[t], TILE, body)
        rs2[t].begin()
        stats[t].begin()
        if t == 0:
            for copy in attn_w[5]:
                copy.start()

    def c_grad(t):
        lanes = plan.lanes[t]
        unit = unit_of[t, ATTN]
        r.work_h[3 * share :, :lanes] = jnp.zeros((width - 3 * share, lanes), BF16)
        whole = 3 * share // TILE

        def step(at, carry):
            rows = block(at, TILE)
            spread(unit.all, nt(r.n[t][...], r.work_h[rows, :lanes]), rows)
            return carry

        lax.fori_loop(0, whole, step, 0)
        last = slice(whole * TILE, (whole + 1) * TILE)
        value = nt(r.n[t][...], r.work_h[last, :lanes])
        value = value + nt(r.work_n[:, :lanes], r.m[t][...])
        spread(unit.all, value, last)
        unit.send()

    def c_sum(t):
        lanes = plan.lanes[t]
        keep_sum(t, 0, r.work_h[:share, :lanes])
        keep_sum(t, 1, r.work_h[2 * share : 3 * share, :lanes])
        keep_sum(t, 2, r.work_n[own, :lanes])
        dn, xhat = r.sums[SECOND][t], r.sums[FIRST][t]
        keep_sum(t, 9, dn[own].astype(F32) * xhat[own].astype(F32))
        keep_sum(t, 11, dn[own])

    def last_norm(t):
        rs2[t].finish()
        stats[t].finish()
        gain = own_col(t, 0)
        dn = r.rpart[t][own].astype(F32) + r.rfar[SECOND][t][...].astype(F32)
        total = r.stat_chip[t][...] + r.stat_far[t][...]
        inv = r.row[t][1:2, :]
        xhat = (r.x[t][own].astype(F32) - r.row[t][0:1, :]) * inv
        value = r.own[t][...] + inv * (
            dn * gain - total[0:1] / width - xhat * (total[1:2] / width)
        )
        padded = plan.padded[t]
        for e in range(plan.examples[t]):
            out = value[:, e * padded : e * padded + plan.length[t]]
            r.v_dx[t][e] = out.astype(BF16)
        row_copies.append(pltpu.make_async_copy(r.v_dx[t], r.o_dx[t], r.row_sem.at[TOWERS + t]))
        row_copies[-1].start()
        keep_sum(t, 8, dn * xhat)
        keep_sum(t, 10, dn)

    def small_send(late):
        rows = r.small[...].T
        first, last = (EARLY, EARLY + LATE) if late else (0, EARLY)
        part = rows[first:last]
        if not plan.fused:
            r.o_rows[first:last] = part
            return
        r.rows[late][0] = part
        small_step(late, 0)

    def small_step(late, step):
        rows, land = r.rows[late].at[step], r.rows_in[late].at[step]
        device = (y_peer, near_dev, far_dev)[step]
        small_copies[late].append(launch(remote(rows, land, device)))

    def small_relay(late, step):
        if not plan.fused:
            return
        small_copies[late][step - 1].wait_recv()
        r.rows[late][step] = r.rows[late][step - 1] + r.rows_in[late][step - 1]
        small_step(late, step)

    def small_finish(late):
        if not plan.fused:
            return
        small_copies[late][2].wait_recv()
        total = r.rows[late][2] + r.rows_in[late][2]
        if late:
            r.o_rows[EARLY : EARLY + LATE] = total
        else:
            r.o_rows[:EARLY] = total

    small_copies = [[], []]

    barrier = pltpu.get_barrier_semaphore()
    partners = [sibling, across]
    if plan.fused:
        partners += [y_peer, near_dev, far_dev]
    for device in partners:
        pl.semaphore_signal(barrier, inc=1, device_id=device, device_id_type=MESH)
    loads = [
        pltpu.make_async_copy(src[t], dst[t], r.in_sem.at[i * TOWERS + t])
        for i, (src, dst) in enumerate(((r.in_x, r.v_y), (r.in_dy, r.v_dx)))
        for t in range(TOWERS)
    ]
    for copy in loads + attn_w[0] + ffn_w[0] + attn_w[1]:
        copy.start()
    param_rows()
    loads[0].wait()
    stage_in(r.x[0], 0, r.v_y[0])
    pl.semaphore_wait(barrier, len(partners))
    gp.start()
    gx[0].start()
    for t in range(1, TOWERS):
        loads[t].wait()
        stage_in(r.x[t], t, r.v_y[t])
    for t in range(TOWERS):
        loads[TOWERS + t].wait()
        stage_in(r.dy[t], t, r.v_dx[t])
    r.small[...] = jnp.zeros_like(r.small)
    gx[1].start()
    gp.forward()
    gp.finish()
    b_prep(0)
    gdy[0].start()
    gx[0].forward()
    gx[0].finish()
    a_norm(0)
    a_qkv(0)
    a_heads(0)
    a_out(0)
    ar1[0].cross()
    gx[2].start()
    gx[1].forward()
    gdy[0].forward()
    gx[1].finish()
    gdy[0].finish()
    a_norm(1)
    a_qkv(1)
    a_heads(1)
    a_out(1)
    ar1[1].cross()
    gdy[1].start()
    gdy[2].start()
    ar1[0].back()
    ar1[0].finish()
    b_main(0)
    b_down(0)
    b_up(0)
    gx[2].forward()
    b_ffn(0)
    b_prep(1)
    gx[2].finish()
    a_norm(2)
    a_qkv(2)
    b_sum(0)
    a_heads(2)
    gdy[1].forward()
    ar1[1].back()
    a_out(2)
    units[0].relay(0)
    gdy[1].finish()
    ar1[1].finish()
    b_main(1)
    b_down(1)
    b_sum(1)
    ar1[2].cross()
    units[0].relay(1)
    units[0].relay(2)
    units[0].relay(3)
    gdy[2].forward()
    rs1[0].cross()
    units[1].relay(0)
    gdy[2].finish()
    b_up(1)
    units[0].finish()
    b_ffn(1)
    b_prep(2)
    ar2[0].cross()
    ar1[2].back()
    ar1[2].finish()
    units[1].relay(1)
    units[1].relay(2)
    units[1].relay(3)
    units[2].relay(0)
    ar2[1].cross()
    units[2].relay(1)
    b_main(2)
    b_sum(2)
    units[2].relay(2)
    rs1[1].cross()
    b_down(2)
    units[2].relay(3)
    units[3].relay(0)
    b_ffn(2)
    b_up(2)
    units[3].relay(1)
    units[1].finish()
    ar2[0].back()
    rs1[2].cross()
    ar2[0].finish()
    y_out(0)
    c_norm(0)
    ar2[1].back()
    units[3].relay(2)
    units[3].relay(3)
    c_heads(0)
    c_sum(0)
    units[2].finish()
    c_prep(0)
    ar2[2].cross()
    units[4].relay(0)
    units[4].relay(1)
    c_grad(0)
    c_dn(0)
    units[4].relay(2)
    units[4].relay(3)
    units[3].finish()
    units[5].relay(0)
    units[5].relay(1)
    rs2[0].cross()
    y_out(1)
    y_out(2)
    ar2[1].finish()
    c_norm(1)
    c_prep(1)
    c_heads(1)
    c_sum(1)
    c_dn(1)
    c_grad(1)
    stats[0].cross()
    ar2[2].back()
    units[5].relay(2)
    units[5].relay(3)
    ar2[2].finish()
    c_norm(2)
    units[6].relay(0)
    units[6].relay(1)
    rs2[1].cross()
    stats[1].cross()
    c_heads(2)
    units[4].finish()
    units[6].relay(2)
    c_prep(2)
    c_dn(2)
    units[6].relay(3)
    units[7].relay(0)
    units[7].relay(1)
    rs2[2].cross()
    last_norm(1)
    last_norm(0)
    small_send(0)
    c_grad(2)
    units[5].finish()
    small_relay(0, 1)
    stats[2].cross()
    units[7].relay(2)
    units[7].relay(3)
    last_norm(2)
    units[6].finish()
    c_sum(2)
    small_relay(0, 2)
    units[8].relay(0)
    units[8].relay(1)
    small_send(1)
    small_relay(1, 1)
    units[8].relay(2)
    units[7].finish()
    small_relay(1, 2)
    units[8].relay(3)
    units[8].finish()
    small_finish(0)
    small_finish(1)
    for copy in list(pending):
        sent(copy)
    for unit in units:
        for copy in unit.hbm:
            copy.wait()
    for copy in row_copies:
        copy.wait()


def deliver(*refs):
    count = 2 * TOWERS + 4
    src, rows = refs[:count], refs[count]
    dst = refs[count + 1 : 2 * count + 1]
    qvb, outb, upb, downb, gains, shifts = refs[2 * count + 1 : 2 * count + 7]
    room = refs[2 * count + 7 : 3 * count + 7]
    in_sem, out_sem = refs[3 * count + 7 :]
    reads = [pltpu.make_async_copy(src[i], room[i], in_sem.at[i]) for i in range(count)]
    writes = [pltpu.make_async_copy(room[i], dst[i], out_sem.at[i]) for i in range(count)]
    for copy in reads:
        copy.start()
    share = rows.shape[1]
    for t in range(TOWERS):
        for j in range(2):
            qvb[t, j, :] = rows[small_row(t, j), :]
            gains[t, j, :] = rows[small_row(t, 8 + j), :]
            shifts[t, j, :] = rows[small_row(t, 10 + j), :]
        outb[t, :] = rows[small_row(t, 2), :]
        downb[t, :] = rows[small_row(t, 7), :]
        for j in range(upb.shape[1] // share):
            upb[t, j * share : (j + 1) * share] = rows[small_row(t, 3 + j), :]
    for read, write in zip(reads, writes):
        read.wait()
        write.start()
    for copy in writes:
        copy.wait()


def per_device(dp, tensor, *args):
    rows, ups = args[0:3], args[15:18]
    text_lengths, pair_lengths = args[3:5]
    qkv_w, qv_b, out_w, out_b, up_w, up_b, down_w, down_b, gain, shift = args[5:15]
    plan = Plan(rows, (qkv_w, out_w, up_w), dp, tensor)
    width, share, hidden = plan.width, plan.share, plan.hidden
    nz = plan.nz

    turned = [jnp.transpose(x, (0, 2, 1)) for x in rows]
    turned_up = [jnp.transpose(x, (0, 2, 1)) for x in ups]
    wqkv = jnp.transpose(qkv_w, (0, 2, 3, 1)).reshape(TOWERS, 3 * share, width)
    vmem = pl.BlockSpec(memory_space=pltpu.VMEM)
    hbm = pl.BlockSpec(memory_space=pl.ANY)
    smem = pl.BlockSpec(memory_space=pltpu.SMEM)

    ins, specs = SimpleNamespace(), SimpleNamespace()
    ins.in_x, specs.in_x = turned, [hbm] * TOWERS
    ins.in_dy, specs.in_dy = turned_up, [hbm] * TOWERS
    ins.in_text, specs.in_text = text_lengths, smem
    ins.in_pair, specs.in_pair = pair_lengths, smem
    ins.in_gain, specs.in_gain = gain, vmem
    ins.in_shift, specs.in_shift = shift, vmem
    ins.in_out_b, specs.in_out_b = out_b, vmem
    ins.in_qv_b, specs.in_qv_b = qv_b, vmem
    ins.in_down_b, specs.in_down_b = down_b, vmem
    ins.in_up_b, specs.in_up_b = up_b, vmem
    ins.wqkv, specs.wqkv = wqkv, hbm
    ins.wout, specs.wout = out_w, hbm
    ins.wup, specs.wup = up_w, hbm
    ins.wdown, specs.wdown = down_w, hbm

    outs = SimpleNamespace()
    outs.o_y = [Out(hbm, x.shape, BF16) for x in turned]
    outs.o_dx = [Out(hbm, x.shape, BF16) for x in turned]
    if plan.fused:
        outs.o_qkv = Out(hbm, (TOWERS, 3, plan.slab, share))
        outs.o_out = Out(hbm, (TOWERS, share, plan.slab))
        outs.o_up = Out(hbm, (TOWERS, plan.slab, hidden))
        outs.o_down = Out(hbm, (TOWERS, plan.slab, hidden))
    else:
        outs.o_g = Out(hbm, (3, TOWERS, width, width), BF16)
    outs.o_rows = Out(vmem, (SMALL, share))

    room = scratch(plan)
    in_refs, in_tree = flatten(vars(ins))
    out_refs, out_tree = flatten(vars(outs))
    room_refs, room_tree = flatten(vars(room))

    def body(*refs):
        first, second = len(in_refs), len(in_refs) + len(out_refs)
        r = SimpleNamespace()
        vars(r).update(jax.tree.unflatten(in_tree, refs[:first]))
        vars(r).update(jax.tree.unflatten(out_tree, refs[first:second]))
        vars(r).update(jax.tree.unflatten(room_tree, refs[second:]))
        kernel(plan, r)

    results = pl.pallas_call(
        body,
        out_shape=[jax.ShapeDtypeStruct(out.shape, out.dtype) for out in out_refs],
        in_specs=flatten(vars(specs))[0],
        out_specs=[out.spec for out in out_refs],
        scratch_shapes=room_refs,
        compiler_params=pltpu.CompilerParams(
            collective_id=1, has_side_effects=True, vmem_limit_bytes=67043328
        ),
        name="layer",
    )(*in_refs)
    got = SimpleNamespace(**jax.tree.unflatten(out_tree, results))

    if not plan.fused:
        sums = lax.psum_scatter(got.o_g.astype(F32), "dp", scatter_dimension=2, tiled=True)
        got.o_up, got.o_down = sums[UP], sums[DOWN]
        qkv = sums[ATTN, :, :, : 3 * share].reshape(TOWERS, sums.shape[2], 3, share)
        got.o_qkv = jnp.transpose(qkv, (0, 2, 1, 3))
        got.o_out = jnp.transpose(sums[ATTN, :, :, 3 * share :], (0, 2, 1))
        got.o_rows = lax.psum(got.o_rows, "dp")

    big = [*got.o_y, *got.o_dx, got.o_qkv, got.o_out, got.o_up, got.o_down]
    pairs = jax.ShapeDtypeStruct((TOWERS, 2, share), F32)
    single = jax.ShapeDtypeStruct((TOWERS, share), F32)
    small = [pairs, single, jax.ShapeDtypeStruct((TOWERS, hidden), F32), single, pairs, pairs]
    count = len(big)
    results = pl.pallas_call(
        deliver,
        out_shape=[jax.ShapeDtypeStruct(x.shape, x.dtype) for x in big] + small,
        in_specs=[hbm] * count + [vmem],
        out_specs=[hbm] * count + [vmem] * len(small),
        scratch_shapes=[pltpu.VMEM(x.shape, x.dtype) for x in big]
        + [pltpu.SemaphoreType.DMA((count,)), pltpu.SemaphoreType.DMA((count,))],
        compiler_params=pltpu.CompilerParams(vmem_limit_bytes=67043328),
    )(*big, got.o_rows)
    rows, sums = results[: 2 * TOWERS], results[2 * TOWERS : count]
    qvb, outb, upb, downb, gains, shifts = results[count:]
    return (
        *[jnp.transpose(x, (0, 2, 1)) for x in rows],
        jnp.transpose(sums[0], (0, 2, 1, 3)),
        qvb,
        sums[1],
        outb,
        sums[2],
        upb,
        jnp.transpose(sums[3], (0, 2, 1)),
        downb,
        gains,
        shifts,
    )


def solution(mesh):
    dp, tensor = mesh.shape["dp"], mesh.shape["tensor"]

    def step(*args):
        return per_device(dp, tensor, *args)

    rows = P("dp", None, "tensor")
    return jax.shard_map(
        step,
        mesh=mesh,
        in_specs=(
            rows,
            rows,
            rows,
            P("dp"),
            P("dp"),
            P(None, None, None, "tensor"),
            P(None, None, "tensor"),
            P(None, "tensor", None),
            P(None, "tensor"),
            P(None, None, "tensor"),
            P(None, "tensor"),
            P(None, "tensor", None),
            P(None, "tensor"),
            P(None, None, "tensor"),
            P(None, None, "tensor"),
            rows,
            rows,
            rows,
        ),
        out_specs=(
            rows,
            rows,
            rows,
            rows,
            rows,
            rows,
            P(None, "dp", None, "tensor"),
            P(None, None, "tensor"),
            P(None, "tensor", "dp"),
            P(None, "tensor"),
            P(None, "dp", "tensor"),
            P(None, "tensor"),
            P(None, "tensor", "dp"),
            P(None, "tensor"),
            P(None, None, "tensor"),
            P(None, None, "tensor"),
        ),
        check_vma=False,
    )
```

```python
from types import SimpleNamespace

import jax
import jax.numpy as jnp
from jax import lax
from jax.experimental import pallas as pl
from jax.experimental.pallas import tpu as pltpu
from jax.sharding import PartitionSpec as P

HEAD_DIM = 64
PATCHES = 196
EPSILON = 1e-06
TOWERS = 3
FIRST, SECOND = 0, 1
UP, DOWN, ATTN = 0, 1, 2
RING = 3
UNITS = (
    (0, DOWN),
    (0, UP),
    (1, DOWN),
    (1, UP),
    (2, DOWN),
    (2, UP),
    (0, ATTN),
    (1, ATTN),
    (2, ATTN),
)
Z_FIRST = (2,)
TILE = 256
COLS = 12
N_REMOTE = 132
EARLY, LATE = 32, 8
SMALL = EARLY + LATE
LATE_COLS = (0, 1, 2, 8, 9, 10, 11)
BF16 = jnp.bfloat16
F32 = jnp.float32
MESH = pl.DeviceIdType.MESH
INV_SQRT2 = 0.7071067811865476
INV_SQRT_2PI = 0.3989422804014327


def nn(a, b):
    return lax.dot_general(a, b, (((1,), (0,)), ((), ())), preferred_element_type=F32)


def nt(a, b):
    return lax.dot_general(a, b, (((1,), (1,)), ((), ())), preferred_element_type=F32)


def up(value, multiple):
    return -(-value // multiple) * multiple


class Plan:
    def __init__(self, rows, weights, dp, tensor):
        qkv, out, upw = weights
        self.dp = dp
        self.examples = [r.shape[0] for r in rows]
        self.length = [r.shape[1] for r in rows]
        self.padded = [up(n, TILE) for n in self.length]
        self.lanes = [e * n for e, n in zip(self.examples, self.padded)]
        self.width = qkv.shape[1]
        self.share = out.shape[1]
        self.hidden = upw.shape[2]
        self.heads = self.share // HEAD_DIM
        self.pad = (3 * self.share) % TILE
        assert tensor == 4 and self.width == 4 * self.share
        assert self.pad + self.share == TILE and self.hidden == self.width
        self.fused = dp == 8 and self.width % (16 * dp) == 0
        self.nz = dp // 2 if self.fused else 1
        self.slab = self.width // dp if self.fused else self.width
        self.halves = 2 if self.fused else 1


def small_row(t, j):
    if t < TOWERS - 1:
        return t * COLS + j
    if j in LATE_COLS:
        return EARLY + LATE_COLS.index(j)
    return t * COLS + [c for c in range(COLS) if c not in LATE_COLS].index(j)


class Out:
    def __init__(self, spec, shape, dtype=F32):
        self.spec, self.shape, self.dtype = spec, shape, dtype


def flatten(tree):
    return jax.tree.flatten(tree, is_leaf=lambda v: not isinstance(v, (dict, list)))


def scratch(plan):
    width, share, hidden, nz = plan.width, plan.share, plan.hidden, plan.nz
    half, most = width // 2, max(plan.lanes)
    dma = pltpu.SemaphoreType.DMA

    def vm(*shape, dtype=BF16):
        return pltpu.VMEM(shape, dtype)

    def each(*lead, dtype=BF16):
        return [pltpu.VMEM((*lead, lanes), dtype) for lanes in plan.lanes]

    k = SimpleNamespace()
    k.x, k.dy, k.n = each(width), each(width), each(width)
    k.sums = [each(width), each(width)]
    k.part, k.rpart = each(width), each(width)
    k.qkv, k.m = each(3 * share), each(TILE)
    k.p = [vm(e * plan.heads, n, n) for e, n in zip(plan.examples, plan.padded)]
    k.near, k.far = each(half), [each(half), each(half)]
    k.rnear, k.rfar = each(2, share), [each(share), each(share)]
    k.own, k.row = each(share, dtype=F32), each(8, dtype=F32)
    k.stat_own, k.stat_near = each(8, dtype=F32), each(8, dtype=F32)
    k.stat_chip, k.stat_far = each(8, dtype=F32), each(8, dtype=F32)
    k.g_all = vm(RING, plan.halves, nz, plan.slab, width)
    k.credit = pltpu.SemaphoreType.REGULAR((RING,))
    k.out_sem = dma((4,))
    if plan.fused:
        k.g_y = vm(RING, nz, plan.slab, width)
        k.g_z = vm(RING, nz, plan.slab, width)
        k.g_far = vm(len(UNITS), 3, plan.slab, width)
        k.zf_near = vm(2, 2, plan.slab, width)
        k.zf_far, k.zf_y = vm(2, plan.slab, width), vm(plan.slab, width)
        k.s_ffn = vm(2, plan.slab, hidden, dtype=F32)
        k.s_qkv = vm(3, plan.slab, share, dtype=F32)
        k.s_out = vm(share, plan.slab, dtype=F32)
        k.rows = [vm(3, n, share, dtype=F32) for n in (EARLY, LATE)]
        k.rows_in = [vm(3, n, share, dtype=F32) for n in (EARLY, LATE)]
    k.wqkv_v, k.wout_v = vm(2, 3 * share, width), vm(2, share, width)
    k.wup_v, k.wdown_v = vm(width, hidden), vm(hidden, width)
    k.up_t, k.down_t = vm(hidden, width), vm(width, hidden)
    k.work_n, k.work_a = vm(width, most), vm(hidden, most)
    k.work_h, k.work_m = vm(width, most), vm(share, most)
    k.pown, k.pfull = vm(share, 128, dtype=F32), vm(width, 128)
    k.prm, k.small = vm(128, share, dtype=F32), vm(share, 128, dtype=F32)
    k.v_y = [vm(e, share, n) for e, n in zip(plan.examples, plan.length)]
    k.v_dx = [vm(e, share, n) for e, n in zip(plan.examples, plan.length)]
    k.row_sem = dma((2 * TOWERS,))
    k.in_sem, k.w_sem, k.part_sem = dma((2 * TOWERS,)), dma((18,)), dma(())
    k.send_sem, k.recv_sem = dma((N_REMOTE,)), dma((N_REMOTE,))
    return k


def kernel(plan, r):
    width, share, hidden, heads = plan.width, plan.share, plan.hidden, plan.heads
    half = width // 2
    nz = plan.nz

    dp_at = lax.axis_index("dp")
    me = lax.axis_index("tensor")
    core = lax.rem(me, 2)
    chip = lax.div(me, 2)
    y_at = lax.rem(dp_at, 2)
    z_at = lax.div(dp_at, 2)
    sibling = (dp_at, me + 1 - 2 * core)
    across = (dp_at, lax.rem(me + 2, 4))
    y_peer = (dp_at + 1 - 2 * y_at, me)

    z_near = z_at + 1 - 2 * lax.rem(z_at, 2)
    z_far, z_near_far = lax.rem(z_at + 2, 4), lax.rem(z_near + 2, 4)
    near_dev, far_dev = (z_near * 2 + y_at, me), (z_far * 2 + y_at, me)

    row_copies = []
    counter = [0]
    pending = []

    def remote(src, dst, device):
        at = counter[0]
        counter[0] += 1
        assert at < N_REMOTE
        return pltpu.make_async_remote_copy(
            src_ref=src,
            dst_ref=dst,
            send_sem=r.send_sem.at[at],
            recv_sem=r.recv_sem.at[at],
            device_id=device,
            device_id_type=MESH,
        )

    def launch(copy):
        copy.start()
        pending.append(copy)
        return copy

    def sent(copy):
        copy.wait_send()
        pending[:] = [other for other in pending if other is not copy]

    def block(at, size):
        return pl.ds(pl.multiple_of(at * size, size), size)

    own = block(me, share)
    my_half, other_half = block(core, half), block(1 - core, half)

    def lanes_loop(lanes, tile, body):
        def step(at, carry):
            body(block(at, tile))
            return carry

        lax.fori_loop(0, lanes // tile, step, 0)

    lane_of_small = lax.broadcasted_iota(jnp.int32, (share, 128), 1)

    def keep_sum(t, j, value):
        column = jnp.sum(value.astype(F32), axis=1, keepdims=True)
        small = r.small
        small[...] = jnp.where(lane_of_small == small_row(t, j), column, small[...])

    def own_col(t, j):
        return r.pown[:, t * COLS + j : t * COLS + j + 1]

    def full_col(t, j):
        return r.pfull[...].astype(F32)[:, t * COLS + j : t * COLS + j + 1]

    class Gather:
        def __init__(self, buf):
            self.to_sibling = remote(buf.at[own], buf.at[own], sibling)
            self.to_across = remote(buf.at[own], buf.at[own], across)
            blk = block(lax.rem(me + 2, 4), share)
            self.forwarded = remote(buf.at[blk], buf.at[blk], sibling)

        def start(self):
            launch(self.to_across)
            launch(self.to_sibling)

        def forward(self):
            self.to_across.wait_recv()
            launch(self.forwarded)

        def finish(self):
            self.to_sibling.wait_recv()
            self.forwarded.wait_recv()

    class AllReduce:
        def __init__(self, t, which):
            self.part, self.near = r.part[t], r.near[t]
            self.far, self.out = r.far[which][t], r.sums[which][t]
            self.c1 = remote(self.part.at[other_half], self.near, sibling)
            self.c2 = remote(self.part.at[my_half], self.far, across)
            self.c3 = remote(self.out.at[my_half], self.out.at[my_half], sibling)

        def begin(self):
            launch(self.c1)

        def cross(self):
            self.c1.wait_recv()
            total = self.part[my_half].astype(F32) + self.near[...].astype(F32)
            self.part[my_half] = total.astype(BF16)
            launch(self.c2)

        def back(self):
            self.c2.wait_recv()
            total = self.part[my_half].astype(F32) + self.far[...].astype(F32)
            self.out[my_half] = total.astype(BF16)
            launch(self.c3)

        def finish(self):
            self.c3.wait_recv()

        def free(self):
            sent(self.c1)
            sent(self.c2)
            sent(self.c3)

    class Scatter:
        def __init__(self, t, which):
            self.part, self.near, self.far = r.rpart[t], r.rnear[t], r.rfar[which][t]
            self.far_blk = block(2 * (1 - chip) + core, share)
            theirs = (2 * (1 - chip) + 1 - core, 2 * chip + 1 - core)
            self.c1 = [
                remote(self.part.at[block(theirs[j], share)], self.near.at[j], sibling)
                for j in range(2)
            ]
            self.c2 = remote(self.part.at[self.far_blk], self.far, across)

        def begin(self):
            for copy in self.c1:
                launch(copy)

        def cross(self):
            self.c1[0].wait_recv()
            blk = self.far_blk
            self.part[blk] = (self.part[blk].astype(F32) + self.near[0].astype(F32)).astype(BF16)
            launch(self.c2)
            self.c1[1].wait_recv()
            self.part[own] = (self.part[own].astype(F32) + self.near[1].astype(F32)).astype(BF16)

        def finish(self):
            self.c2.wait_recv()

        def free(self):
            for copy in self.c1:
                sent(copy)
            sent(self.c2)

    class Stats:
        def __init__(self, t):
            self.c1 = remote(r.stat_own[t], r.stat_near[t], sibling)
            self.c2 = remote(r.stat_chip[t], r.stat_far[t], across)
            self.t = t

        def begin(self):
            launch(self.c1)

        def cross(self):
            t = self.t
            self.c1.wait_recv()
            r.stat_chip[t][...] = r.stat_own[t][...] + r.stat_near[t][...]
            launch(self.c2)

        def finish(self):
            self.c2.wait_recv()

    class Unit:
        def __init__(self, at, t, kind):
            self.at, self.t, self.kind = at, t, kind
            self.slot = at % RING
            self.all = r.g_all.at[self.slot]
            self.sums = r.g_z.at[self.slot] if plan.fused else None
            self.first, self.z_copies, self.hbm = [], [], []
            self.z_first = at in Z_FIRST

        def across_z(self, src, dst, device):
            self.z_copies.append(launch(remote(src, dst, device)))

        def send(self):
            if not plan.fused:
                dst = r.o_g.at[self.kind, self.t]
                copy = pltpu.make_async_copy(self.all.at[0, 0], dst, r.part_sem)
                copy.start()
                copy.wait()
                return
            if self.at >= RING:
                pl.semaphore_wait(r.credit.at[self.slot], 1)
            if self.z_first:
                for i, blk in enumerate((z_near_far, z_near)):
                    for yy in range(2):
                        dst = r.zf_near.at[i, yy]
                        self.first.append(launch(remote(self.all.at[yy, blk], dst, near_dev)))
                return
            for blk in (z_near_far, z_near, z_far, z_at):
                src, dst = self.all.at[1 - y_at, blk], r.g_y.at[self.slot, blk]
                self.first.append(launch(remote(src, dst, y_peer)))

        def relay(self, step):
            if not plan.fused:
                return
            if step == 0 and self.at >= RING:
                for copy in units[self.at - RING].z_copies:
                    sent(copy)
            if self.z_first:
                self.relay_z(step)
            else:
                self.relay_y(step)
            if step == 3:
                for copy in self.first:
                    sent(copy)
                if self.at + RING < len(units):
                    credit = r.credit.at[self.slot]
                    pl.semaphore_signal(credit, inc=1, device_id=y_peer, device_id_type=MESH)

        def relay_y(self, step):
            blk = (z_near_far, z_near, z_far, z_at)[step]
            self.first[step].wait_recv()
            total = self.all[y_at, blk].astype(F32) + r.g_y[self.slot, blk].astype(F32)
            land = r.g_far.at[self.at]
            if step == 2:
                self.z_copies[0].wait_recv()
                total = total + r.g_far[self.at, 1].astype(F32)
            self.sums[blk] = total.astype(BF16)
            if step == 0:
                self.across_z(self.sums.at[blk], land.at[1], near_dev)
            if step == 1:
                self.across_z(self.sums.at[blk], land.at[0], near_dev)
            if step == 2:
                self.across_z(self.sums.at[blk], land.at[2], far_dev)

        def relay_z(self, step):
            def known(i, yy, blk):
                return self.all[yy, blk].astype(F32) + r.zf_near[i, yy].astype(F32)

            if step == 0:
                for yy in range(2):
                    self.first[yy].wait_recv()
                    self.sums[yy] = known(0, yy, z_far).astype(BF16)
                    self.across_z(self.sums.at[yy], r.zf_far.at[yy], far_dev)
            if step == 1:
                for yy in range(2):
                    self.first[2 + yy].wait_recv()
                    self.z_copies[yy].wait_recv()
                for at, yy in ((2, 1 - y_at), (3, y_at)):
                    total = known(1, yy, z_at) + r.zf_far[yy].astype(F32)
                    self.sums[at] = total.astype(BF16)
                self.across_z(self.sums.at[2], r.zf_y, y_peer)

        def finish(self):
            if not plan.fused:
                return
            if self.z_first:
                self.z_copies[2].wait_recv()
                total = self.sums[3].astype(F32) + r.zf_y[...].astype(F32)
            else:
                self.z_copies[1].wait_recv()
                self.z_copies[2].wait_recv()
                total = self.sums[z_at].astype(F32)
                for i in (0, 2):
                    total = total + r.g_far[self.at, i].astype(F32)
            t, sem = self.t, r.out_sem
            for before in units[: self.at]:
                if before.kind == self.kind:
                    for copy in before.hbm:
                        copy.wait()
                    before.hbm = []
            if self.kind == UP or self.kind == DOWN:
                out = r.o_up if self.kind == UP else r.o_down
                r.s_ffn[self.kind] = total
                self.hbm = [pltpu.make_async_copy(r.s_ffn.at[self.kind], out.at[t], sem.at[self.kind])]
            else:
                for c in range(3):
                    r.s_qkv[c] = total[:, c * share : (c + 1) * share]
                r.s_out[...] = total[:, 3 * share :].T
                self.hbm = [
                    pltpu.make_async_copy(r.s_qkv, r.o_qkv.at[t], sem.at[2]),
                    pltpu.make_async_copy(r.s_out, r.o_out.at[t], sem.at[3]),
                ]
            for copy in self.hbm:
                copy.start()

    gx = [Gather(r.x[t]) for t in range(TOWERS)]
    gdy = [Gather(r.dy[t]) for t in range(TOWERS)]
    gp = Gather(r.pfull)
    ar1 = [AllReduce(t, FIRST) for t in range(TOWERS)]
    ar2 = [AllReduce(t, SECOND) for t in range(TOWERS)]
    rs1 = [Scatter(t, FIRST) for t in range(TOWERS)]
    rs2 = [Scatter(t, SECOND) for t in range(TOWERS)]
    stats = [Stats(t) for t in range(TOWERS)]
    units = []
    for at, (t, kind) in enumerate(UNITS):
        units.append(Unit(at, t, kind))
    unit_of = {(unit.t, unit.kind): unit for unit in units}

    def attn_load(use):
        t, slot = use % TOWERS, use % 2
        pairs = ((r.wqkv, r.wqkv_v), (r.wout, r.wout_v))
        return [
            pltpu.make_async_copy(src.at[t], dst.at[slot], r.w_sem.at[6 + 2 * use + i])
            for i, (src, dst) in enumerate(pairs)
        ]

    attn_w = [attn_load(use) for use in range(2 * TOWERS)]
    ffn_w = [
        [
            pltpu.make_async_copy(r.wup.at[t], r.wup_v, r.w_sem.at[2 * t]),
            pltpu.make_async_copy(r.wdown.at[t], r.wdown_v, r.w_sem.at[2 * t + 1]),
        ]
        for t in range(TOWERS)
    ]

    def transpose_into(dst, src, rows, cols):
        for at in range(0, rows, TILE):
            size = min(TILE, rows - at)
            dst[:cols, at : at + size] = src[at : at + size, :].T

    def stage_in(ref, t, source):
        length, padded = plan.length[t], plan.padded[t]
        for e in range(plan.examples[t]):
            base = e * padded
            if length < padded:
                first = length // 128 * 128
                ref[own, base + first : base + padded] = jnp.zeros((share, padded - first), BF16)
            ref[own, base : base + length] = source[e]

    def param_rows():
        prm = r.prm
        prm[...] = jnp.zeros_like(prm)
        up_bias = r.in_up_b[...].astype(F32)
        for t in range(TOWERS):
            base = t * COLS
            for j in range(2):
                prm[base + j, :] = r.in_gain[t, j, :].astype(F32)
                prm[base + 2 + j, :] = r.in_shift[t, j, :].astype(F32)
                prm[base + 5 + j, :] = r.in_qv_b[t, j, :].astype(F32)
            prm[base + 4, :] = r.in_out_b[t, :].astype(F32)
            prm[base + 7, :] = r.in_down_b[t, :].astype(F32)
            for j in range(hidden // share):
                prm[base + 8 + j, :] = up_bias[t, j * share : (j + 1) * share]
        r.pown[...] = prm[...].T
        r.pfull[own] = r.pown[...].astype(BF16)

    def a_norm(t):
        gain, shift = full_col(t, 0), full_col(t, 2)

        def body(ls):
            x = r.x[t][:, ls].astype(F32)
            mean = jnp.sum(x, axis=0, keepdims=True) / width
            center = x - mean
            inv = lax.rsqrt(jnp.sum(center * center, axis=0, keepdims=True) / width + EPSILON)
            r.n[t][:, ls] = (center * inv * gain + shift).astype(BF16)
            r.row[t][0:1, ls] = mean
            r.row[t][1:2, ls] = inv

        lanes_loop(plan.lanes[t], 128, body)

    def a_qkv(t):
        for copy in attn_w[t]:
            copy.wait()
        bias = jnp.concatenate(
            [own_col(t, 5), jnp.zeros((share, 1), F32), own_col(t, 6)], axis=0
        )

        def body(ls):
            value = nn(r.wqkv_v[t % 2], r.n[t][:, ls]) + bias
            r.qkv[t][:, ls] = value.astype(BF16)

        lanes_loop(plan.lanes[t], TILE, body)

    def valid_keys(t, e):
        if t == 0:
            return plan.length[0]
        if t == 1:
            return r.in_text[e]
        return r.in_pair[e] + (PATCHES + 1)

    def a_heads(t):
        padded = plan.padded[t]
        key_at = lax.broadcasted_iota(jnp.int32, (padded, 1), 0)
        qkv = r.qkv[t]
        r.m[t][: plan.pad] = jnp.zeros((plan.pad, plan.lanes[t]), BF16)
        for e in range(plan.examples[t]):
            base = e * padded
            valid = key_at < valid_keys(t, e)

            def head(h, carry):
                rows_q = block(h, HEAD_DIM)
                rows_k = block(h + heads, HEAD_DIM)
                rows_v = block(h + 2 * heads, HEAD_DIM)
                rows_m = block(h + plan.pad // HEAD_DIM, HEAD_DIM)
                keys = qkv[rows_k, base : base + padded].T
                values = qkv[rows_v, base : base + padded]
                for q in range(padded // TILE):
                    at = base + q * TILE
                    s = nn(keys, qkv[rows_q, at : at + TILE]) * (HEAD_DIM**-0.5)
                    s = jnp.where(valid, s, -1000000000.0)
                    p = jnp.exp(s - jnp.max(s, axis=0, keepdims=True))
                    p = (p * (1.0 / jnp.sum(p, axis=0, keepdims=True))).astype(BF16)
                    r.p[t][e * heads + h, :, q * TILE : (q + 1) * TILE] = p
                    r.m[t][rows_m, at : at + TILE] = nn(values, p).astype(BF16)
                return carry

            lax.fori_loop(0, heads, head, 0)

    def a_out(t):
        transpose_into(r.work_a, r.wout_v.at[t % 2], share, width)

        def body(ls):
            mixed = r.m[t][plan.pad :, ls]
            r.part[t][:, ls] = nn(r.work_a[:, :share], mixed).astype(BF16)

        lanes_loop(plan.lanes[t], TILE, body)
        ar1[t].begin()
        for copy in attn_w[t + 2]:
            copy.start()

    def b_prep(t):
        for copy in ffn_w[t]:
            copy.wait()
        transpose_into(r.up_t, r.wup_v, width, hidden)
        transpose_into(r.down_t, r.wdown_v, hidden, width)

    def b_main(t):
        out_bias, gain, shift = full_col(t, 4), full_col(t, 1), full_col(t, 3)
        up_bias = jnp.concatenate([own_col(t, 8 + j) for j in range(hidden // share)], axis=0)
        ar1[t].free()

        def body(ls):
            x, s = r.x[t], r.sums[FIRST][t]
            resid = x[:, ls].astype(F32) + (s[:, ls].astype(F32) + out_bias)
            r.own[t][:, ls] = x[own, ls].astype(F32) + (s[own, ls].astype(F32) + own_col(t, 4))
            mean = jnp.sum(resid, axis=0, keepdims=True) / width
            center = resid - mean
            inv = lax.rsqrt(jnp.sum(center * center, axis=0, keepdims=True) / width + EPSILON)
            xhat = center * inv
            r.row[t][2:3, ls] = inv
            normed = (xhat * gain + shift).astype(BF16)
            s[:, ls] = xhat.astype(BF16)
            r.work_n[:, ls] = normed
            h = nn(r.up_t[...], normed) + up_bias
            cdf = 0.5 * (1.0 + lax.erf(h * INV_SQRT2))
            r.work_a[:, ls] = (h * cdf).astype(BF16)
            slope = cdf + h * (jnp.exp(-0.5 * (h * h)) * INV_SQRT_2PI)
            dact = nn(r.wdown_v[...], r.dy[t][:, ls])
            dhid = (dact * slope).astype(BF16)
            r.work_h[:hidden, ls] = dhid
            r.part[t][:, ls] = nn(r.wup_v[...], dhid).astype(BF16)

        lanes_loop(plan.lanes[t], TILE, body)
        ar2[t].begin()
        if t + 1 < TOWERS:
            for copy in ffn_w[t + 1]:
                copy.start()

    def b_ffn(t):
        def body(ls):
            r.rpart[t][:, ls] = nn(r.down_t[...], r.work_a[:, ls]).astype(BF16)

        lanes_loop(plan.lanes[t], TILE, body)
        rs1[t].begin()

    def spread(dst, value, ls):
        for b in range(plan.halves * nz):
            part = value[b * plan.slab : (b + 1) * plan.slab].astype(BF16)
            dst[b % plan.halves, b // plan.halves, :, ls] = part

    def grad_loop(unit, lhs, rhs):
        dst = unit.all

        def step(at, carry):
            rows = block(at, TILE)
            spread(dst, nt(lhs(), rhs(rows)), rows)
            return carry

        lax.fori_loop(0, hidden // TILE, step, 0)
        unit.send()

    def b_up(t):
        lanes = plan.lanes[t]
        grad_loop(
            unit_of[t, UP], lambda: r.work_n[:, :lanes], lambda rows: r.work_h[rows, :lanes]
        )

    def b_down(t):
        lanes = plan.lanes[t]
        grad_loop(unit_of[t, DOWN], lambda: r.dy[t][...], lambda rows: r.work_a[rows, :lanes])

    def b_sum(t):
        lanes = plan.lanes[t]
        for j in range(hidden // share):
            keep_sum(t, 3 + j, r.work_h[j * share : (j + 1) * share, :lanes])
        keep_sum(t, 7, r.dy[t][own])

    def y_out(t):
        rs1[t].finish()
        value = r.own[t][...] + (
            r.rpart[t][own].astype(F32) + r.rfar[FIRST][t][...].astype(F32) + own_col(t, 7)
        )
        padded = plan.padded[t]
        for e in range(plan.examples[t]):
            out = value[:, e * padded : e * padded + plan.length[t]]
            r.v_y[t][e] = out.astype(BF16)
        row_copies.append(pltpu.make_async_copy(r.v_y[t], r.o_y[t], r.row_sem.at[t]))
        row_copies[-1].start()

    def c_norm(t):
        for copy in attn_w[TOWERS + t]:
            copy.wait()
        slot = (TOWERS + t) % 2
        gain, gain_own = full_col(t, 1), own_col(t, 1)

        def body(ls):
            dn, xhat = r.sums[SECOND][t], r.sums[FIRST][t]
            xh = xhat[:, ls].astype(F32)
            e = dn[:, ls].astype(F32) * gain
            m1 = jnp.sum(e, axis=0, keepdims=True) / width
            m2 = jnp.sum(e * xh, axis=0, keepdims=True) / width
            inv = r.row[t][2:3, ls]
            dres = r.dy[t][:, ls].astype(F32) + inv * (e - m1 - xh * m2)
            r.work_n[:, ls] = dres.astype(BF16)
            e_own = dn[own, ls].astype(F32) * gain_own
            r.own[t][:, ls] = r.dy[t][own, ls].astype(F32) + inv * (
                e_own - m1 - xhat[own, ls].astype(F32) * m2
            )

        lanes_loop(plan.lanes[t], 128, body)

        def mix(ls):
            r.work_m[:, ls] = nn(r.wout_v[slot], r.work_n[:, ls]).astype(BF16)

        lanes_loop(plan.lanes[t], TILE, mix)

    def c_heads(t):
        padded = plan.padded[t]
        qkv = r.qkv[t]
        scale = HEAD_DIM**-0.5
        for e in range(plan.examples[t]):
            base = e * padded

            def head(h, carry):
                rows_q = block(h, HEAD_DIM)
                rows_k = block(h + heads, HEAD_DIM)
                rows_v = block(h + 2 * heads, HEAD_DIM)
                keys = qkv[rows_k, base : base + padded]
                values = qkv[rows_v, base : base + padded].T
                dk = dv = None
                for q in range(padded // TILE):
                    at = base + q * TILE
                    dm = r.work_m[rows_q, at : at + TILE]
                    p = r.p[t][e * heads + h, :, q * TILE : (q + 1) * TILE]
                    dp = nn(values, dm)
                    pf = p.astype(F32)
                    delta = jnp.sum(pf * dp, axis=0, keepdims=True)
                    ds = (pf * (dp - delta)).astype(BF16)
                    dq = nn(keys, ds) * scale
                    r.work_h[rows_q, at : at + TILE] = dq.astype(BF16)
                    dk_q = nt(qkv[rows_q, at : at + TILE], ds)
                    dv_q = nt(dm, p)
                    dk = dk_q if dk is None else dk + dk_q
                    dv = dv_q if dv is None else dv + dv_q
                r.work_h[rows_k, base : base + padded] = (dk * scale).astype(BF16)
                r.work_h[rows_v, base : base + padded] = dv.astype(BF16)
                return carry

            lax.fori_loop(0, heads, head, 0)

    def c_prep(t):
        transpose_into(r.up_t, r.wqkv_v.at[(TOWERS + t) % 2], 3 * share, width)

    def c_dn(t):
        gain = full_col(t, 0)
        rs1[t].free()
        r.stat_own[t][...] = jnp.zeros_like(r.stat_own[t])

        def body(ls):
            dn = nn(r.up_t[:, : 3 * share], r.work_h[: 3 * share, ls])
            e = dn * gain
            xhat = (r.x[t][:, ls].astype(F32) - r.row[t][0:1, ls]) * r.row[t][1:2, ls]
            r.stat_own[t][0:1, ls] = jnp.sum(e, axis=0, keepdims=True)
            r.stat_own[t][1:2, ls] = jnp.sum(e * xhat, axis=0, keepdims=True)
            r.rpart[t][:, ls] = dn.astype(BF16)

        lanes_loop(plan.lanes[t], TILE, body)
        rs2[t].begin()
        stats[t].begin()
        if t == 0:
            for copy in attn_w[5]:
                copy.start()

    def c_grad(t):
        lanes = plan.lanes[t]
        unit = unit_of[t, ATTN]
        r.work_h[3 * share :, :lanes] = jnp.zeros((width - 3 * share, lanes), BF16)
        whole = 3 * share // TILE

        def step(at, carry):
            rows = block(at, TILE)
            spread(unit.all, nt(r.n[t][...], r.work_h[rows, :lanes]), rows)
            return carry

        lax.fori_loop(0, whole, step, 0)
        last = slice(whole * TILE, (whole + 1) * TILE)
        value = nt(r.n[t][...], r.work_h[last, :lanes])
        value = value + nt(r.work_n[:, :lanes], r.m[t][...])
        spread(unit.all, value, last)
        unit.send()

    def c_sum(t):
        lanes = plan.lanes[t]
        keep_sum(t, 0, r.work_h[:share, :lanes])
        keep_sum(t, 1, r.work_h[2 * share : 3 * share, :lanes])
        keep_sum(t, 2, r.work_n[own, :lanes])
        dn, xhat = r.sums[SECOND][t], r.sums[FIRST][t]
        keep_sum(t, 9, dn[own].astype(F32) * xhat[own].astype(F32))
        keep_sum(t, 11, dn[own])

    def last_norm(t):
        rs2[t].finish()
        stats[t].finish()
        gain = own_col(t, 0)
        dn = r.rpart[t][own].astype(F32) + r.rfar[SECOND][t][...].astype(F32)
        total = r.stat_chip[t][...] + r.stat_far[t][...]
        inv = r.row[t][1:2, :]
        xhat = (r.x[t][own].astype(F32) - r.row[t][0:1, :]) * inv
        value = r.own[t][...] + inv * (
            dn * gain - total[0:1] / width - xhat * (total[1:2] / width)
        )
        padded = plan.padded[t]
        for e in range(plan.examples[t]):
            out = value[:, e * padded : e * padded + plan.length[t]]
            r.v_dx[t][e] = out.astype(BF16)
        row_copies.append(pltpu.make_async_copy(r.v_dx[t], r.o_dx[t], r.row_sem.at[TOWERS + t]))
        row_copies[-1].start()
        keep_sum(t, 8, dn * xhat)
        keep_sum(t, 10, dn)

    def small_send(late):
        rows = r.small[...].T
        first, last = (EARLY, EARLY + LATE) if late else (0, EARLY)
        part = rows[first:last]
        if not plan.fused:
            r.o_rows[first:last] = part
            return
        r.rows[late][0] = part
        small_step(late, 0)

    def small_step(late, step):
        rows, land = r.rows[late].at[step], r.rows_in[late].at[step]
        device = (y_peer, near_dev, far_dev)[step]
        small_copies[late].append(launch(remote(rows, land, device)))

    def small_relay(late, step):
        if not plan.fused:
            return
        small_copies[late][step - 1].wait_recv()
        r.rows[late][step] = r.rows[late][step - 1] + r.rows_in[late][step - 1]
        small_step(late, step)

    def small_finish(late):
        if not plan.fused:
            return
        small_copies[late][2].wait_recv()
        total = r.rows[late][2] + r.rows_in[late][2]
        if late:
            r.o_rows[EARLY : EARLY + LATE] = total
        else:
            r.o_rows[:EARLY] = total

    small_copies = [[], []]

    barrier = pltpu.get_barrier_semaphore()
    partners = [sibling, across]
    if plan.fused:
        partners += [y_peer, near_dev, far_dev]
    for device in partners:
        pl.semaphore_signal(barrier, inc=1, device_id=device, device_id_type=MESH)
    loads = [
        pltpu.make_async_copy(src[t], dst[t], r.in_sem.at[i * TOWERS + t])
        for i, (src, dst) in enumerate(((r.in_x, r.v_y), (r.in_dy, r.v_dx)))
        for t in range(TOWERS)
    ]
    for copy in loads + attn_w[0] + ffn_w[0] + attn_w[1]:
        copy.start()
    param_rows()
    loads[0].wait()
    stage_in(r.x[0], 0, r.v_y[0])
    pl.semaphore_wait(barrier, len(partners))
    gp.start()
    gx[0].start()
    for t in range(1, TOWERS):
        loads[t].wait()
        stage_in(r.x[t], t, r.v_y[t])
    for t in range(TOWERS):
        loads[TOWERS + t].wait()
        stage_in(r.dy[t], t, r.v_dx[t])
    r.small[...] = jnp.zeros_like(r.small)
    gp.forward()
    gp.finish()
    gdy[0].start()
    gx[0].forward()
    gx[1].start()
    gx[0].finish()
    a_norm(0)
    a_qkv(0)
    a_heads(0)
    a_out(0)
    gdy[0].forward()
    ar1[0].cross()
    gx[1].forward()
    gx[1].finish()
    gdy[0].finish()
    a_norm(1)
    a_qkv(1)
    a_heads(1)
    gx[2].start()
    a_out(1)
    b_prep(0)
    ar1[1].cross()
    ar1[0].back()
    ar1[0].finish()
    b_main(0)
    b_down(0)
    b_ffn(0)
    b_sum(0)
    gx[2].forward()
    b_prep(1)
    gdy[1].start()
    gdy[2].start()
    gx[2].finish()
    a_norm(2)
    a_qkv(2)
    b_up(0)
    units[0].relay(0)
    units[0].relay(1)
    a_heads(2)
    units[0].relay(2)
    units[0].relay(3)
    a_out(2)
    ar1[2].cross()
    units[1].relay(0)
    ar1[1].back()
    ar1[1].finish()
    gdy[1].forward()
    gdy[1].finish()
    units[1].relay(1)
    b_main(1)
    units[1].relay(2)
    ar2[0].cross()
    b_down(1)
    b_up(1)
    b_ffn(1)
    units[1].relay(3)
    b_sum(1)
    b_prep(2)
    gdy[2].forward()
    rs1[0].cross()
    ar1[2].back()
    units[0].finish()
    gdy[2].finish()
    ar1[2].finish()
    b_main(2)
    b_down(2)
    rs1[1].cross()
    units[2].relay(0)
    b_sum(2)
    ar2[1].cross()
    units[1].finish()
    ar2[0].back()
    units[3].relay(0)
    y_out(1)
    ar2[2].cross()
    units[3].relay(1)
    b_ffn(2)
    y_out(0)
    units[2].relay(1)
    units[2].relay(2)
    units[4].relay(0)
    units[2].relay(3)
    b_up(2)
    ar2[0].finish()
    units[3].relay(2)
    c_norm(0)
    c_prep(0)
    units[4].relay(1)
    c_heads(0)
    c_sum(0)
    c_dn(0)
    ar2[1].back()
    units[4].relay(2)
    units[2].finish()
    units[3].relay(3)
    units[5].relay(0)
    ar2[1].finish()
    rs1[2].cross()
    c_grad(0)
    c_norm(1)
    c_prep(1)
    c_heads(1)
    c_dn(1)
    units[4].relay(3)
    rs2[0].cross()
    units[3].finish()
    c_sum(1)
    ar2[2].back()
    units[5].relay(1)
    c_grad(1)
    units[6].relay(0)
    y_out(2)
    rs2[1].cross()
    stats[0].cross()
    ar2[2].finish()
    c_norm(2)
    units[4].finish()
    units[6].relay(1)
    units[5].relay(2)
    c_heads(2)
    last_norm(0)
    c_prep(2)
    units[7].relay(0)
    stats[1].cross()
    c_dn(2)
    rs2[2].cross()
    units[6].relay(2)
    c_sum(2)
    units[5].relay(3)
    last_norm(1)
    small_send(0)
    c_grad(2)
    units[7].relay(1)
    units[7].relay(2)
    stats[2].cross()
    last_norm(2)
    units[6].relay(3)
    small_send(1)
    units[6].finish()
    units[5].finish()
    small_relay(0, 1)
    units[8].relay(0)
    small_relay(0, 2)
    units[8].relay(1)
    small_relay(1, 1)
    units[8].relay(2)
    units[8].relay(3)
    units[7].relay(3)
    units[7].finish()
    small_relay(1, 2)
    small_finish(0)
    units[8].finish()
    small_finish(1)
    for copy in list(pending):
        sent(copy)
    for unit in units:
        for copy in unit.hbm:
            copy.wait()
    for copy in row_copies:
        copy.wait()


def deliver(*refs):
    count = 2 * TOWERS + 4
    src, rows = refs[:count], refs[count]
    dst = refs[count + 1 : 2 * count + 1]
    qvb, outb, upb, downb, gains, shifts = refs[2 * count + 1 : 2 * count + 7]
    room = refs[2 * count + 7 : 3 * count + 7]
    in_sem, out_sem = refs[3 * count + 7 :]
    reads = [pltpu.make_async_copy(src[i], room[i], in_sem.at[i]) for i in range(count)]
    writes = [pltpu.make_async_copy(room[i], dst[i], out_sem.at[i]) for i in range(count)]
    for copy in reads:
        copy.start()
    share = rows.shape[1]
    for t in range(TOWERS):
        for j in range(2):
            qvb[t, j, :] = rows[small_row(t, j), :]
            gains[t, j, :] = rows[small_row(t, 8 + j), :]
            shifts[t, j, :] = rows[small_row(t, 10 + j), :]
        outb[t, :] = rows[small_row(t, 2), :]
        downb[t, :] = rows[small_row(t, 7), :]
        for j in range(upb.shape[1] // share):
            upb[t, j * share : (j + 1) * share] = rows[small_row(t, 3 + j), :]
    for read, write in zip(reads, writes):
        read.wait()
        write.start()
    for copy in writes:
        copy.wait()


def per_device(dp, tensor, *args):
    rows, ups = args[0:3], args[15:18]
    text_lengths, pair_lengths = args[3:5]
    qkv_w, qv_b, out_w, out_b, up_w, up_b, down_w, down_b, gain, shift = args[5:15]
    plan = Plan(rows, (qkv_w, out_w, up_w), dp, tensor)
    width, share, hidden = plan.width, plan.share, plan.hidden
    nz = plan.nz

    turned = [jnp.transpose(x, (0, 2, 1)) for x in rows]
    turned_up = [jnp.transpose(x, (0, 2, 1)) for x in ups]
    wqkv = jnp.transpose(qkv_w, (0, 2, 3, 1)).reshape(TOWERS, 3 * share, width)
    vmem = pl.BlockSpec(memory_space=pltpu.VMEM)
    hbm = pl.BlockSpec(memory_space=pl.ANY)
    smem = pl.BlockSpec(memory_space=pltpu.SMEM)

    ins, specs = SimpleNamespace(), SimpleNamespace()
    ins.in_x, specs.in_x = turned, [hbm] * TOWERS
    ins.in_dy, specs.in_dy = turned_up, [hbm] * TOWERS
    ins.in_text, specs.in_text = text_lengths, smem
    ins.in_pair, specs.in_pair = pair_lengths, smem
    ins.in_gain, specs.in_gain = gain, vmem
    ins.in_shift, specs.in_shift = shift, vmem
    ins.in_out_b, specs.in_out_b = out_b, vmem
    ins.in_qv_b, specs.in_qv_b = qv_b, vmem
    ins.in_down_b, specs.in_down_b = down_b, vmem
    ins.in_up_b, specs.in_up_b = up_b, vmem
    ins.wqkv, specs.wqkv = wqkv, hbm
    ins.wout, specs.wout = out_w, hbm
    ins.wup, specs.wup = up_w, hbm
    ins.wdown, specs.wdown = down_w, hbm

    outs = SimpleNamespace()
    outs.o_y = [Out(hbm, x.shape, BF16) for x in turned]
    outs.o_dx = [Out(hbm, x.shape, BF16) for x in turned]
    if plan.fused:
        outs.o_qkv = Out(hbm, (TOWERS, 3, plan.slab, share))
        outs.o_out = Out(hbm, (TOWERS, share, plan.slab))
        outs.o_up = Out(hbm, (TOWERS, plan.slab, hidden))
        outs.o_down = Out(hbm, (TOWERS, plan.slab, hidden))
    else:
        outs.o_g = Out(hbm, (3, TOWERS, width, width), BF16)
    outs.o_rows = Out(vmem, (SMALL, share))

    room = scratch(plan)
    in_refs, in_tree = flatten(vars(ins))
    out_refs, out_tree = flatten(vars(outs))
    room_refs, room_tree = flatten(vars(room))

    def body(*refs):
        first, second = len(in_refs), len(in_refs) + len(out_refs)
        r = SimpleNamespace()
        vars(r).update(jax.tree.unflatten(in_tree, refs[:first]))
        vars(r).update(jax.tree.unflatten(out_tree, refs[first:second]))
        vars(r).update(jax.tree.unflatten(room_tree, refs[second:]))
        kernel(plan, r)

    results = pl.pallas_call(
        body,
        out_shape=[jax.ShapeDtypeStruct(out.shape, out.dtype) for out in out_refs],
        in_specs=flatten(vars(specs))[0],
        out_specs=[out.spec for out in out_refs],
        scratch_shapes=room_refs,
        compiler_params=pltpu.CompilerParams(
            collective_id=1, has_side_effects=True, vmem_limit_bytes=67043328
        ),
        name="layer",
    )(*in_refs)
    got = SimpleNamespace(**jax.tree.unflatten(out_tree, results))

    if not plan.fused:
        sums = lax.psum_scatter(got.o_g.astype(F32), "dp", scatter_dimension=2, tiled=True)
        got.o_up, got.o_down = sums[UP], sums[DOWN]
        qkv = sums[ATTN, :, :, : 3 * share].reshape(TOWERS, sums.shape[2], 3, share)
        got.o_qkv = jnp.transpose(qkv, (0, 2, 1, 3))
        got.o_out = jnp.transpose(sums[ATTN, :, :, 3 * share :], (0, 2, 1))
        got.o_rows = lax.psum(got.o_rows, "dp")

    big = [*got.o_y, *got.o_dx, got.o_qkv, got.o_out, got.o_up, got.o_down]
    pairs = jax.ShapeDtypeStruct((TOWERS, 2, share), F32)
    single = jax.ShapeDtypeStruct((TOWERS, share), F32)
    small = [pairs, single, jax.ShapeDtypeStruct((TOWERS, hidden), F32), single, pairs, pairs]
    count = len(big)
    results = pl.pallas_call(
        deliver,
        out_shape=[jax.ShapeDtypeStruct(x.shape, x.dtype) for x in big] + small,
        in_specs=[hbm] * count + [vmem],
        out_specs=[hbm] * count + [vmem] * len(small),
        scratch_shapes=[pltpu.VMEM(x.shape, x.dtype) for x in big]
        + [pltpu.SemaphoreType.DMA((count,)), pltpu.SemaphoreType.DMA((count,))],
        compiler_params=pltpu.CompilerParams(vmem_limit_bytes=67043328),
    )(*big, got.o_rows)
    rows, sums = results[: 2 * TOWERS], results[2 * TOWERS : count]
    qvb, outb, upb, downb, gains, shifts = results[count:]
    return (
        *[jnp.transpose(x, (0, 2, 1)) for x in rows],
        jnp.transpose(sums[0], (0, 2, 1, 3)),
        qvb,
        sums[1],
        outb,
        sums[2],
        upb,
        jnp.transpose(sums[3], (0, 2, 1)),
        downb,
        gains,
        shifts,
    )


def solution(mesh):
    dp, tensor = mesh.shape["dp"], mesh.shape["tensor"]

    def step(*args):
        return per_device(dp, tensor, *args)

    rows = P("dp", None, "tensor")
    return jax.shard_map(
        step,
        mesh=mesh,
        in_specs=(
            rows,
            rows,
            rows,
            P("dp"),
            P("dp"),
            P(None, None, None, "tensor"),
            P(None, None, "tensor"),
            P(None, "tensor", None),
            P(None, "tensor"),
            P(None, None, "tensor"),
            P(None, "tensor"),
            P(None, "tensor", None),
            P(None, "tensor"),
            P(None, None, "tensor"),
            P(None, None, "tensor"),
            rows,
            rows,
            rows,
        ),
        out_specs=(
            rows,
            rows,
            rows,
            rows,
            rows,
            rows,
            P(None, "dp", None, "tensor"),
            P(None, None, "tensor"),
            P(None, "tensor", "dp"),
            P(None, "tensor"),
            P(None, "dp", "tensor"),
            P(None, "tensor"),
            P(None, "tensor", "dp"),
            P(None, "tensor"),
            P(None, None, "tensor"),
            P(None, None, "tensor"),
        ),
        check_vma=False,
    )
```

```python
from types import SimpleNamespace

import jax
import jax.numpy as jnp
from jax import lax
from jax.experimental import pallas as pl
from jax.experimental.pallas import tpu as pltpu
from jax.sharding import PartitionSpec as P

HEAD_DIM = 64
PATCHES = 196
EPSILON = 1e-06
TOWERS = 3
FIRST, SECOND = 0, 1
UP, DOWN, ATTN = 0, 1, 2
RING = 3
UNITS = (
    (0, DOWN),
    (0, UP),
    (1, DOWN),
    (1, UP),
    (2, DOWN),
    (2, UP),
    (0, ATTN),
    (1, ATTN),
    (2, ATTN),
)
Z_FIRST = (2,)
TILE = 256
COLS = 12
N_REMOTE = 132
EARLY, LATE = 32, 8
SMALL = EARLY + LATE
LATE_COLS = (0, 1, 2, 8, 9, 10, 11)
BF16 = jnp.bfloat16
F32 = jnp.float32
MESH = pl.DeviceIdType.MESH
INV_SQRT2 = 0.7071067811865476
INV_SQRT_2PI = 0.3989422804014327


def nn(a, b):
    return lax.dot_general(a, b, (((1,), (0,)), ((), ())), preferred_element_type=F32)


def nt(a, b):
    return lax.dot_general(a, b, (((1,), (1,)), ((), ())), preferred_element_type=F32)


def up(value, multiple):
    return -(-value // multiple) * multiple


class Plan:
    def __init__(self, rows, weights, dp, tensor):
        qkv, out, upw = weights
        self.dp = dp
        self.examples = [r.shape[0] for r in rows]
        self.length = [r.shape[1] for r in rows]
        self.padded = [up(n, TILE) for n in self.length]
        self.lanes = [e * n for e, n in zip(self.examples, self.padded)]
        self.width = qkv.shape[1]
        self.share = out.shape[1]
        self.hidden = upw.shape[2]
        self.heads = self.share // HEAD_DIM
        self.pad = (3 * self.share) % TILE
        assert tensor == 4 and self.width == 4 * self.share
        assert self.pad + self.share == TILE and self.hidden == self.width
        self.fused = dp == 8 and self.width % (16 * dp) == 0
        self.nz = dp // 2 if self.fused else 1
        self.slab = self.width // dp if self.fused else self.width
        self.halves = 2 if self.fused else 1


def small_row(t, j):
    if t < TOWERS - 1:
        return t * COLS + j
    if j in LATE_COLS:
        return EARLY + LATE_COLS.index(j)
    return t * COLS + [c for c in range(COLS) if c not in LATE_COLS].index(j)


class Out:
    def __init__(self, spec, shape, dtype=F32):
        self.spec, self.shape, self.dtype = spec, shape, dtype


def flatten(tree):
    return jax.tree.flatten(tree, is_leaf=lambda v: not isinstance(v, (dict, list)))


def scratch(plan):
    width, share, hidden, nz = plan.width, plan.share, plan.hidden, plan.nz
    half, most = width // 2, max(plan.lanes)
    dma = pltpu.SemaphoreType.DMA

    def vm(*shape, dtype=BF16):
        return pltpu.VMEM(shape, dtype)

    def each(*lead, dtype=BF16):
        return [pltpu.VMEM((*lead, lanes), dtype) for lanes in plan.lanes]

    k = SimpleNamespace()
    k.x, k.dy, k.n = each(width), each(width), each(width)
    k.sums = [each(width), each(width)]
    k.part, k.rpart = each(width), each(width)
    k.qkv, k.m = each(3 * share), each(TILE)
    k.p = [vm(e * plan.heads, n, n) for e, n in zip(plan.examples, plan.padded)]
    k.near, k.far = each(half), [each(half), each(half)]
    k.rnear, k.rfar = each(2, share), [each(share), each(share)]
    k.own, k.row = each(share, dtype=F32), each(8, dtype=F32)
    k.stat_own, k.stat_near = each(8, dtype=F32), each(8, dtype=F32)
    k.stat_chip, k.stat_far = each(8, dtype=F32), each(8, dtype=F32)
    k.g_all = vm(RING, plan.halves, nz, plan.slab, width)
    k.credit = pltpu.SemaphoreType.REGULAR((RING,))
    k.out_sem = dma((4,))
    if plan.fused:
        k.g_y = vm(RING, nz, plan.slab, width)
        k.g_z = vm(RING, nz, plan.slab, width)
        k.g_far = vm(len(UNITS), 3, plan.slab, width)
        k.zf_near = vm(2, 2, plan.slab, width)
        k.zf_far, k.zf_y = vm(2, plan.slab, width), vm(plan.slab, width)
        k.s_ffn = vm(2, plan.slab, hidden, dtype=F32)
        k.s_qkv = vm(3, plan.slab, share, dtype=F32)
        k.s_out = vm(share, plan.slab, dtype=F32)
        k.rows = [vm(3, n, share, dtype=F32) for n in (EARLY, LATE)]
        k.rows_in = [vm(3, n, share, dtype=F32) for n in (EARLY, LATE)]
    k.wqkv_v, k.wout_v = vm(2, 3 * share, width), vm(2, share, width)
    k.wup_v, k.wdown_v = vm(width, hidden), vm(hidden, width)
    k.up_t, k.down_t = vm(hidden, width), vm(width, hidden)
    k.work_n, k.work_a = vm(width, most), vm(hidden, most)
    k.work_h, k.work_m = vm(width, most), vm(share, most)
    k.pown, k.pfull = vm(share, 128, dtype=F32), vm(width, 128)
    k.prm, k.small = vm(128, share, dtype=F32), vm(share, 128, dtype=F32)
    k.v_y = [vm(e, share, n) for e, n in zip(plan.examples, plan.length)]
    k.v_dx = [vm(e, share, n) for e, n in zip(plan.examples, plan.length)]
    k.row_sem = dma((2 * TOWERS,))
    k.in_sem, k.w_sem, k.part_sem = dma((2 * TOWERS,)), dma((18,)), dma(())
    k.send_sem, k.recv_sem = dma((N_REMOTE,)), dma((N_REMOTE,))
    return k


def kernel(plan, r):
    width, share, hidden, heads = plan.width, plan.share, plan.hidden, plan.heads
    half = width // 2
    nz = plan.nz

    dp_at = lax.axis_index("dp")
    me = lax.axis_index("tensor")
    core = lax.rem(me, 2)
    chip = lax.div(me, 2)
    y_at = lax.rem(dp_at, 2)
    z_at = lax.div(dp_at, 2)
    sibling = (dp_at, me + 1 - 2 * core)
    across = (dp_at, lax.rem(me + 2, 4))
    y_peer = (dp_at + 1 - 2 * y_at, me)

    z_near = z_at + 1 - 2 * lax.rem(z_at, 2)
    z_far, z_near_far = lax.rem(z_at + 2, 4), lax.rem(z_near + 2, 4)
    near_dev, far_dev = (z_near * 2 + y_at, me), (z_far * 2 + y_at, me)

    row_copies = []
    counter = [0]
    pending = []

    def remote(src, dst, device):
        at = counter[0]
        counter[0] += 1
        assert at < N_REMOTE
        return pltpu.make_async_remote_copy(
            src_ref=src,
            dst_ref=dst,
            send_sem=r.send_sem.at[at],
            recv_sem=r.recv_sem.at[at],
            device_id=device,
            device_id_type=MESH,
        )

    def launch(copy):
        copy.start()
        pending.append(copy)
        return copy

    def sent(copy):
        copy.wait_send()
        pending[:] = [other for other in pending if other is not copy]

    def block(at, size):
        return pl.ds(pl.multiple_of(at * size, size), size)

    own = block(me, share)
    my_half, other_half = block(core, half), block(1 - core, half)

    def lanes_loop(lanes, tile, body):
        def step(at, carry):
            body(block(at, tile))
            return carry

        lax.fori_loop(0, lanes // tile, step, 0)

    lane_of_small = lax.broadcasted_iota(jnp.int32, (share, 128), 1)

    def keep_sum(t, j, value):
        column = jnp.sum(value.astype(F32), axis=1, keepdims=True)
        small = r.small
        small[...] = jnp.where(lane_of_small == small_row(t, j), column, small[...])

    def own_col(t, j):
        return r.pown[:, t * COLS + j : t * COLS + j + 1]

    def full_col(t, j):
        return r.pfull[...].astype(F32)[:, t * COLS + j : t * COLS + j + 1]

    class Gather:
        def __init__(self, buf):
            self.to_sibling = remote(buf.at[own], buf.at[own], sibling)
            self.to_across = remote(buf.at[own], buf.at[own], across)
            blk = block(lax.rem(me + 2, 4), share)
            self.forwarded = remote(buf.at[blk], buf.at[blk], sibling)

        def start(self):
            launch(self.to_across)
            launch(self.to_sibling)

        def forward(self):
            self.to_across.wait_recv()
            launch(self.forwarded)

        def finish(self):
            self.to_sibling.wait_recv()
            self.forwarded.wait_recv()

    class AllReduce:
        def __init__(self, t, which):
            self.part, self.near = r.part[t], r.near[t]
            self.far, self.out = r.far[which][t], r.sums[which][t]
            self.c1 = remote(self.part.at[other_half], self.near, sibling)
            self.c2 = remote(self.part.at[my_half], self.far, across)
            self.c3 = remote(self.out.at[my_half], self.out.at[my_half], sibling)

        def begin(self):
            launch(self.c1)

        def cross(self):
            self.c1.wait_recv()
            total = self.part[my_half].astype(F32) + self.near[...].astype(F32)
            self.part[my_half] = total.astype(BF16)
            launch(self.c2)

        def back(self):
            self.c2.wait_recv()
            total = self.part[my_half].astype(F32) + self.far[...].astype(F32)
            self.out[my_half] = total.astype(BF16)
            launch(self.c3)

        def finish(self):
            self.c3.wait_recv()

        def free(self):
            sent(self.c1)
            sent(self.c2)
            sent(self.c3)

    class Scatter:
        def __init__(self, t, which):
            self.part, self.near, self.far = r.rpart[t], r.rnear[t], r.rfar[which][t]
            self.far_blk = block(2 * (1 - chip) + core, share)
            theirs = (2 * (1 - chip) + 1 - core, 2 * chip + 1 - core)
            self.c1 = [
                remote(self.part.at[block(theirs[j], share)], self.near.at[j], sibling)
                for j in range(2)
            ]
            self.c2 = remote(self.part.at[self.far_blk], self.far, across)

        def begin(self):
            for copy in self.c1:
                launch(copy)

        def cross(self):
            self.c1[0].wait_recv()
            blk = self.far_blk
            self.part[blk] = (self.part[blk].astype(F32) + self.near[0].astype(F32)).astype(BF16)
            launch(self.c2)
            self.c1[1].wait_recv()
            self.part[own] = (self.part[own].astype(F32) + self.near[1].astype(F32)).astype(BF16)

        def finish(self):
            self.c2.wait_recv()

        def free(self):
            for copy in self.c1:
                sent(copy)
            sent(self.c2)

    class Stats:
        def __init__(self, t):
            self.c1 = remote(r.stat_own[t], r.stat_near[t], sibling)
            self.c2 = remote(r.stat_chip[t], r.stat_far[t], across)
            self.t = t

        def begin(self):
            launch(self.c1)

        def cross(self):
            t = self.t
            self.c1.wait_recv()
            r.stat_chip[t][...] = r.stat_own[t][...] + r.stat_near[t][...]
            launch(self.c2)

        def finish(self):
            self.c2.wait_recv()

    class Unit:
        def __init__(self, at, t, kind):
            self.at, self.t, self.kind = at, t, kind
            self.slot = at % RING
            self.all = r.g_all.at[self.slot]
            self.sums = r.g_z.at[self.slot] if plan.fused else None
            self.first, self.z_copies, self.hbm = [], [], []
            self.z_first = at in Z_FIRST

        def across_z(self, src, dst, device):
            self.z_copies.append(launch(remote(src, dst, device)))

        def send(self):
            if not plan.fused:
                dst = r.o_g.at[self.kind, self.t]
                copy = pltpu.make_async_copy(self.all.at[0, 0], dst, r.part_sem)
                copy.start()
                copy.wait()
                return
            if self.at >= RING:
                pl.semaphore_wait(r.credit.at[self.slot], 1)
            if self.z_first:
                for i, blk in enumerate((z_near_far, z_near)):
                    for yy in range(2):
                        dst = r.zf_near.at[i, yy]
                        self.first.append(launch(remote(self.all.at[yy, blk], dst, near_dev)))
                return
            for blk in (z_near_far, z_near, z_far, z_at):
                src, dst = self.all.at[1 - y_at, blk], r.g_y.at[self.slot, blk]
                self.first.append(launch(remote(src, dst, y_peer)))

        def relay(self, step):
            if not plan.fused:
                return
            if step == 0 and self.at >= RING:
                for copy in units[self.at - RING].z_copies:
                    sent(copy)
            if self.z_first:
                self.relay_z(step)
            else:
                self.relay_y(step)
            if step == 3:
                for copy in self.first:
                    sent(copy)
                if self.at + RING < len(units):
                    credit = r.credit.at[self.slot]
                    pl.semaphore_signal(credit, inc=1, device_id=y_peer, device_id_type=MESH)

        def relay_y(self, step):
            blk = (z_near_far, z_near, z_far, z_at)[step]
            self.first[step].wait_recv()
            total = self.all[y_at, blk].astype(F32) + r.g_y[self.slot, blk].astype(F32)
            land = r.g_far.at[self.at]
            if step == 2:
                self.z_copies[0].wait_recv()
                total = total + r.g_far[self.at, 1].astype(F32)
            self.sums[blk] = total.astype(BF16)
            if step == 0:
                self.across_z(self.sums.at[blk], land.at[1], near_dev)
            if step == 1:
                self.across_z(self.sums.at[blk], land.at[0], near_dev)
            if step == 2:
                self.across_z(self.sums.at[blk], land.at[2], far_dev)

        def relay_z(self, step):
            def known(i, yy, blk):
                return self.all[yy, blk].astype(F32) + r.zf_near[i, yy].astype(F32)

            if step == 0:
                for yy in range(2):
                    self.first[yy].wait_recv()
                    self.sums[yy] = known(0, yy, z_far).astype(BF16)
                    self.across_z(self.sums.at[yy], r.zf_far.at[yy], far_dev)
            if step == 1:
                for yy in range(2):
                    self.first[2 + yy].wait_recv()
                    self.z_copies[yy].wait_recv()
                for at, yy in ((2, 1 - y_at), (3, y_at)):
                    total = known(1, yy, z_at) + r.zf_far[yy].astype(F32)
                    self.sums[at] = total.astype(BF16)
                self.across_z(self.sums.at[2], r.zf_y, y_peer)

        def finish(self):
            if not plan.fused:
                return
            if self.z_first:
                self.z_copies[2].wait_recv()
                total = self.sums[3].astype(F32) + r.zf_y[...].astype(F32)
            else:
                self.z_copies[1].wait_recv()
                self.z_copies[2].wait_recv()
                total = self.sums[z_at].astype(F32)
                for i in (0, 2):
                    total = total + r.g_far[self.at, i].astype(F32)
            t, sem = self.t, r.out_sem
            for before in units[: self.at]:
                if before.kind == self.kind:
                    for copy in before.hbm:
                        copy.wait()
                    before.hbm = []
            if self.kind == UP or self.kind == DOWN:
                out = r.o_up if self.kind == UP else r.o_down
                r.s_ffn[self.kind] = total
                self.hbm = [pltpu.make_async_copy(r.s_ffn.at[self.kind], out.at[t], sem.at[self.kind])]
            else:
                for c in range(3):
                    r.s_qkv[c] = total[:, c * share : (c + 1) * share]
                r.s_out[...] = total[:, 3 * share :].T
                self.hbm = [
                    pltpu.make_async_copy(r.s_qkv, r.o_qkv.at[t], sem.at[2]),
                    pltpu.make_async_copy(r.s_out, r.o_out.at[t], sem.at[3]),
                ]
            for copy in self.hbm:
                copy.start()

    gx = [Gather(r.x[t]) for t in range(TOWERS)]
    gdy = [Gather(r.dy[t]) for t in range(TOWERS)]
    gp = Gather(r.pfull)
    ar1 = [AllReduce(t, FIRST) for t in range(TOWERS)]
    ar2 = [AllReduce(t, SECOND) for t in range(TOWERS)]
    rs1 = [Scatter(t, FIRST) for t in range(TOWERS)]
    rs2 = [Scatter(t, SECOND) for t in range(TOWERS)]
    stats = [Stats(t) for t in range(TOWERS)]
    units = []
    for at, (t, kind) in enumerate(UNITS):
        units.append(Unit(at, t, kind))
    unit_of = {(unit.t, unit.kind): unit for unit in units}

    def attn_load(use):
        t, slot = use % TOWERS, use % 2
        pairs = ((r.wqkv, r.wqkv_v), (r.wout, r.wout_v))
        return [
            pltpu.make_async_copy(src.at[t], dst.at[slot], r.w_sem.at[6 + 2 * use + i])
            for i, (src, dst) in enumerate(pairs)
        ]

    attn_w = [attn_load(use) for use in range(2 * TOWERS)]
    ffn_w = [
        [
            pltpu.make_async_copy(r.wup.at[t], r.wup_v, r.w_sem.at[2 * t]),
            pltpu.make_async_copy(r.wdown.at[t], r.wdown_v, r.w_sem.at[2 * t + 1]),
        ]
        for t in range(TOWERS)
    ]

    def transpose_into(dst, src, rows, cols):
        for at in range(0, rows, TILE):
            size = min(TILE, rows - at)
            dst[:cols, at : at + size] = src[at : at + size, :].T

    def stage_in(ref, t, source):
        length, padded = plan.length[t], plan.padded[t]
        for e in range(plan.examples[t]):
            base = e * padded
            if length < padded:
                first = length // 128 * 128
                ref[own, base + first : base + padded] = jnp.zeros((share, padded - first), BF16)
            ref[own, base : base + length] = source[e]

    def param_rows():
        prm = r.prm
        prm[...] = jnp.zeros_like(prm)
        up_bias = r.in_up_b[...].astype(F32)
        for t in range(TOWERS):
            base = t * COLS
            for j in range(2):
                prm[base + j, :] = r.in_gain[t, j, :].astype(F32)
                prm[base + 2 + j, :] = r.in_shift[t, j, :].astype(F32)
                prm[base + 5 + j, :] = r.in_qv_b[t, j, :].astype(F32)
            prm[base + 4, :] = r.in_out_b[t, :].astype(F32)
            prm[base + 7, :] = r.in_down_b[t, :].astype(F32)
            for j in range(hidden // share):
                prm[base + 8 + j, :] = up_bias[t, j * share : (j + 1) * share]
        r.pown[...] = prm[...].T
        r.pfull[own] = r.pown[...].astype(BF16)

    def a_norm(t):
        gain, shift = full_col(t, 0), full_col(t, 2)

        def body(ls):
            x = r.x[t][:, ls].astype(F32)
            mean = jnp.sum(x, axis=0, keepdims=True) / width
            center = x - mean
            inv = lax.rsqrt(jnp.sum(center * center, axis=0, keepdims=True) / width + EPSILON)
            r.n[t][:, ls] = (center * inv * gain + shift).astype(BF16)
            r.row[t][0:1, ls] = mean
            r.row[t][1:2, ls] = inv

        lanes_loop(plan.lanes[t], 128, body)

    def a_qkv(t):
        for copy in attn_w[t]:
            copy.wait()
        bias = jnp.concatenate(
            [own_col(t, 5), jnp.zeros((share, 1), F32), own_col(t, 6)], axis=0
        )

        def body(ls):
            value = nn(r.wqkv_v[t % 2], r.n[t][:, ls]) + bias
            r.qkv[t][:, ls] = value.astype(BF16)

        lanes_loop(plan.lanes[t], TILE, body)

    def valid_keys(t, e):
        if t == 0:
            return plan.length[0]
        if t == 1:
            return r.in_text[e]
        return r.in_pair[e] + (PATCHES + 1)

    def a_heads(t):
        padded = plan.padded[t]
        key_at = lax.broadcasted_iota(jnp.int32, (padded, 1), 0)
        qkv = r.qkv[t]
        r.m[t][: plan.pad] = jnp.zeros((plan.pad, plan.lanes[t]), BF16)
        for e in range(plan.examples[t]):
            base = e * padded
            valid = key_at < valid_keys(t, e)

            def head(h, carry):
                rows_q = block(h, HEAD_DIM)
                rows_k = block(h + heads, HEAD_DIM)
                rows_v = block(h + 2 * heads, HEAD_DIM)
                rows_m = block(h + plan.pad // HEAD_DIM, HEAD_DIM)
                keys = qkv[rows_k, base : base + padded].T
                values = qkv[rows_v, base : base + padded]
                for q in range(padded // TILE):
                    at = base + q * TILE
                    s = nn(keys, qkv[rows_q, at : at + TILE]) * (HEAD_DIM**-0.5)
                    s = jnp.where(valid, s, -1000000000.0)
                    p = jnp.exp(s - jnp.max(s, axis=0, keepdims=True))
                    p = (p * (1.0 / jnp.sum(p, axis=0, keepdims=True))).astype(BF16)
                    r.p[t][e * heads + h, :, q * TILE : (q + 1) * TILE] = p
                    r.m[t][rows_m, at : at + TILE] = nn(values, p).astype(BF16)
                return carry

            lax.fori_loop(0, heads, head, 0)

    def a_out(t):
        transpose_into(r.work_a, r.wout_v.at[t % 2], share, width)

        def body(ls):
            mixed = r.m[t][plan.pad :, ls]
            r.part[t][:, ls] = nn(r.work_a[:, :share], mixed).astype(BF16)

        lanes_loop(plan.lanes[t], TILE, body)
        ar1[t].begin()
        for copy in attn_w[t + 2]:
            copy.start()

    def b_prep(t):
        for copy in ffn_w[t]:
            copy.wait()
        transpose_into(r.up_t, r.wup_v, width, hidden)
        transpose_into(r.down_t, r.wdown_v, hidden, width)

    def b_main(t):
        out_bias, gain, shift = full_col(t, 4), full_col(t, 1), full_col(t, 3)
        up_bias = jnp.concatenate([own_col(t, 8 + j) for j in range(hidden // share)], axis=0)
        ar1[t].free()

        def body(ls):
            x, s = r.x[t], r.sums[FIRST][t]
            resid = x[:, ls].astype(F32) + (s[:, ls].astype(F32) + out_bias)
            r.own[t][:, ls] = x[own, ls].astype(F32) + (s[own, ls].astype(F32) + own_col(t, 4))
            mean = jnp.sum(resid, axis=0, keepdims=True) / width
            center = resid - mean
            inv = lax.rsqrt(jnp.sum(center * center, axis=0, keepdims=True) / width + EPSILON)
            xhat = center * inv
            r.row[t][2:3, ls] = inv
            normed = (xhat * gain + shift).astype(BF16)
            s[:, ls] = xhat.astype(BF16)
            r.work_n[:, ls] = normed
            h = nn(r.up_t[...], normed) + up_bias
            cdf = 0.5 * (1.0 + lax.erf(h * INV_SQRT2))
            r.work_a[:, ls] = (h * cdf).astype(BF16)
            slope = cdf + h * (jnp.exp(-0.5 * (h * h)) * INV_SQRT_2PI)
            dact = nn(r.wdown_v[...], r.dy[t][:, ls])
            dhid = (dact * slope).astype(BF16)
            r.work_h[:hidden, ls] = dhid
            r.part[t][:, ls] = nn(r.wup_v[...], dhid).astype(BF16)

        lanes_loop(plan.lanes[t], TILE, body)
        ar2[t].begin()
        if t + 1 < TOWERS:
            for copy in ffn_w[t + 1]:
                copy.start()

    def b_ffn(t):
        def body(ls):
            r.rpart[t][:, ls] = nn(r.down_t[...], r.work_a[:, ls]).astype(BF16)

        lanes_loop(plan.lanes[t], TILE, body)
        rs1[t].begin()

    def spread(dst, value, ls):
        for b in range(plan.halves * nz):
            part = value[b * plan.slab : (b + 1) * plan.slab].astype(BF16)
            dst[b % plan.halves, b // plan.halves, :, ls] = part

    def grad_loop(unit, lhs, rhs):
        dst = unit.all

        def step(at, carry):
            rows = block(at, TILE)
            spread(dst, nt(lhs(), rhs(rows)), rows)
            return carry

        lax.fori_loop(0, hidden // TILE, step, 0)
        unit.send()

    def b_up(t):
        lanes = plan.lanes[t]
        grad_loop(
            unit_of[t, UP], lambda: r.work_n[:, :lanes], lambda rows: r.work_h[rows, :lanes]
        )

    def b_down(t):
        lanes = plan.lanes[t]
        grad_loop(unit_of[t, DOWN], lambda: r.dy[t][...], lambda rows: r.work_a[rows, :lanes])

    def b_sum(t):
        lanes = plan.lanes[t]
        for j in range(hidden // share):
            keep_sum(t, 3 + j, r.work_h[j * share : (j + 1) * share, :lanes])
        keep_sum(t, 7, r.dy[t][own])

    def y_out(t):
        rs1[t].finish()
        value = r.own[t][...] + (
            r.rpart[t][own].astype(F32) + r.rfar[FIRST][t][...].astype(F32) + own_col(t, 7)
        )
        padded = plan.padded[t]
        for e in range(plan.examples[t]):
            out = value[:, e * padded : e * padded + plan.length[t]]
            r.v_y[t][e] = out.astype(BF16)
        row_copies.append(pltpu.make_async_copy(r.v_y[t], r.o_y[t], r.row_sem.at[t]))
        row_copies[-1].start()

    def c_norm(t):
        for copy in attn_w[TOWERS + t]:
            copy.wait()
        slot = (TOWERS + t) % 2
        gain, gain_own = full_col(t, 1), own_col(t, 1)

        def body(ls):
            dn, xhat = r.sums[SECOND][t], r.sums[FIRST][t]
            xh = xhat[:, ls].astype(F32)
            e = dn[:, ls].astype(F32) * gain
            m1 = jnp.sum(e, axis=0, keepdims=True) / width
            m2 = jnp.sum(e * xh, axis=0, keepdims=True) / width
            inv = r.row[t][2:3, ls]
            dres = r.dy[t][:, ls].astype(F32) + inv * (e - m1 - xh * m2)
            r.work_n[:, ls] = dres.astype(BF16)
            e_own = dn[own, ls].astype(F32) * gain_own
            r.own[t][:, ls] = r.dy[t][own, ls].astype(F32) + inv * (
                e_own - m1 - xhat[own, ls].astype(F32) * m2
            )

        lanes_loop(plan.lanes[t], 128, body)

        def mix(ls):
            r.work_m[:, ls] = nn(r.wout_v[slot], r.work_n[:, ls]).astype(BF16)

        lanes_loop(plan.lanes[t], TILE, mix)

    def c_heads(t):
        padded = plan.padded[t]
        qkv = r.qkv[t]
        scale = HEAD_DIM**-0.5
        for e in range(plan.examples[t]):
            base = e * padded

            def head(h, carry):
                rows_q = block(h, HEAD_DIM)
                rows_k = block(h + heads, HEAD_DIM)
                rows_v = block(h + 2 * heads, HEAD_DIM)
                keys = qkv[rows_k, base : base + padded]
                values = qkv[rows_v, base : base + padded].T
                dk = dv = None
                for q in range(padded // TILE):
                    at = base + q * TILE
                    dm = r.work_m[rows_q, at : at + TILE]
                    p = r.p[t][e * heads + h, :, q * TILE : (q + 1) * TILE]
                    dp = nn(values, dm)
                    pf = p.astype(F32)
                    delta = jnp.sum(pf * dp, axis=0, keepdims=True)
                    ds = (pf * (dp - delta)).astype(BF16)
                    dq = nn(keys, ds) * scale
                    r.work_h[rows_q, at : at + TILE] = dq.astype(BF16)
                    dk_q = nt(qkv[rows_q, at : at + TILE], ds)
                    dv_q = nt(dm, p)
                    dk = dk_q if dk is None else dk + dk_q
                    dv = dv_q if dv is None else dv + dv_q
                r.work_h[rows_k, base : base + padded] = (dk * scale).astype(BF16)
                r.work_h[rows_v, base : base + padded] = dv.astype(BF16)
                return carry

            lax.fori_loop(0, heads, head, 0)

    def c_prep(t):
        transpose_into(r.up_t, r.wqkv_v.at[(TOWERS + t) % 2], 3 * share, width)

    def c_dn(t):
        gain = full_col(t, 0)
        rs1[t].free()
        r.stat_own[t][...] = jnp.zeros_like(r.stat_own[t])

        def body(ls):
            dn = nn(r.up_t[:, : 3 * share], r.work_h[: 3 * share, ls])
            e = dn * gain
            xhat = (r.x[t][:, ls].astype(F32) - r.row[t][0:1, ls]) * r.row[t][1:2, ls]
            r.stat_own[t][0:1, ls] = jnp.sum(e, axis=0, keepdims=True)
            r.stat_own[t][1:2, ls] = jnp.sum(e * xhat, axis=0, keepdims=True)
            r.rpart[t][:, ls] = dn.astype(BF16)

        lanes_loop(plan.lanes[t], TILE, body)
        rs2[t].begin()
        stats[t].begin()
        if t == 0:
            for copy in attn_w[5]:
                copy.start()

    def c_grad(t):
        lanes = plan.lanes[t]
        unit = unit_of[t, ATTN]
        r.work_h[3 * share :, :lanes] = jnp.zeros((width - 3 * share, lanes), BF16)
        whole = 3 * share // TILE

        def step(at, carry):
            rows = block(at, TILE)
            spread(unit.all, nt(r.n[t][...], r.work_h[rows, :lanes]), rows)
            return carry

        lax.fori_loop(0, whole, step, 0)
        last = slice(whole * TILE, (whole + 1) * TILE)
        value = nt(r.n[t][...], r.work_h[last, :lanes])
        value = value + nt(r.work_n[:, :lanes], r.m[t][...])
        spread(unit.all, value, last)
        unit.send()

    def c_sum(t):
        lanes = plan.lanes[t]
        keep_sum(t, 0, r.work_h[:share, :lanes])
        keep_sum(t, 1, r.work_h[2 * share : 3 * share, :lanes])
        keep_sum(t, 2, r.work_n[own, :lanes])
        dn, xhat = r.sums[SECOND][t], r.sums[FIRST][t]
        keep_sum(t, 9, dn[own].astype(F32) * xhat[own].astype(F32))
        keep_sum(t, 11, dn[own])

    def last_norm(t):
        rs2[t].finish()
        stats[t].finish()
        gain = own_col(t, 0)
        dn = r.rpart[t][own].astype(F32) + r.rfar[SECOND][t][...].astype(F32)
        total = r.stat_chip[t][...] + r.stat_far[t][...]
        inv = r.row[t][1:2, :]
        xhat = (r.x[t][own].astype(F32) - r.row[t][0:1, :]) * inv
        value = r.own[t][...] + inv * (
            dn * gain - total[0:1] / width - xhat * (total[1:2] / width)
        )
        padded = plan.padded[t]
        for e in range(plan.examples[t]):
            out = value[:, e * padded : e * padded + plan.length[t]]
            r.v_dx[t][e] = out.astype(BF16)
        row_copies.append(pltpu.make_async_copy(r.v_dx[t], r.o_dx[t], r.row_sem.at[TOWERS + t]))
        row_copies[-1].start()
        keep_sum(t, 8, dn * xhat)
        keep_sum(t, 10, dn)

    def small_send(late):
        rows = r.small[...].T
        first, last = (EARLY, EARLY + LATE) if late else (0, EARLY)
        part = rows[first:last]
        if not plan.fused:
            r.o_rows[first:last] = part
            return
        r.rows[late][0] = part
        small_step(late, 0)

    def small_step(late, step):
        rows, land = r.rows[late].at[step], r.rows_in[late].at[step]
        device = (y_peer, near_dev, far_dev)[step]
        small_copies[late].append(launch(remote(rows, land, device)))

    def small_relay(late, step):
        if not plan.fused:
            return
        small_copies[late][step - 1].wait_recv()
        r.rows[late][step] = r.rows[late][step - 1] + r.rows_in[late][step - 1]
        small_step(late, step)

    def small_finish(late):
        if not plan.fused:
            return
        small_copies[late][2].wait_recv()
        total = r.rows[late][2] + r.rows_in[late][2]
        if late:
            r.o_rows[EARLY : EARLY + LATE] = total
        else:
            r.o_rows[:EARLY] = total

    small_copies = [[], []]

    barrier = pltpu.get_barrier_semaphore()
    partners = [sibling, across]
    if plan.fused:
        partners += [y_peer, near_dev, far_dev]
    for device in partners:
        pl.semaphore_signal(barrier, inc=1, device_id=device, device_id_type=MESH)
    loads = [
        pltpu.make_async_copy(src[t], dst[t], r.in_sem.at[i * TOWERS + t])
        for i, (src, dst) in enumerate(((r.in_x, r.v_y), (r.in_dy, r.v_dx)))
        for t in range(TOWERS)
    ]
    for copy in loads + attn_w[0] + ffn_w[0] + attn_w[1]:
        copy.start()
    param_rows()
    loads[0].wait()
    stage_in(r.x[0], 0, r.v_y[0])
    pl.semaphore_wait(barrier, len(partners))
    gp.start()
    gx[0].start()
    for t in range(1, TOWERS):
        loads[t].wait()
        stage_in(r.x[t], t, r.v_y[t])
    for t in range(TOWERS):
        loads[TOWERS + t].wait()
        stage_in(r.dy[t], t, r.v_dx[t])
    r.small[...] = jnp.zeros_like(r.small)
    gp.forward()
    gp.finish()
    gdy[0].start()
    gx[0].forward()
    gx[1].start()
    gx[0].finish()
    a_norm(0)
    a_qkv(0)
    a_heads(0)
    a_out(0)
    gdy[0].forward()
    ar1[0].cross()
    gx[1].forward()
    gx[1].finish()
    gdy[0].finish()
    a_norm(1)
    a_qkv(1)
    a_heads(1)
    gx[2].start()
    a_out(1)
    b_prep(0)
    ar1[1].cross()
    ar1[0].back()
    ar1[0].finish()
    b_main(0)
    b_down(0)
    b_ffn(0)
    b_sum(0)
    gx[2].forward()
    b_prep(1)
    gdy[1].start()
    gdy[2].start()
    gx[2].finish()
    a_norm(2)
    a_qkv(2)
    b_up(0)
    units[0].relay(0)
    units[0].relay(1)
    a_heads(2)
    units[0].relay(2)
    units[0].relay(3)
    a_out(2)
    ar1[2].cross()
    units[1].relay(0)
    ar1[1].back()
    ar1[1].finish()
    gdy[1].forward()
    gdy[1].finish()
    units[1].relay(1)
    b_main(1)
    units[1].relay(2)
    ar2[0].cross()
    b_down(1)
    b_up(1)
    b_ffn(1)
    units[1].relay(3)
    b_sum(1)
    b_prep(2)
    gdy[2].forward()
    rs1[0].cross()
    ar1[2].back()
    units[0].finish()
    gdy[2].finish()
    ar1[2].finish()
    b_main(2)
    b_down(2)
    rs1[1].cross()
    units[2].relay(0)
    b_sum(2)
    ar2[1].cross()
    units[1].finish()
    ar2[0].back()
    units[3].relay(0)
    ar2[2].cross()
    units[3].relay(1)
    b_ffn(2)
    y_out(0)
    units[2].relay(1)
    units[2].relay(2)
    units[4].relay(0)
    units[2].relay(3)
    b_up(2)
    ar2[0].finish()
    units[3].relay(2)
    c_norm(0)
    c_prep(0)
    units[4].relay(1)
    c_heads(0)
    c_sum(0)
    c_dn(0)
    ar2[1].back()
    units[4].relay(2)
    units[2].finish()
    units[3].relay(3)
    units[5].relay(0)
    ar2[1].finish()
    rs1[2].cross()
    c_grad(0)
    y_out(1)
    c_norm(1)
    c_prep(1)
    c_heads(1)
    c_dn(1)
    units[4].relay(3)
    rs2[0].cross()
    units[3].finish()
    c_sum(1)
    ar2[2].back()
    units[5].relay(1)
    c_grad(1)
    units[6].relay(0)
    y_out(2)
    rs2[1].cross()
    stats[0].cross()
    ar2[2].finish()
    c_norm(2)
    units[4].finish()
    units[6].relay(1)
    units[5].relay(2)
    c_heads(2)
    last_norm(0)
    c_prep(2)
    units[7].relay(0)
    stats[1].cross()
    c_dn(2)
    rs2[2].cross()
    units[6].relay(2)
    c_sum(2)
    units[5].relay(3)
    last_norm(1)
    small_send(0)
    c_grad(2)
    units[7].relay(1)
    units[7].relay(2)
    stats[2].cross()
    units[6].relay(3)
    last_norm(2)
    small_send(1)
    units[6].finish()
    units[5].finish()
    small_relay(0, 1)
    units[8].relay(0)
    small_relay(0, 2)
    units[8].relay(1)
    small_relay(1, 1)
    units[8].relay(2)
    units[8].relay(3)
    units[7].relay(3)
    units[7].finish()
    small_relay(1, 2)
    small_finish(0)
    units[8].finish()
    small_finish(1)
    for copy in list(pending):
        sent(copy)
    for unit in units:
        for copy in unit.hbm:
            copy.wait()
    for copy in row_copies:
        copy.wait()


def deliver(*refs):
    count = 2 * TOWERS + 4
    src, rows = refs[:count], refs[count]
    dst = refs[count + 1 : 2 * count + 1]
    qvb, outb, upb, downb, gains, shifts = refs[2 * count + 1 : 2 * count + 7]
    room = refs[2 * count + 7 : 3 * count + 7]
    in_sem, out_sem = refs[3 * count + 7 :]
    reads = [pltpu.make_async_copy(src[i], room[i], in_sem.at[i]) for i in range(count)]
    writes = [pltpu.make_async_copy(room[i], dst[i], out_sem.at[i]) for i in range(count)]
    for copy in reads:
        copy.start()
    share = rows.shape[1]
    for t in range(TOWERS):
        for j in range(2):
            qvb[t, j, :] = rows[small_row(t, j), :]
            gains[t, j, :] = rows[small_row(t, 8 + j), :]
            shifts[t, j, :] = rows[small_row(t, 10 + j), :]
        outb[t, :] = rows[small_row(t, 2), :]
        downb[t, :] = rows[small_row(t, 7), :]
        for j in range(upb.shape[1] // share):
            upb[t, j * share : (j + 1) * share] = rows[small_row(t, 3 + j), :]
    for read, write in zip(reads, writes):
        read.wait()
        write.start()
    for copy in writes:
        copy.wait()


def per_device(dp, tensor, *args):
    rows, ups = args[0:3], args[15:18]
    text_lengths, pair_lengths = args[3:5]
    qkv_w, qv_b, out_w, out_b, up_w, up_b, down_w, down_b, gain, shift = args[5:15]
    plan = Plan(rows, (qkv_w, out_w, up_w), dp, tensor)
    width, share, hidden = plan.width, plan.share, plan.hidden
    nz = plan.nz

    turned = [jnp.transpose(x, (0, 2, 1)) for x in rows]
    turned_up = [jnp.transpose(x, (0, 2, 1)) for x in ups]
    wqkv = jnp.transpose(qkv_w, (0, 2, 3, 1)).reshape(TOWERS, 3 * share, width)
    vmem = pl.BlockSpec(memory_space=pltpu.VMEM)
    hbm = pl.BlockSpec(memory_space=pl.ANY)
    smem = pl.BlockSpec(memory_space=pltpu.SMEM)

    ins, specs = SimpleNamespace(), SimpleNamespace()
    ins.in_x, specs.in_x = turned, [hbm] * TOWERS
    ins.in_dy, specs.in_dy = turned_up, [hbm] * TOWERS
    ins.in_text, specs.in_text = text_lengths, smem
    ins.in_pair, specs.in_pair = pair_lengths, smem
    ins.in_gain, specs.in_gain = gain, vmem
    ins.in_shift, specs.in_shift = shift, vmem
    ins.in_out_b, specs.in_out_b = out_b, vmem
    ins.in_qv_b, specs.in_qv_b = qv_b, vmem
    ins.in_down_b, specs.in_down_b = down_b, vmem
    ins.in_up_b, specs.in_up_b = up_b, vmem
    ins.wqkv, specs.wqkv = wqkv, hbm
    ins.wout, specs.wout = out_w, hbm
    ins.wup, specs.wup = up_w, hbm
    ins.wdown, specs.wdown = down_w, hbm

    outs = SimpleNamespace()
    outs.o_y = [Out(hbm, x.shape, BF16) for x in turned]
    outs.o_dx = [Out(hbm, x.shape, BF16) for x in turned]
    if plan.fused:
        outs.o_qkv = Out(hbm, (TOWERS, 3, plan.slab, share))
        outs.o_out = Out(hbm, (TOWERS, share, plan.slab))
        outs.o_up = Out(hbm, (TOWERS, plan.slab, hidden))
        outs.o_down = Out(hbm, (TOWERS, plan.slab, hidden))
    else:
        outs.o_g = Out(hbm, (3, TOWERS, width, width), BF16)
    outs.o_rows = Out(vmem, (SMALL, share))

    room = scratch(plan)
    in_refs, in_tree = flatten(vars(ins))
    out_refs, out_tree = flatten(vars(outs))
    room_refs, room_tree = flatten(vars(room))

    def body(*refs):
        first, second = len(in_refs), len(in_refs) + len(out_refs)
        r = SimpleNamespace()
        vars(r).update(jax.tree.unflatten(in_tree, refs[:first]))
        vars(r).update(jax.tree.unflatten(out_tree, refs[first:second]))
        vars(r).update(jax.tree.unflatten(room_tree, refs[second:]))
        kernel(plan, r)

    results = pl.pallas_call(
        body,
        out_shape=[jax.ShapeDtypeStruct(out.shape, out.dtype) for out in out_refs],
        in_specs=flatten(vars(specs))[0],
        out_specs=[out.spec for out in out_refs],
        scratch_shapes=room_refs,
        compiler_params=pltpu.CompilerParams(
            collective_id=1, has_side_effects=True, vmem_limit_bytes=67043328
        ),
        name="layer",
    )(*in_refs)
    got = SimpleNamespace(**jax.tree.unflatten(out_tree, results))

    if not plan.fused:
        sums = lax.psum_scatter(got.o_g.astype(F32), "dp", scatter_dimension=2, tiled=True)
        got.o_up, got.o_down = sums[UP], sums[DOWN]
        qkv = sums[ATTN, :, :, : 3 * share].reshape(TOWERS, sums.shape[2], 3, share)
        got.o_qkv = jnp.transpose(qkv, (0, 2, 1, 3))
        got.o_out = jnp.transpose(sums[ATTN, :, :, 3 * share :], (0, 2, 1))
        got.o_rows = lax.psum(got.o_rows, "dp")

    big = [*got.o_y, *got.o_dx, got.o_qkv, got.o_out, got.o_up, got.o_down]
    pairs = jax.ShapeDtypeStruct((TOWERS, 2, share), F32)
    single = jax.ShapeDtypeStruct((TOWERS, share), F32)
    small = [pairs, single, jax.ShapeDtypeStruct((TOWERS, hidden), F32), single, pairs, pairs]
    count = len(big)
    results = pl.pallas_call(
        deliver,
        out_shape=[jax.ShapeDtypeStruct(x.shape, x.dtype) for x in big] + small,
        in_specs=[hbm] * count + [vmem],
        out_specs=[hbm] * count + [vmem] * len(small),
        scratch_shapes=[pltpu.VMEM(x.shape, x.dtype) for x in big]
        + [pltpu.SemaphoreType.DMA((count,)), pltpu.SemaphoreType.DMA((count,))],
        compiler_params=pltpu.CompilerParams(vmem_limit_bytes=67043328),
    )(*big, got.o_rows)
    rows, sums = results[: 2 * TOWERS], results[2 * TOWERS : count]
    qvb, outb, upb, downb, gains, shifts = results[count:]
    return (
        *[jnp.transpose(x, (0, 2, 1)) for x in rows],
        jnp.transpose(sums[0], (0, 2, 1, 3)),
        qvb,
        sums[1],
        outb,
        sums[2],
        upb,
        jnp.transpose(sums[3], (0, 2, 1)),
        downb,
        gains,
        shifts,
    )


def solution(mesh):
    dp, tensor = mesh.shape["dp"], mesh.shape["tensor"]

    def step(*args):
        return per_device(dp, tensor, *args)

    rows = P("dp", None, "tensor")
    return jax.shard_map(
        step,
        mesh=mesh,
        in_specs=(
            rows,
            rows,
            rows,
            P("dp"),
            P("dp"),
            P(None, None, None, "tensor"),
            P(None, None, "tensor"),
            P(None, "tensor", None),
            P(None, "tensor"),
            P(None, None, "tensor"),
            P(None, "tensor"),
            P(None, "tensor", None),
            P(None, "tensor"),
            P(None, None, "tensor"),
            P(None, None, "tensor"),
            rows,
            rows,
            rows,
        ),
        out_specs=(
            rows,
            rows,
            rows,
            rows,
            rows,
            rows,
            P(None, "dp", None, "tensor"),
            P(None, None, "tensor"),
            P(None, "tensor", "dp"),
            P(None, "tensor"),
            P(None, "dp", "tensor"),
            P(None, "tensor"),
            P(None, "tensor", "dp"),
            P(None, "tensor"),
            P(None, None, "tensor"),
            P(None, None, "tensor"),
        ),
        check_vma=False,
    )
```
